32 devices in a mesh: space: 8 (over z, core), tracer: 4 (over y, x).
Axes of the slice: x: 2, y: 2, z: 4, core: 2. Of those that a mesh axis runs over, the one named last changes fastest.
Arguments:
- mixing_ratio_field: float32 [256, 2, 128, 256], P('tracer', None, 'space'), may hold values from 0.1 to 10
- eastward_face_cfl: float32 [2, 128, 256], P(None, 'space'), may hold values from 0.05 to 0.45
- northward_face_cfl: float32 [2, 128, 256], P(None, 'space'), may hold values from 0.05 to 0.45
- upward_face_cfl: float32 [2, 128, 256], P(None, 'space'), may hold values from 0.05 to 0.45
- thermal_anomaly: float32 [2, 128, 256], P(None, ('space', 'tracer')), may hold values from 0.8 to 1.2
- radiant_flux: float32 [2, 128, 256], P(None, ('space', 'tracer')), may hold values from 0.2 to 1
- daylight_mask: int32 [2, 128, 2], P(None, ('space', 'tracer')), may hold values from 0 to 1, as said below
- baseline_kinetic_coefficient: float32 [768], replicated, may hold values from 0.02 to 1
- arrhenius_barrier: float32 [768], replicated, may hold values from 0.5 to 3
- photodissociation_factor: float32 [768], replicated, may hold values from 0.02 to 1
- stoichiometry_table: int32 [3, 768], replicated, may hold values from 0 to 255
Outputs:
- result: float32 [256, 2, 128, 256], P(None, None, ('space', 'tracer'))
The draws below stay inside these ranges and needn't reach their ends.
Inputs may be any that keep to these rules, and one draw needn't show every extreme that they name: For every level l, row x below 64 and block b, daylight_mask[l, x, b] + daylight_mask[l, x + 64, b] == 1: a block and the block 64 rows further along the first dimension are never both sunlit or both dark.
All inputs are finite; a program needn't handle non-finite values.
Results may differ from the reference program's by a relative error of at most 0.0003.
Values sent between devices are 32-bit elements; how exact they have to be, the bound alone decides.
No kernel may reach another device: no remote copies, remote signals or barrier semaphores. Data moves between devices by JAX's collectives and lax.ppermute only.
A program may use at most 128 MiB of HBM per device.

```python
import math
import jax
import jax.numpy as jnp
from jax import lax

S = 256
R = 768
PATCH_SIZE = 128
SECTIONS = 3
DAY_STEPS = 2
NIGHT_STEPS = 1
GRID_WIDTH_NORTH = 256
ALTITUDE_TIERS = 2
GRID_WIDTH_EAST = 128


def draw_daylight_mask(key, part):
    half_rows = GRID_WIDTH_EAST // 2
    scores = jax.random.randint(key, (ALTITUDE_TIERS, half_rows, GRID_WIDTH_NORTH // PATCH_SIZE), 0, half_rows)
    rows = lax.broadcasted_iota(jnp.int32, (ALTITUDE_TIERS, half_rows, GRID_WIDTH_NORTH // PATCH_SIZE), 1)
    first_half = (scores <= rows).astype(jnp.int32)
    return jnp.concatenate([first_half, 1 - first_half], axis=1)


def touch_ends(array, own_key, least, high):
    shape = array.shape
    index_at = [jax.random.randint(jax.random.fold_in(own_key, axis), (), 0, shape[axis]) for axis in range(len(shape))]
    array = array.at[tuple(index_at)].set(least)
    longest = shape.index(max(shape))
    index_at[longest] = (index_at[longest] + 1) % shape[longest]
    return array.at[tuple(index_at)].set(high)


def block_levels(own_key, dims, pieces, least, top_value):
    gain, own = 1.0, jax.random.fold_in(own_key, 6)
    for position, shards_of in pieces:
        draws = jnp.exp(jax.random.uniform(jax.random.fold_in(own, position), (shards_of,), jnp.float32, least / len(pieces), top_value / len(pieces)))
        gain = gain * jnp.repeat(draws, dims[position] // shards_of).reshape([-1 if axis == position else 1 for axis in range(len(dims))])
    return gain


def setup_inputs(seed: int = 0) -> dict:
    key_list = jax.random.split(jax.random.key(seed), 12)
    mixing_ratio_field = jnp.clip(jnp.exp(math.log(10.0) - 4.6051702 * jax.random.uniform(key_list[0], (S, ALTITUDE_TIERS, GRID_WIDTH_EAST, GRID_WIDTH_NORTH), jnp.float32) ** block_levels(key_list[0], (S, ALTITUDE_TIERS, GRID_WIDTH_EAST, GRID_WIDTH_NORTH), ((0, 4), (2, 8)), -0.2, 0.2)), 0.1, 10.0)
    eastward_face_cfl = jnp.clip(0.05 + 0.39999999 * jax.random.uniform(key_list[1], (ALTITUDE_TIERS, GRID_WIDTH_EAST, GRID_WIDTH_NORTH), jnp.float32) ** block_levels(key_list[1], (ALTITUDE_TIERS, GRID_WIDTH_EAST, GRID_WIDTH_NORTH), ((1, 8),), -0.2, 0.2), 0.05, 0.45)
    northward_face_cfl = jnp.clip(0.05 + 0.39999999 * jax.random.uniform(key_list[2], (ALTITUDE_TIERS, GRID_WIDTH_EAST, GRID_WIDTH_NORTH), jnp.float32) ** block_levels(key_list[2], (ALTITUDE_TIERS, GRID_WIDTH_EAST, GRID_WIDTH_NORTH), ((1, 8),), -0.2, 0.2), 0.05, 0.45)
    upward_face_cfl = jnp.clip(0.05 + 0.39999999 * jax.random.uniform(key_list[3], (ALTITUDE_TIERS, GRID_WIDTH_EAST, GRID_WIDTH_NORTH), jnp.float32) ** block_levels(key_list[3], (ALTITUDE_TIERS, GRID_WIDTH_EAST, GRID_WIDTH_NORTH), ((1, 8),), -0.2, 0.2), 0.05, 0.45)
    thermal_anomaly = jnp.clip(0.8 + 0.40000004 * jax.random.uniform(key_list[4], (ALTITUDE_TIERS, GRID_WIDTH_EAST, GRID_WIDTH_NORTH), jnp.float32) ** block_levels(key_list[4], (ALTITUDE_TIERS, GRID_WIDTH_EAST, GRID_WIDTH_NORTH), ((1, 32),), -0.2, 0.2), 0.8, 1.2)
    radiant_flux = jnp.clip(0.2 + 0.8 * jax.random.uniform(key_list[5], (ALTITUDE_TIERS, GRID_WIDTH_EAST, GRID_WIDTH_NORTH), jnp.float32) ** block_levels(key_list[5], (ALTITUDE_TIERS, GRID_WIDTH_EAST, GRID_WIDTH_NORTH), ((1, 32),), -0.2, 0.2), 0.2, 1.0)
    daylight_mask = draw_daylight_mask(jax.random.fold_in(key_list[11], 71), 0)
    baseline_kinetic_coefficient = jnp.clip(jnp.exp(jax.random.uniform(key_list[7], (R,), jnp.float32, math.log(0.02), math.log(1.0))), 0.02, 1.0)
    arrhenius_barrier = jnp.clip(jax.random.uniform(key_list[8], (R,), jnp.float32, 0.5, 3.0), 0.5, 3.0)
    photodissociation_factor = jnp.clip(jnp.exp(jax.random.uniform(key_list[9], (R,), jnp.float32, math.log(0.02), math.log(1.0))), 0.02, 1.0)
    stoichiometry_table = touch_ends(jax.random.randint(key_list[10], (3, R), 0, S), jax.random.fold_in(key_list[10], 1), 0, S - 1).astype(jnp.int32)
    return {"mixing_ratio_field": mixing_ratio_field, "eastward_face_cfl": eastward_face_cfl, "northward_face_cfl": northward_face_cfl, "upward_face_cfl": upward_face_cfl, "thermal_anomaly": thermal_anomaly, "radiant_flux": radiant_flux, "daylight_mask": daylight_mask, "baseline_kinetic_coefficient": baseline_kinetic_coefficient, "arrhenius_barrier": arrhenius_barrier, "photodissociation_factor": photodissociation_factor, "stoichiometry_table": stoichiometry_table}


def minmod(left_slope, right_slope):
    return 0.5 * (jnp.sign(left_slope) + jnp.sign(right_slope)) * jnp.minimum(jnp.abs(left_slope), jnp.abs(right_slope))


def face_flux(far_cell, near_cell, past_cell, courant):
    return courant * (near_cell + 0.5 * (1.0 - courant) * minmod(near_cell - far_cell, past_cell - near_cell))


def sweep_rows(field, courant):
    inner = field.shape[2] - 4
    fluxes = face_flux(field[:, :, 0:inner + 1], field[:, :, 1:inner + 2], field[:, :, 2:inner + 3], courant[None, :, 2:inner + 3])
    return field[:, :, 2:inner + 2] - (fluxes[:, :, 1:] - fluxes[:, :, :-1])


def sweep_cols(field, courant):
    fluxes = face_flux(jnp.roll(field, 2, axis=3), jnp.roll(field, 1, axis=3), field, courant[None])
    return field - (jnp.roll(fluxes, -1, axis=3) - fluxes)


def sweep_levels(field, courant):
    zero_layer = jnp.zeros_like(field[:, :1])
    lower_cells = jnp.concatenate([zero_layer, field[:, :-1]], axis=1)
    upper_cells = jnp.concatenate([field[:, 1:], zero_layer], axis=1)
    fluxes = face_flux(lower_cells, field, upper_cells, courant[None])
    inflow = jnp.concatenate([zero_layer, fluxes[:, :-1]], axis=1)
    return field - (fluxes - inflow)


def react_ref(field, warmth, glow, baseline_kinetic_coefficient, arrhenius_barrier, photodissociation_factor, stoichiometry_table, substeps, lit):
    species = field.shape[0]
    rates = baseline_kinetic_coefficient[:, None] * jnp.exp(-arrhenius_barrier[:, None] * (warmth[None, :] - 1.0))
    if lit:
        rates = rates + photodissociation_factor[:, None] * glow[None, :]
    step_size = 1.0 / substeps
    for sub_num in range(substeps):
        first_conc = field[stoichiometry_table[0]]
        second_conc = field[stoichiometry_table[1]]
        speed = rates * first_conc * second_conc
        produced = jax.ops.segment_sum(speed, stoichiometry_table[2], num_segments=species)
        consumed = jax.ops.segment_sum(rates * second_conc, stoichiometry_table[0], num_segments=species)
        consumed = consumed + jax.ops.segment_sum(rates * first_conc, stoichiometry_table[1], num_segments=species)
        field = (field + step_size * produced) / (1.0 + step_size * consumed)
    return field


def reference(mixing_ratio_field, eastward_face_cfl, northward_face_cfl, upward_face_cfl, thermal_anomaly, radiant_flux, daylight_mask, baseline_kinetic_coefficient, arrhenius_barrier, photodissociation_factor, stoichiometry_table):
    field = mixing_ratio_field
    padded_courant = jnp.pad(eastward_face_cfl, ((0, 0), (2, 2), (0, 0)))
    for section_num in range(SECTIONS):
        padded = jnp.pad(field, ((0, 0), (0, 0), (2, 2), (0, 0)))
        field = sweep_rows(padded, padded_courant)
        field = sweep_cols(field, northward_face_cfl)
        field = sweep_levels(field, upward_face_cfl)
    species = field.shape[0]
    blocks = jnp.moveaxis(field.reshape(species, -1, PATCH_SIZE), 1, 0)
    warm_patches = thermal_anomaly.reshape(-1, PATCH_SIZE)
    glow_blocks = radiant_flux.reshape(-1, PATCH_SIZE)
    flags = daylight_mask.reshape(-1)

    def one_block(items):
        block, warmth, glow, flag = items
        bright = react_ref(block, warmth, glow, baseline_kinetic_coefficient, arrhenius_barrier, photodissociation_factor, stoichiometry_table, DAY_STEPS, True)
        dark = react_ref(block, warmth, glow, baseline_kinetic_coefficient, arrhenius_barrier, photodissociation_factor, stoichiometry_table, NIGHT_STEPS, False)
        return jnp.where(flag == 1, bright, dark)

    reacted = lax.map(one_block, (blocks, warm_patches, glow_blocks, flags))
    return jnp.moveaxis(reacted, 0, 1).reshape(field.shape)
```

```python
import functools

import jax
import jax.numpy as jnp
from jax import lax
from jax.experimental import pallas as pl
from jax.experimental.pallas import tpu as pltpu
from jax.sharding import PartitionSpec as P

SECTIONS = 3
DAY_STEPS = 2
LANES = 128
SUB = 8
LOW = 2 * SECTIONS
HIGH = SECTIONS


def flat_rows(cells):
    *lead, rows, width = cells.shape
    sub = min(rows, SUB)
    split = cells.reshape(*lead, rows // sub, sub, width // LANES, LANES)
    return jnp.moveaxis(split, -2, -3).reshape(-1, LANES)


class Sizes:
    def __init__(self, field, groups):
        self.species, self.levels, self.rows, self.width = field.shape
        self.tiles = self.width // LANES
        self.groups = groups
        self.part = self.rows // groups
        self.blocks = self.levels * self.tiles * self.part
        self.stride = self.levels * self.rows * self.tiles
        self.columns = self.levels * self.tiles
        self.low_rows = LOW * self.columns * self.species
        self.high_rows = HIGH * self.columns * self.species
        self.edge_rows = 3 * self.columns * SUB

    def source_row(self, level, row, tile):
        return ((level * (self.rows // SUB) + row // SUB) * self.tiles + tile) * SUB + row % SUB

    def pairs(self):
        return [(level, tile) for level in range(self.levels) for tile in range(self.tiles)]


def pack_kernel(z, x_ref, east_ref, north_ref, up_ref, low_ref, high_ref):
    for offset, rows, out_ref in ((z.rows - LOW, LOW, low_ref), (0, HIGH, high_ref)):
        for row in range(rows):
            for col, (level, tile) in enumerate(z.pairs()):
                for start in range(0, z.species, SUB):
                    source = start * z.stride + z.source_row(level, row + offset, tile)
                    target = (row * z.columns + col) * z.species + start
                    out_ref[pl.ds(target, SUB), :] = x_ref[pl.ds(source, SUB, stride=z.stride), :]
    for out_ref, base, last in ((low_ref, z.low_rows, True), (high_ref, z.high_rows, False)):
        row = z.rows - SUB if last else 0
        for kind, ref in enumerate((east_ref, north_ref, up_ref)):
            for col, (level, tile) in enumerate(z.pairs()):
                target = base + (kind * z.columns + col) * SUB
                source = z.source_row(level, row, tile)
                out_ref[pl.ds(target, SUB), :] = ref[pl.ds(source, SUB), :]


def middle(a, b):
    return jnp.maximum(jnp.minimum(a, b), jnp.minimum(jnp.maximum(a, b), 0.0))


def shift_columns(parts, amount):
    lane = lax.broadcasted_iota(jnp.int32, parts[0].shape, 1)
    rolled = [pltpu.roll(part, amount % LANES, 1) for part in parts]
    count = len(parts)
    if amount > 0:
        return [jnp.where(lane < amount, rolled[i - 1], rolled[i]) for i in range(count)]
    return [jnp.where(lane >= LANES + amount, rolled[(i + 1) % count], rolled[i]) for i in range(count)]


def transport_kernel(z, x_ref, east_ref, north_ref, up_ref, low_ref, high_ref, out_ref, coef, first, second):
    span = z.rows + 2 * SUB

    def coef_row(kind, which, col, j):
        return ((kind * 2 + which) * z.columns + col) * span + j

    for kind, ref in enumerate((east_ref, north_ref, up_ref)):
        for level in range(z.levels):
            for piece in range(span // SUB):
                values = []
                for tile in range(z.tiles):
                    col = level * z.tiles + tile
                    edge = (kind * z.columns + col) * SUB
                    if piece == 0:
                        value = low_ref[pl.ds(z.low_rows + edge, SUB), :]
                    elif piece == span // SUB - 1:
                        value = high_ref[pl.ds(z.high_rows + edge, SUB), :]
                    else:
                        value = ref[pl.ds(z.source_row(level, (piece - 1) * SUB, tile), SUB), :]
                    values.append(value)
                if kind == 1:
                    values = shift_columns(values, -1)
                for tile, value in enumerate(values):
                    col = level * z.tiles + tile
                    coef[pl.ds(coef_row(kind, 0, col, piece * SUB), SUB), :] = value
                    coef[pl.ds(coef_row(kind, 1, col, piece * SUB), SUB), :] = 0.5 * value * (1.0 - value)

    def weights(kind, col, j):
        return [
            jnp.broadcast_to(coef[pl.ds(coef_row(kind, which, col, j), 1), :], (SUB, LANES))
            for which in range(2)
        ]

    def one_tile(index, carry):
        start = pl.multiple_of(index * SUB, SUB)

        def place(j, col):
            return pl.ds((j * z.columns + col) * SUB, SUB)

        def initial(j, col):
            level, tile = divmod(col, z.tiles)
            row = j - SUB
            if row < 0:
                base = ((row + LOW) * z.columns + col) * z.species
                return low_ref[pl.ds(pl.multiple_of(base + start, SUB), SUB), :]
            if row >= z.rows:
                base = ((row - z.rows) * z.columns + col) * z.species
                return high_ref[pl.ds(pl.multiple_of(base + start, SUB), SUB), :]
            return x_ref[pl.ds(start * z.stride + z.source_row(level, row, tile), SUB, stride=z.stride), :]

        cols = range(z.columns)
        for step in range(SECTIONS):
            bottom = SUB - LOW + 2 * step
            top = SUB + z.rows + HIGH - step
            if step == 0:
                read = initial
            else:
                source = (first, second)[(step + 1) % 2]
                read = lambda j, col, source=source: source[place(j, col), :]
            here = [read(bottom + 1, col) for col in cols]
            below = [read(bottom, col) for col in cols]
            rise = [here[col] - below[col] for col in cols]
            into = None
            for j in range(bottom + 1, top - 1):
                above = [read(j + 1, col) for col in cols]
                climb = [above[col] - here[col] for col in cols]
                out = []
                for col in cols:
                    a, b = weights(0, col, j + 1)
                    out.append(a * here[col] + b * middle(rise[col], climb[col]))
                if into is not None:
                    c = [here[col] - (out[col] - into[col]) for col in cols]
                    for level in range(z.levels):
                        mine = slice(level * z.tiles, (level + 1) * z.tiles)
                        row = c[mine]
                        back = [v - w for v, w in zip(row, shift_columns(row, 1))]
                        ahead = shift_columns(back, -1)
                        leave = []
                        for tile in range(z.tiles):
                            a, b = weights(1, level * z.tiles + tile, j)
                            leave.append(a * row[tile] + b * middle(back[tile], ahead[tile]))
                        enter = shift_columns(leave, 1)
                        c[mine] = [row[t] - (leave[t] - enter[t]) for t in range(z.tiles)]
                    for tile in range(z.tiles):
                        column = [c[level * z.tiles + tile] for level in range(z.levels)]
                        steps = [column[0]]
                        steps += [column[k + 1] - column[k] for k in range(z.levels - 1)]
                        steps += [-column[-1]]
                        lift = None
                        for level in range(z.levels):
                            col = level * z.tiles + tile
                            a, b = weights(2, col, j)
                            rising = a * column[level] + b * middle(steps[level], steps[level + 1])
                            net = rising if lift is None else rising - lift
                            lift = rising
                            value = column[level] - net
                            if step < SECTIONS - 1:
                                (first, second)[step % 2][place(j, col), :] = value
                            else:
                                group, part_row = divmod(j - SUB, z.part)
                                target = (level * z.tiles + tile) * z.part + part_row
                                base = (group * z.species + start) * z.blocks + target
                                out_ref[pl.ds(base, SUB, stride=z.blocks), :] = value
                into = out
                rise = climb
                here = above
        return carry

    lax.fori_loop(0, z.species // SUB, one_tile, 0)


def chemistry_kernel(
    species, blocks, c_ref, warm_ref, glow_ref, lit_ref, rate_ref, barrier_ref, photo_ref, table_ref,
    out_ref, made_a, made_b, lost_a, lost_b, lost_c, lost_d,
):
    pieces = blocks // SUB
    reactions = rate_ref.shape[0]
    made = (made_a, made_b)
    lost = ((lost_a, lost_b), (lost_c, lost_d))

    def cell(index, piece):
        return pl.ds(pl.multiple_of(index * blocks, SUB) + piece * SUB, SUB)

    lit = [lit_ref[pl.ds(piece * SUB, SUB), :] == 1 for piece in range(pieces)]
    warm = [warm_ref[pl.ds(piece * SUB, SUB), :] - 1.0 for piece in range(pieces)]
    glow = [jnp.where(lit[p], glow_ref[pl.ds(p * SUB, SUB), :], 0.0) for p in range(pieces)]

    for sub in range(DAY_STEPS):
        source = c_ref if sub == 0 else out_ref
        steps = [jnp.where(lit[p], float(DAY_STEPS), 1.0) for p in range(pieces)]

        def begin(s, carry):
            for p in range(pieces):
                made[0][cell(s, p), :] = steps[p] * source[cell(s, p), :]
                made[1][cell(s, p), :] = jnp.zeros((SUB, LANES), jnp.float32)
                for k in range(2):
                    for side in range(2):
                        fill = steps[p] if k == 0 and side == 0 else jnp.zeros((SUB, LANES), jnp.float32)
                        lost[k][side][cell(s, p), :] = fill
            return carry

        lax.fori_loop(0, species, begin, 0, unroll=4)

        def react(r, parity):
            first, second, product = table_ref[0, r], table_ref[1, r], table_ref[2, r]
            rate, barrier, photo = rate_ref[r], barrier_ref[r], photo_ref[r]
            for p in range(pieces):
                k = rate * jnp.exp(-barrier * warm[p]) + photo * glow[p]
                x = source[cell(first, p), :]
                y = source[cell(second, p), :]
                kx = k * x
                ky = k * y
                made[parity][cell(product, p), :] += kx * y
                lost[parity][0][cell(first, p), :] += ky
                lost[parity][1][cell(second, p), :] += kx

        def two(i, carry):
            react(2 * i, 0)
            react(2 * i + 1, 1)
            return carry

        lax.fori_loop(0, reactions // 2, two, 0, unroll=4)

        def finish(s, carry):
            for p in range(pieces):
                at = cell(s, p)
                top = made[0][at, :] + made[1][at, :]
                bottom = (lost[0][0][at, :] + lost[0][1][at, :]) + (lost[1][0][at, :] + lost[1][1][at, :])
                value = top / bottom
                if sub > 0:
                    value = jnp.where(lit[p], value, source[at, :])
                out_ref[at, :] = value
            return carry

        lax.fori_loop(0, species, finish, 0, unroll=4)


VMEM = pl.BlockSpec(memory_space=pltpu.VMEM)
SMEM = pl.BlockSpec(memory_space=pltpu.SMEM)


def rows_of(count):
    return jax.ShapeDtypeStruct((count, LANES), jnp.float32)


def pack(z, *flat):
    return pl.pallas_call(
        functools.partial(pack_kernel, z),
        out_shape=(rows_of(z.low_rows + z.edge_rows), rows_of(z.high_rows + z.edge_rows)),
        in_specs=[VMEM] * 4,
        out_specs=(VMEM, VMEM),
        name="pack",
    )(*flat)


def transport(z, *flat):
    span = z.rows + 2 * SUB
    return pl.pallas_call(
        functools.partial(transport_kernel, z),
        out_shape=rows_of(z.groups * z.species * z.blocks),
        in_specs=[VMEM] * 6,
        out_specs=VMEM,
        scratch_shapes=[
            pltpu.VMEM((6 * z.columns * span, LANES), jnp.float32),
            pltpu.VMEM((span * z.columns * SUB, LANES), jnp.float32),
            pltpu.VMEM((span * z.columns * SUB, LANES), jnp.float32),
        ],
        name="transport",
    )(*flat)


def chemistry(species, blocks, *args):
    size = (species * blocks, LANES)
    return pl.pallas_call(
        functools.partial(chemistry_kernel, species, blocks),
        out_shape=rows_of(species * blocks),
        in_specs=[VMEM] * 4 + [SMEM] * 4,
        out_specs=VMEM,
        scratch_shapes=[pltpu.VMEM(size, jnp.float32)] * 6,
        name="chemistry",
    )(*args)


def body(
    mixing_ratio_field,
    eastward_face_cfl,
    northward_face_cfl,
    upward_face_cfl,
    thermal_anomaly,
    radiant_flux,
    daylight_mask,
    baseline_kinetic_coefficient,
    arrhenius_barrier,
    photodissociation_factor,
    stoichiometry_table,
):
    groups = lax.axis_size("tracer")
    strips = lax.axis_size("space")
    z = Sizes(mixing_ratio_field, groups)
    flat = [
        flat_rows(a)
        for a in (mixing_ratio_field, eastward_face_cfl, northward_face_cfl, upward_face_cfl)
    ]
    low, high = pack(z, *flat)
    low = lax.ppermute(low, "space", [(i, i + 1) for i in range(strips - 1)])
    high = lax.ppermute(high, "space", [(i + 1, i) for i in range(strips - 1)])
    moved = transport(z, *flat, low, high)
    moved = moved.reshape(groups, z.species * z.blocks, LANES)
    moved = lax.all_to_all(moved, "tracer", split_axis=0, concat_axis=0, tiled=True)
    species = z.species * groups
    lit = jnp.moveaxis(daylight_mask, 2, 1).reshape(z.blocks, 1)
    lit = jnp.broadcast_to(lit, (z.blocks, LANES))
    out = chemistry(
        species,
        z.blocks,
        moved.reshape(species * z.blocks, LANES),
        flat_rows(thermal_anomaly),
        flat_rows(radiant_flux),
        lit,
        baseline_kinetic_coefficient,
        arrhenius_barrier,
        photodissociation_factor,
        stoichiometry_table,
    )
    out = out.reshape(species, z.levels, z.tiles, z.part, LANES)
    return jnp.moveaxis(out, 2, 3).reshape(species, z.levels, z.part, z.width)


def solution(mesh):
    placed = (
        P("tracer", None, "space", None),
        P(None, "space", None),
        P(None, "space", None),
        P(None, "space", None),
        P(None, ("space", "tracer"), None),
        P(None, ("space", "tracer"), None),
        P(None, ("space", "tracer"), None),
        P(),
        P(),
        P(),
        P(),
    )
    return jax.shard_map(
        body,
        mesh=mesh,
        in_specs=placed,
        out_specs=P(None, None, ("space", "tracer"), None),
        check_vma=False,
    )
```

```python
import functools

import jax
import jax.numpy as jnp
from jax import lax
from jax.experimental import pallas as pl
from jax.experimental.pallas import tpu as pltpu
from jax.sharding import PartitionSpec as P

SECTIONS = 3
DAY_STEPS = 2
LANES = 128
SUB = 8
LOW = 2 * SECTIONS
HIGH = SECTIONS
TOGETHER = 2


def flat_rows(cells):
    *lead, rows, width = cells.shape
    sub = min(rows, SUB)
    split = cells.reshape(*lead, rows // sub, sub, width // LANES, LANES)
    return jnp.moveaxis(split, -2, -3).reshape(-1, LANES)


class Sizes:
    def __init__(self, field, groups):
        self.species, self.levels, self.rows, self.width = field.shape
        self.tiles = self.width // LANES
        self.groups = groups
        self.part = self.rows // groups
        self.blocks = self.levels * self.tiles * self.part
        self.stride = self.levels * self.rows * self.tiles
        self.columns = self.levels * self.tiles
        self.low_rows = LOW * self.columns * self.species
        self.high_rows = HIGH * self.columns * self.species
        self.edge_rows = 3 * self.columns * SUB

    def source_row(self, level, row, tile):
        return ((level * (self.rows // SUB) + row // SUB) * self.tiles + tile) * SUB + row % SUB

    def pairs(self):
        return [(level, tile) for level in range(self.levels) for tile in range(self.tiles)]


def pack_kernel(z, x_ref, east_ref, north_ref, up_ref, low_ref, high_ref):
    def one_species(index, carry):
        for offset, rows, out_ref in ((z.rows - LOW, LOW, low_ref), (0, HIGH, high_ref)):
            for col, (level, tile) in enumerate(z.pairs()):
                source = index * z.stride + z.source_row(level, offset, tile)
                target = (index * z.columns + col) * rows
                out_ref[pl.ds(target, rows), :] = x_ref[pl.ds(source, rows), :]
        return carry

    lax.fori_loop(0, z.species, one_species, 0, unroll=4)
    for out_ref, base, last in ((low_ref, z.low_rows, True), (high_ref, z.high_rows, False)):
        row = z.rows - SUB if last else 0
        for kind, ref in enumerate((east_ref, north_ref, up_ref)):
            for col, (level, tile) in enumerate(z.pairs()):
                target = base + (kind * z.columns + col) * SUB
                source = z.source_row(level, row, tile)
                out_ref[pl.ds(target, SUB), :] = ref[pl.ds(source, SUB), :]


def middle(a, b):
    return jnp.maximum(jnp.minimum(a, b), jnp.minimum(jnp.maximum(a, b), 0.0))


def shift_columns(parts, amount):
    lane = lax.broadcasted_iota(jnp.int32, parts[0].shape, 1)
    rolled = [pltpu.roll(part, amount % LANES, 1) for part in parts]
    count = len(parts)
    if amount > 0:
        return [jnp.where(lane < amount, rolled[i - 1], rolled[i]) for i in range(count)]
    return [jnp.where(lane >= LANES + amount, rolled[(i + 1) % count], rolled[i]) for i in range(count)]


def transport_kernel(z, x_ref, east_ref, north_ref, up_ref, low_ref, high_ref, out_ref, coef, *scratch):
    span = z.rows + 2 * SUB

    def coef_row(kind, which, col, j):
        return ((kind * 2 + which) * z.columns + col) * span + j

    for kind, ref in enumerate((east_ref, north_ref, up_ref)):
        for level in range(z.levels):
            for piece in range(span // SUB):
                values = []
                for tile in range(z.tiles):
                    col = level * z.tiles + tile
                    edge = (kind * z.columns + col) * SUB
                    if piece == 0:
                        value = low_ref[pl.ds(z.low_rows + edge, SUB), :]
                    elif piece == span // SUB - 1:
                        value = high_ref[pl.ds(z.high_rows + edge, SUB), :]
                    else:
                        value = ref[pl.ds(z.source_row(level, (piece - 1) * SUB, tile), SUB), :]
                    values.append(value)
                if kind == 1:
                    values = shift_columns(values, -1)
                for tile, value in enumerate(values):
                    col = level * z.tiles + tile
                    coef[pl.ds(coef_row(kind, 0, col, piece * SUB), SUB), :] = value
                    coef[pl.ds(coef_row(kind, 1, col, piece * SUB), SUB), :] = 0.5 * value * (1.0 - value)

    def weights(kind, col, j):
        return [coef[pl.ds(coef_row(kind, which, col, j), SUB), :] for which in range(2)]

    cols = range(z.columns)

    def one_species(index, fields, fluxes):
        for col, (level, tile) in enumerate(z.pairs()):
            base = index * z.columns + col
            fields[0][pl.ds(col * span + SUB - LOW, LOW), :] = low_ref[pl.ds(base * LOW, LOW), :]
            fields[0][pl.ds(col * span + SUB + z.rows, HIGH), :] = high_ref[pl.ds(base * HIGH, HIGH), :]
            for row in range(0, z.rows, SUB):
                source = index * z.stride + z.source_row(level, row, tile)
                fields[0][pl.ds(col * span + SUB + row, SUB), :] = x_ref[pl.ds(pl.multiple_of(source, SUB), SUB), :]
        for step in range(SECTIONS):
            read, write = fields[step % 2], fields[(step + 1) % 2]
            bottom = SUB - LOW + 2 * (step + 1)
            top = SUB + z.rows + HIGH - (step + 1)
            for j in range(bottom - 1, top, SUB):
                for col in cols:
                    below, here, above = [read[pl.ds(col * span + j + k, SUB), :] for k in (-1, 0, 1)]
                    a, b = weights(0, col, j + 1)
                    fluxes[pl.ds(col * span + j, SUB), :] = a * here + b * middle(here - below, above - here)
            for j in range(bottom, top, SUB):
                c = []
                for col in cols:
                    leave = fluxes[pl.ds(col * span + j, SUB), :]
                    enter = fluxes[pl.ds(col * span + j - 1, SUB), :]
                    c.append(read[pl.ds(col * span + j, SUB), :] - (leave - enter))
                for level in range(z.levels):
                    mine = slice(level * z.tiles, (level + 1) * z.tiles)
                    row = c[mine]
                    back = [v - w for v, w in zip(row, shift_columns(row, 1))]
                    ahead = shift_columns(back, -1)
                    leave = []
                    for tile in range(z.tiles):
                        a, b = weights(1, level * z.tiles + tile, j)
                        leave.append(a * row[tile] + b * middle(back[tile], ahead[tile]))
                    enter = shift_columns(leave, 1)
                    c[mine] = [row[t] - (leave[t] - enter[t]) for t in range(z.tiles)]
                for tile in range(z.tiles):
                    column = [c[level * z.tiles + tile] for level in range(z.levels)]
                    steps = [column[0]]
                    steps += [column[k + 1] - column[k] for k in range(z.levels - 1)]
                    steps += [-column[-1]]
                    lift = None
                    for level in range(z.levels):
                        col = level * z.tiles + tile
                        a, b = weights(2, col, j)
                        rising = a * column[level] + b * middle(steps[level], steps[level + 1])
                        net = rising if lift is None else rising - lift
                        lift = rising
                        value = column[level] - net
                        if step < SECTIONS - 1:
                            write[pl.ds(col * span + j, SUB), :] = value
                            continue
                        for start in range(0, SUB, z.part):
                            group = (j - SUB + start) // z.part
                            base = (group * z.species + index) * z.blocks + col * z.part
                            out_ref[pl.ds(base, z.part), :] = value[start : start + z.part]

    def some_species(index, carry):
        for k in range(TOGETHER):
            one_species(index * TOGETHER + k, scratch[3 * k : 3 * k + 2], scratch[3 * k + 2])
        return carry

    lax.fori_loop(0, z.species // TOGETHER, some_species, 0)


def chemistry_kernel(
    species, blocks, c_ref, warm_ref, glow_ref, lit_ref, rate_ref, barrier_ref, photo_ref, table_ref,
    out_ref, made_a, made_b, lost_a, lost_b, lost_c, lost_d,
):
    pieces = blocks // SUB
    reactions = rate_ref.shape[0]
    made = (made_a, made_b)
    lost = ((lost_a, lost_b), (lost_c, lost_d))

    def cell(index, piece):
        return pl.ds(pl.multiple_of(index * blocks, SUB) + piece * SUB, SUB)

    lit = [lit_ref[pl.ds(piece * SUB, SUB), :] == 1 for piece in range(pieces)]
    warm = [warm_ref[pl.ds(piece * SUB, SUB), :] - 1.0 for piece in range(pieces)]
    glow = [jnp.where(lit[p], glow_ref[pl.ds(p * SUB, SUB), :], 0.0) for p in range(pieces)]

    for sub in range(DAY_STEPS):
        source = c_ref if sub == 0 else out_ref
        steps = [jnp.where(lit[p], float(DAY_STEPS), 1.0) for p in range(pieces)]

        def begin(s, carry):
            for p in range(pieces):
                made[0][cell(s, p), :] = steps[p] * source[cell(s, p), :]
                made[1][cell(s, p), :] = jnp.zeros((SUB, LANES), jnp.float32)
                for k in range(2):
                    for side in range(2):
                        fill = steps[p] if k == 0 and side == 0 else jnp.zeros((SUB, LANES), jnp.float32)
                        lost[k][side][cell(s, p), :] = fill
            return carry

        lax.fori_loop(0, species, begin, 0, unroll=4)

        def react(r, parity):
            first, second, product = table_ref[0, r], table_ref[1, r], table_ref[2, r]
            rate, barrier, photo = rate_ref[r], barrier_ref[r], photo_ref[r]
            for p in range(pieces):
                k = rate * jnp.exp(-barrier * warm[p]) + photo * glow[p]
                x = source[cell(first, p), :]
                y = source[cell(second, p), :]
                kx = k * x
                ky = k * y
                made[parity][cell(product, p), :] += kx * y
                lost[parity][0][cell(first, p), :] += ky
                lost[parity][1][cell(second, p), :] += kx

        def two(i, carry):
            react(2 * i, 0)
            react(2 * i + 1, 1)
            return carry

        lax.fori_loop(0, reactions // 2, two, 0, unroll=4)

        def finish(s, carry):
            for p in range(pieces):
                at = cell(s, p)
                top = made[0][at, :] + made[1][at, :]
                bottom = (lost[0][0][at, :] + lost[0][1][at, :]) + (lost[1][0][at, :] + lost[1][1][at, :])
                value = top / bottom
                if sub > 0:
                    value = jnp.where(lit[p], value, source[at, :])
                out_ref[at, :] = value
            return carry

        lax.fori_loop(0, species, finish, 0, unroll=4)


VMEM = pl.BlockSpec(memory_space=pltpu.VMEM)
SMEM = pl.BlockSpec(memory_space=pltpu.SMEM)


def rows_of(count):
    return jax.ShapeDtypeStruct((count, LANES), jnp.float32)


def pack(z, *flat):
    return pl.pallas_call(
        functools.partial(pack_kernel, z),
        out_shape=(rows_of(z.low_rows + z.edge_rows), rows_of(z.high_rows + z.edge_rows)),
        in_specs=[VMEM] * 4,
        out_specs=(VMEM, VMEM),
        name="pack",
    )(*flat)


def transport(z, *flat):
    span = z.rows + 2 * SUB
    return pl.pallas_call(
        functools.partial(transport_kernel, z),
        out_shape=rows_of(z.groups * z.species * z.blocks),
        in_specs=[VMEM] * 6,
        out_specs=VMEM,
        scratch_shapes=[
            pltpu.VMEM((6 * z.columns * span, LANES), jnp.float32),
        ]
        + [pltpu.VMEM((span * z.columns, LANES), jnp.float32)] * (3 * TOGETHER),
        name="transport",
    )(*flat)


def chemistry(species, blocks, *args):
    size = (species * blocks, LANES)
    return pl.pallas_call(
        functools.partial(chemistry_kernel, species, blocks),
        out_shape=rows_of(species * blocks),
        in_specs=[VMEM] * 4 + [SMEM] * 4,
        out_specs=VMEM,
        scratch_shapes=[pltpu.VMEM(size, jnp.float32)] * 6,
        name="chemistry",
    )(*args)


def body(
    mixing_ratio_field,
    eastward_face_cfl,
    northward_face_cfl,
    upward_face_cfl,
    thermal_anomaly,
    radiant_flux,
    daylight_mask,
    baseline_kinetic_coefficient,
    arrhenius_barrier,
    photodissociation_factor,
    stoichiometry_table,
):
    groups = lax.axis_size("tracer")
    strips = lax.axis_size("space")
    z = Sizes(mixing_ratio_field, groups)
    flat = [
        flat_rows(a)
        for a in (mixing_ratio_field, eastward_face_cfl, northward_face_cfl, upward_face_cfl)
    ]
    low, high = pack(z, *flat)
    low = lax.ppermute(low, "space", [(i, i + 1) for i in range(strips - 1)])
    high = lax.ppermute(high, "space", [(i + 1, i) for i in range(strips - 1)])
    moved = transport(z, *flat, low, high)
    moved = moved.reshape(groups, z.species * z.blocks, LANES)
    moved = lax.all_to_all(moved, "tracer", split_axis=0, concat_axis=0, tiled=True)
    species = z.species * groups
    lit = jnp.moveaxis(daylight_mask, 2, 1).reshape(z.blocks, 1)
    lit = jnp.broadcast_to(lit, (z.blocks, LANES))
    out = chemistry(
        species,
        z.blocks,
        moved.reshape(species * z.blocks, LANES),
        flat_rows(thermal_anomaly),
        flat_rows(radiant_flux),
        lit,
        baseline_kinetic_coefficient,
        arrhenius_barrier,
        photodissociation_factor,
        stoichiometry_table,
    )
    out = out.reshape(species, z.levels, z.tiles, z.part, LANES)
    return jnp.moveaxis(out, 2, 3).reshape(species, z.levels, z.part, z.width)


def solution(mesh):
    placed = (
        P("tracer", None, "space", None),
        P(None, "space", None),
        P(None, "space", None),
        P(None, "space", None),
        P(None, ("space", "tracer"), None),
        P(None, ("space", "tracer"), None),
        P(None, ("space", "tracer"), None),
        P(),
        P(),
        P(),
        P(),
    )
    return jax.shard_map(
        body,
        mesh=mesh,
        in_specs=placed,
        out_specs=P(None, None, ("space", "tracer"), None),
        check_vma=False,
    )
```

```python
import functools

import jax
import jax.numpy as jnp
from jax import lax
from jax.experimental import pallas as pl
from jax.experimental.pallas import tpu as pltpu
from jax.sharding import PartitionSpec as P

SECTIONS = 3
DAY_STEPS = 2
LANES = 128
SUB = 8
LOW = 2 * SECTIONS
HIGH = SECTIONS
TOGETHER = 2
CHUNK = 8


def flat_rows(cells):
    *lead, rows, width = cells.shape
    sub = min(rows, SUB)
    split = cells.reshape(*lead, rows // sub, sub, width // LANES, LANES)
    return jnp.moveaxis(split, -2, -3).reshape(-1, LANES)


class Sizes:
    def __init__(self, field, groups):
        self.species, self.levels, self.rows, self.width = field.shape
        self.tiles = self.width // LANES
        self.groups = groups
        self.part = self.rows // groups
        self.blocks = self.levels * self.tiles * self.part
        self.stride = self.levels * self.rows * self.tiles
        self.columns = self.levels * self.tiles
        self.low_rows = LOW * self.columns * self.species
        self.high_rows = HIGH * self.columns * self.species
        self.span = self.rows + 2 * SUB
        self.edge_rows = 3 * self.columns * SUB

    def source_row(self, level, row, tile):
        return ((level * (self.rows // SUB) + row // SUB) * self.tiles + tile) * SUB + row % SUB

    def pairs(self):
        return [(level, tile) for level in range(self.levels) for tile in range(self.tiles)]


def pack_kernel(z, x_ref, east_ref, north_ref, up_ref, low_ref, high_ref):
    def one_species(index, carry):
        for offset, rows, out_ref in ((z.rows - LOW, LOW, low_ref), (0, HIGH, high_ref)):
            for col, (level, tile) in enumerate(z.pairs()):
                source = index * z.stride + z.source_row(level, offset, tile)
                target = (index * z.columns + col) * rows
                out_ref[pl.ds(target, rows), :] = x_ref[pl.ds(source, rows), :]
        return carry

    lax.fori_loop(0, z.species, one_species, 0, unroll=4)
    for out_ref, base, last in ((low_ref, z.low_rows, True), (high_ref, z.high_rows, False)):
        row = z.rows - SUB if last else 0
        for kind, ref in enumerate((east_ref, north_ref, up_ref)):
            for col, (level, tile) in enumerate(z.pairs()):
                target = base + (kind * z.columns + col) * SUB
                source = z.source_row(level, row, tile)
                out_ref[pl.ds(target, SUB), :] = ref[pl.ds(source, SUB), :]


def middle(a, b):
    return jnp.maximum(jnp.minimum(a, b), jnp.minimum(jnp.maximum(a, b), 0.0))


def shift_columns(parts, amount):
    if amount > 0:
        return [pltpu.roll(parts[-1], 1, 1)] + parts[:-1]
    return parts[1:] + [pltpu.roll(parts[0], LANES - 1, 1)]


def spread_matrix(tiles, back):
    natural = lax.broadcasted_iota(jnp.int32, (tiles * LANES, tiles * LANES), 1 if back else 0)
    spread = lax.broadcasted_iota(jnp.int32, (tiles * LANES, tiles * LANES), 0 if back else 1)
    hit = natural == (spread % LANES) * tiles + spread // LANES
    return jnp.where(hit, 1.0, 0.0).astype(jnp.bfloat16)


def reorder(parts, matrix):
    x = jnp.concatenate(parts, axis=1)
    total = None
    for _ in range(3):
        piece = x.astype(jnp.bfloat16)
        x = x - piece.astype(jnp.float32)
        term = jnp.dot(piece, matrix, preferred_element_type=jnp.float32)
        total = term if total is None else total + term
    return [total[:, k * LANES : (k + 1) * LANES] for k in range(len(parts))]


def transport_kernel(
    z, x_ref, east_ref, north_ref, up_ref, low_ref, high_ref, out_ref, coef, natural, strip, final, *scratch
):
    span = z.span
    forth = spread_matrix(z.tiles, False)

    def coef_row(kind, which, col, j):
        return ((kind * 2 + which) * z.columns + col) * span + j

    for kind, ref in enumerate((east_ref, north_ref, up_ref)):
        for level in range(z.levels):
            parts = []
            for tile in range(z.tiles):
                edge = (kind * z.columns + level * z.tiles + tile) * SUB
                pieces = [low_ref[pl.ds(z.low_rows + edge, SUB), :]]
                for row in range(0, z.rows, SUB):
                    pieces.append(ref[pl.ds(z.source_row(level, row, tile), SUB), :])
                pieces.append(high_ref[pl.ds(z.high_rows + edge, SUB), :])
                parts.append(jnp.concatenate(pieces, axis=0))
            parts = reorder(parts, forth)
            if kind == 1:
                parts = shift_columns(parts, -1)
            for tile, value in enumerate(parts):
                col = level * z.tiles + tile
                coef[pl.ds(coef_row(kind, 0, col, 0), span), :] = value
                coef[pl.ds(coef_row(kind, 1, col, 0), span), :] = 0.5 * value * (1.0 - value)

    def weights(kind, col, j):
        return [coef[pl.ds(coef_row(kind, which, col, j), SUB), :] for which in range(2)]

    cols = range(z.columns)

    def gather(index, carry):
        for k in range(CHUNK):
            for col, (level, tile) in enumerate(z.pairs()):
                one = index * CHUNK + k
                base = one * z.columns + col
                at = (k * z.columns + col) * span + SUB
                natural[pl.ds(at - LOW, LOW), :] = low_ref[pl.ds(base * LOW, LOW), :]
                natural[pl.ds(at + z.rows, HIGH), :] = high_ref[pl.ds(base * HIGH, HIGH), :]
                for row in range(0, z.rows, SUB):
                    source = one * z.stride + z.source_row(level, row, tile)
                    natural[pl.ds(at + row, SUB), :] = x_ref[pl.ds(pl.multiple_of(source, SUB), SUB), :]
        count = CHUNK * z.levels
        whole = natural[...].reshape(count, z.tiles, span, LANES)
        parts = reorder([whole[:, t].reshape(count * span, LANES) for t in range(z.tiles)], forth)
        for one in range(count):
            for tile in range(z.tiles):
                at = ((index * count + one) * z.tiles + tile) * span
                strip[pl.ds(pl.multiple_of(at, SUB), span), :] = parts[tile][one * span : (one + 1) * span]
        return carry

    lax.fori_loop(0, z.species // CHUNK, gather, 0)

    def one_species(index, fields, fluxes):
        for step in range(SECTIONS):
            write = fields[step % 2]
            if step == 0:
                read = lambda col, j: strip[pl.ds((index * z.columns + col) * span + j, SUB), :]
            else:
                read = lambda col, j, ref=fields[(step + 1) % 2]: ref[pl.ds(col * span + j, SUB), :]
            bottom = SUB - LOW + 2 * (step + 1)
            top = SUB + z.rows + HIGH - (step + 1)
            for j in range(bottom - 1, top, SUB):
                for col in cols:
                    below, here, above = [read(col, j + k) for k in (-1, 0, 1)]
                    a, b = weights(0, col, j + 1)
                    fluxes[pl.ds(col * span + j, SUB), :] = a * here + b * middle(here - below, above - here)
            for j in range(bottom, top, SUB):
                c = []
                for col in cols:
                    leave = fluxes[pl.ds(col * span + j, SUB), :]
                    enter = fluxes[pl.ds(col * span + j - 1, SUB), :]
                    c.append(read(col, j) - (leave - enter))
                for level in range(z.levels):
                    mine = slice(level * z.tiles, (level + 1) * z.tiles)
                    row = c[mine]
                    back = [v - w for v, w in zip(row, shift_columns(row, 1))]
                    ahead = shift_columns(back, -1)
                    leave = []
                    for tile in range(z.tiles):
                        a, b = weights(1, level * z.tiles + tile, j)
                        leave.append(a * row[tile] + b * middle(back[tile], ahead[tile]))
                    enter = shift_columns(leave, 1)
                    c[mine] = [row[t] - (leave[t] - enter[t]) for t in range(z.tiles)]
                for tile in range(z.tiles):
                    column = [c[level * z.tiles + tile] for level in range(z.levels)]
                    steps = [column[0]]
                    steps += [column[k + 1] - column[k] for k in range(z.levels - 1)]
                    steps += [-column[-1]]
                    lift = None
                    for level in range(z.levels):
                        col = level * z.tiles + tile
                        a, b = weights(2, col, j)
                        rising = a * column[level] + b * middle(steps[level], steps[level + 1])
                        net = rising if lift is None else rising - lift
                        lift = rising
                        value = column[level] - net
                        if step < SECTIONS - 1:
                            write[pl.ds(col * span + j, SUB), :] = value
                        else:
                            base = (index * z.columns + col) * z.rows + j - SUB
                            final[pl.ds(pl.multiple_of(base, SUB), SUB), :] = value

    def some_species(index, carry):
        for k in range(TOGETHER):
            one_species(index * TOGETHER + k, scratch[3 * k : 3 * k + 2], scratch[3 * k + 2])
        return carry

    lax.fori_loop(0, z.species // TOGETHER, some_species, 0)

    back = spread_matrix(z.tiles, True)

    def scatter(index, carry):
        count = CHUNK * z.levels
        size = count * z.tiles * z.rows
        whole = final[pl.ds(pl.multiple_of(index * size, SUB), size), :].reshape(count, z.tiles, z.rows, LANES)
        parts = reorder([whole[:, t].reshape(count * z.rows, LANES) for t in range(z.tiles)], back)
        for one in range(count):
            k, level = divmod(one, z.levels)
            for tile in range(z.tiles):
                for group in range(z.groups):
                    start = one * z.rows + group * z.part
                    at = (group * z.species + index * CHUNK + k) * z.blocks + (level * z.tiles + tile) * z.part
                    out_ref[pl.ds(at, z.part), :] = parts[tile][start : start + z.part]
        return carry

    lax.fori_loop(0, z.species // CHUNK, scatter, 0)


def chemistry_kernel(
    species, blocks, c_ref, warm_ref, glow_ref, lit_ref, rate_ref, barrier_ref, photo_ref, table_ref,
    out_ref, made_a, made_b, lost_a, lost_b, lost_c, lost_d,
):
    pieces = blocks // SUB
    reactions = rate_ref.shape[0]
    made = (made_a, made_b)
    lost = ((lost_a, lost_b), (lost_c, lost_d))

    def cell(index, piece):
        return pl.ds(pl.multiple_of(index * blocks, SUB) + piece * SUB, SUB)

    lit = [lit_ref[pl.ds(piece * SUB, SUB), :] == 1 for piece in range(pieces)]
    warm = [warm_ref[pl.ds(piece * SUB, SUB), :] - 1.0 for piece in range(pieces)]
    glow = [jnp.where(lit[p], glow_ref[pl.ds(p * SUB, SUB), :], 0.0) for p in range(pieces)]

    for sub in range(DAY_STEPS):
        source = c_ref if sub == 0 else out_ref
        steps = [jnp.where(lit[p], float(DAY_STEPS), 1.0) for p in range(pieces)]

        def begin(s, carry):
            for p in range(pieces):
                made[0][cell(s, p), :] = steps[p] * source[cell(s, p), :]
                made[1][cell(s, p), :] = jnp.zeros((SUB, LANES), jnp.float32)
                for k in range(2):
                    for side in range(2):
                        fill = steps[p] if k == 0 and side == 0 else jnp.zeros((SUB, LANES), jnp.float32)
                        lost[k][side][cell(s, p), :] = fill
            return carry

        lax.fori_loop(0, species, begin, 0, unroll=4)

        def react(r, parity):
            first, second, product = table_ref[0, r], table_ref[1, r], table_ref[2, r]
            rate, barrier, photo = rate_ref[r], barrier_ref[r], photo_ref[r]
            for p in range(pieces):
                k = rate * jnp.exp(-barrier * warm[p]) + photo * glow[p]
                x = source[cell(first, p), :]
                y = source[cell(second, p), :]
                kx = k * x
                ky = k * y
                made[parity][cell(product, p), :] += kx * y
                lost[parity][0][cell(first, p), :] += ky
                lost[parity][1][cell(second, p), :] += kx

        def two(i, carry):
            react(2 * i, 0)
            react(2 * i + 1, 1)
            return carry

        lax.fori_loop(0, reactions // 2, two, 0, unroll=4)

        def finish(s, carry):
            for p in range(pieces):
                at = cell(s, p)
                top = made[0][at, :] + made[1][at, :]
                bottom = (lost[0][0][at, :] + lost[0][1][at, :]) + (lost[1][0][at, :] + lost[1][1][at, :])
                value = top / bottom
                if sub > 0:
                    value = jnp.where(lit[p], value, source[at, :])
                out_ref[at, :] = value
            return carry

        lax.fori_loop(0, species, finish, 0, unroll=4)


VMEM = pl.BlockSpec(memory_space=pltpu.VMEM)
SMEM = pl.BlockSpec(memory_space=pltpu.SMEM)


def rows_of(count):
    return jax.ShapeDtypeStruct((count, LANES), jnp.float32)


def pack(z, *flat):
    return pl.pallas_call(
        functools.partial(pack_kernel, z),
        out_shape=(rows_of(z.low_rows + z.edge_rows), rows_of(z.high_rows + z.edge_rows)),
        in_specs=[VMEM] * 4,
        out_specs=(VMEM, VMEM),
        compiler_params=pltpu.CompilerParams(vmem_limit_bytes=12 << 20),
        name="pack",
    )(*flat)


def transport(z, *flat):
    span = z.span
    return pl.pallas_call(
        functools.partial(transport_kernel, z),
        out_shape=rows_of(z.groups * z.species * z.blocks),
        in_specs=[VMEM] * 6,
        out_specs=VMEM,
        scratch_shapes=[
            pltpu.VMEM((6 * z.columns * span, LANES), jnp.float32),
            pltpu.VMEM((CHUNK * z.columns * span, LANES), jnp.float32),
            pltpu.VMEM((z.species * z.columns * span, LANES), jnp.float32),
            pltpu.VMEM((z.species * z.columns * z.rows, LANES), jnp.float32),
        ]
        + [pltpu.VMEM((span * z.columns, LANES), jnp.float32)] * (3 * TOGETHER),
        compiler_params=pltpu.CompilerParams(vmem_limit_bytes=32 << 20),
        name="transport",
    )(*flat)


def chemistry(species, blocks, *args):
    size = (species * blocks, LANES)
    return pl.pallas_call(
        functools.partial(chemistry_kernel, species, blocks),
        out_shape=rows_of(species * blocks),
        in_specs=[VMEM] * 4 + [SMEM] * 4,
        out_specs=VMEM,
        scratch_shapes=[pltpu.VMEM(size, jnp.float32)] * 6,
        compiler_params=pltpu.CompilerParams(vmem_limit_bytes=32 << 20),
        name="chemistry",
    )(*args)


def body(
    mixing_ratio_field,
    eastward_face_cfl,
    northward_face_cfl,
    upward_face_cfl,
    thermal_anomaly,
    radiant_flux,
    daylight_mask,
    baseline_kinetic_coefficient,
    arrhenius_barrier,
    photodissociation_factor,
    stoichiometry_table,
):
    groups = lax.axis_size("tracer")
    strips = lax.axis_size("space")
    z = Sizes(mixing_ratio_field, groups)
    flat = [
        flat_rows(a)
        for a in (mixing_ratio_field, eastward_face_cfl, northward_face_cfl, upward_face_cfl)
    ]
    low, high = pack(z, *flat)
    low = lax.ppermute(low, "space", [(i, i + 1) for i in range(strips - 1)])
    high = lax.ppermute(high, "space", [(i + 1, i) for i in range(strips - 1)])
    moved = transport(z, *flat, low, high)
    moved = moved.reshape(groups, z.species * z.blocks, LANES)
    moved = lax.all_to_all(moved, "tracer", split_axis=0, concat_axis=0, tiled=True)
    species = z.species * groups
    lit = jnp.moveaxis(daylight_mask, 2, 1).reshape(z.blocks, 1)
    lit = jnp.broadcast_to(lit, (z.blocks, LANES))
    out = chemistry(
        species,
        z.blocks,
        moved.reshape(species * z.blocks, LANES),
        flat_rows(thermal_anomaly),
        flat_rows(radiant_flux),
        lit,
        baseline_kinetic_coefficient,
        arrhenius_barrier,
        photodissociation_factor,
        stoichiometry_table,
    )
    out = out.reshape(species, z.levels, z.tiles, z.part, LANES)
    return jnp.moveaxis(out, 2, 3).reshape(species, z.levels, z.part, z.width)


def solution(mesh):
    placed = (
        P("tracer", None, "space", None),
        P(None, "space", None),
        P(None, "space", None),
        P(None, "space", None),
        P(None, ("space", "tracer"), None),
        P(None, ("space", "tracer"), None),
        P(None, ("space", "tracer"), None),
        P(),
        P(),
        P(),
        P(),
    )
    return jax.shard_map(
        body,
        mesh=mesh,
        in_specs=placed,
        out_specs=P(None, None, ("space", "tracer"), None),
        check_vma=False,
    )
```

```python
import functools

import jax
import jax.numpy as jnp
from jax import lax
from jax.experimental import pallas as pl
from jax.experimental.pallas import tpu as pltpu
from jax.sharding import PartitionSpec as P

SECTIONS = 3
DAY_STEPS = 2
LANES = 128
SUB = 8
LOW = 2 * SECTIONS
HIGH = SECTIONS
PARTS = 2
TOGETHER = 8
CHUNK = 8
LOG2E = 1.4426950408889634


def flat_rows(cells):
    *lead, rows, width = cells.shape
    sub = min(rows, SUB)
    split = cells.reshape(*lead, rows // sub, sub, width // LANES, LANES)
    return jnp.moveaxis(split, -2, -3).reshape(-1, LANES)


class Sizes:
    def __init__(self, field, groups):
        self.species, self.levels, self.rows, self.width = field.shape
        self.tiles = self.width // LANES
        self.groups = groups
        self.part = self.rows // groups
        self.blocks = self.levels * self.tiles * self.part
        self.stride = self.levels * self.rows * self.tiles
        self.columns = self.levels * self.tiles
        self.low_rows = LOW * self.columns * self.species
        self.high_rows = HIGH * self.columns * self.species
        self.span = self.rows + 2 * SUB
        self.edge_rows = 3 * self.columns * SUB

    def source_row(self, level, row, tile):
        return ((level * (self.rows // SUB) + row // SUB) * self.tiles + tile) * SUB + row % SUB

    def pairs(self):
        return [(level, tile) for level in range(self.levels) for tile in range(self.tiles)]


def pack_kernel(z, x_hbm, east_hbm, north_hbm, up_hbm, low_ref, high_ref, x_ref, east_ref, north_ref, up_ref, sems):
    pairs = ((x_hbm, x_ref), (east_hbm, east_ref), (north_hbm, north_ref), (up_hbm, up_ref))
    copies = [pltpu.make_async_copy(src, dst, sems.at[k]) for k, (src, dst) in enumerate(pairs)]
    for copy in copies:
        copy.start()
    for copy in copies[1:]:
        copy.wait()
    for out_ref, base, last in ((low_ref, z.low_rows, True), (high_ref, z.high_rows, False)):
        row = z.rows - SUB if last else 0
        for kind, ref in enumerate((east_ref, north_ref, up_ref)):
            for col, (level, tile) in enumerate(z.pairs()):
                target = base + (kind * z.columns + col) * SUB
                source = z.source_row(level, row, tile)
                out_ref[pl.ds(target, SUB), :] = ref[pl.ds(source, SUB), :]
    copies[0].wait()

    def one_species(index, carry):
        for offset, rows, out_ref in ((z.rows - LOW, LOW, low_ref), (0, HIGH, high_ref)):
            for col, (level, tile) in enumerate(z.pairs()):
                source = index * z.stride + z.source_row(level, offset, tile)
                target = (index * z.columns + col) * rows
                out_ref[pl.ds(target, rows), :] = x_ref[pl.ds(source, rows), :]
        return carry

    lax.fori_loop(0, z.species, one_species, 0, unroll=4)


def middle(a, b):
    return jnp.maximum(jnp.minimum(a, b), jnp.minimum(jnp.maximum(a, b), 0.0))


def shift_columns(parts, amount):
    if amount > 0:
        return [pltpu.roll(parts[-1], 1, 1)] + parts[:-1]
    return parts[1:] + [pltpu.roll(parts[0], LANES - 1, 1)]


def spread_matrix(tiles, back):
    natural = lax.broadcasted_iota(jnp.int32, (tiles * LANES, tiles * LANES), 1 if back else 0)
    spread = lax.broadcasted_iota(jnp.int32, (tiles * LANES, tiles * LANES), 0 if back else 1)
    hit = natural == (spread % LANES) * tiles + spread // LANES
    return jnp.where(hit, 1.0, 0.0).astype(jnp.bfloat16)


def reorder(parts, matrix):
    x = jnp.concatenate(parts, axis=1)
    total = None
    for _ in range(3):
        piece = x.astype(jnp.bfloat16)
        x = x - piece.astype(jnp.float32)
        term = jnp.dot(piece, matrix, preferred_element_type=jnp.float32)
        total = term if total is None else total + term
    return [total[:, k * LANES : (k + 1) * LANES] for k in range(len(parts))]


def transport_kernel(
    z, first, count, x_ref, east_ref, north_ref, up_ref, low_ref, high_ref, out_ref, coef, natural, strip, final, *scratch
):
    span = z.span
    forth = spread_matrix(z.tiles, False)

    def coef_row(kind, which, col, j):
        return ((kind * 2 + which) * z.columns + col) * span + j

    for kind, ref in enumerate((east_ref, north_ref, up_ref)):
        for level in range(z.levels):
            parts = []
            for tile in range(z.tiles):
                edge = (kind * z.columns + level * z.tiles + tile) * SUB
                pieces = [low_ref[pl.ds(z.low_rows + edge, SUB), :]]
                for row in range(0, z.rows, SUB):
                    pieces.append(ref[pl.ds(z.source_row(level, row, tile), SUB), :])
                pieces.append(high_ref[pl.ds(z.high_rows + edge, SUB), :])
                parts.append(jnp.concatenate(pieces, axis=0))
            parts = reorder(parts, forth)
            if kind == 1:
                parts = shift_columns(parts, -1)
            for tile, value in enumerate(parts):
                col = level * z.tiles + tile
                coef[pl.ds(coef_row(kind, 0, col, 0), span), :] = value
                coef[pl.ds(coef_row(kind, 1, col, 0), span), :] = 0.5 * value * (1.0 - value)

    def weights(kind, col, j):
        return [coef[pl.ds(coef_row(kind, which, col, j), SUB), :] for which in range(2)]

    cols = range(z.columns)

    def gather(index, carry):
        for k in range(CHUNK):
            for col, (level, tile) in enumerate(z.pairs()):
                one = first + index * CHUNK + k
                base = one * z.columns + col
                at = (k * z.columns + col) * span + SUB
                natural[pl.ds(at - LOW, LOW), :] = low_ref[pl.ds(base * LOW, LOW), :]
                natural[pl.ds(at + z.rows, HIGH), :] = high_ref[pl.ds(base * HIGH, HIGH), :]
                for row in range(0, z.rows, SUB):
                    source = one * z.stride + z.source_row(level, row, tile)
                    natural[pl.ds(at + row, SUB), :] = x_ref[pl.ds(pl.multiple_of(source, SUB), SUB), :]
        many = CHUNK * z.levels
        whole = natural[...].reshape(many, z.tiles, span, LANES)
        parts = reorder([whole[:, t].reshape(many * span, LANES) for t in range(z.tiles)], forth)
        for one in range(many):
            for tile in range(z.tiles):
                at = ((index * many + one) * z.tiles + tile) * span
                strip[pl.ds(pl.multiple_of(at, SUB), span), :] = parts[tile][one * span : (one + 1) * span]
        return carry

    lax.fori_loop(0, count // CHUNK, gather, 0)

    def one_species(index, fields, fluxes):
        for step in range(SECTIONS):
            write = fields[step % 2]
            if step == 0:
                read = lambda col, j: strip[pl.ds((index * z.columns + col) * span + j, SUB), :]
            else:
                read = lambda col, j, ref=fields[(step + 1) % 2]: ref[pl.ds(col * span + j, SUB), :]
            bottom = SUB - LOW + 2 * (step + 1)
            top = SUB + z.rows + HIGH - (step + 1)
            for j in range(bottom - 1, top, SUB):
                for col in cols:
                    below, here, above = [read(col, j + k) for k in (-1, 0, 1)]
                    a, b = weights(0, col, j + 1)
                    fluxes[pl.ds(col * span + j, SUB), :] = a * here + b * middle(here - below, above - here)
            for j in range(bottom, top, SUB):
                c = []
                for col in cols:
                    leave = fluxes[pl.ds(col * span + j, SUB), :]
                    enter = fluxes[pl.ds(col * span + j - 1, SUB), :]
                    c.append(read(col, j) - (leave - enter))
                for level in range(z.levels):
                    mine = slice(level * z.tiles, (level + 1) * z.tiles)
                    row = c[mine]
                    back = [v - w for v, w in zip(row, shift_columns(row, 1))]
                    ahead = shift_columns(back, -1)
                    leave = []
                    for tile in range(z.tiles):
                        a, b = weights(1, level * z.tiles + tile, j)
                        leave.append(a * row[tile] + b * middle(back[tile], ahead[tile]))
                    enter = shift_columns(leave, 1)
                    c[mine] = [row[t] - (leave[t] - enter[t]) for t in range(z.tiles)]
                for tile in range(z.tiles):
                    column = [c[level * z.tiles + tile] for level in range(z.levels)]
                    steps = [column[0]]
                    steps += [column[k + 1] - column[k] for k in range(z.levels - 1)]
                    steps += [-column[-1]]
                    lift = None
                    for level in range(z.levels):
                        col = level * z.tiles + tile
                        a, b = weights(2, col, j)
                        rising = a * column[level] + b * middle(steps[level], steps[level + 1])
                        net = rising if lift is None else rising - lift
                        lift = rising
                        value = column[level] - net
                        if step < SECTIONS - 1:
                            write[pl.ds(col * span + j, SUB), :] = value
                        else:
                            base = (index * z.columns + col) * z.rows + j - SUB
                            final[pl.ds(pl.multiple_of(base, SUB), SUB), :] = value

    def some_species(index, carry):
        for k in range(TOGETHER):
            one_species(index * TOGETHER + k, scratch[3 * k : 3 * k + 2], scratch[3 * k + 2])
        return carry

    lax.fori_loop(0, count // TOGETHER, some_species, 0)

    back = spread_matrix(z.tiles, True)

    def scatter(index, carry):
        many = CHUNK * z.levels
        size = many * z.tiles * z.rows
        whole = final[pl.ds(pl.multiple_of(index * size, SUB), size), :].reshape(many, z.tiles, z.rows, LANES)
        parts = reorder([whole[:, t].reshape(many * z.rows, LANES) for t in range(z.tiles)], back)
        for one in range(many):
            k, level = divmod(one, z.levels)
            for tile in range(z.tiles):
                for group in range(z.groups):
                    start = one * z.rows + group * z.part
                    at = (group * count + index * CHUNK + k) * z.blocks + (level * z.tiles + tile) * z.part
                    out_ref[pl.ds(at, z.part), :] = parts[tile][start : start + z.part]
        return carry

    lax.fori_loop(0, count // CHUNK, scatter, 0)


def rates_kernel(pieces, after_ref, warm_ref, glow_ref, lit_ref, rate_ref, barrier_ref, photo_ref, out_ref):
    warm = [(1.0 - warm_ref[pl.ds(p * SUB, SUB), :]) * LOG2E for p in range(pieces)]
    glow = [
        jnp.where(lit_ref[pl.ds(p * SUB, SUB), :] == 1, glow_ref[pl.ds(p * SUB, SUB), :], 0.0)
        for p in range(pieces)
    ]

    def one(r, carry):
        for p in range(pieces):
            at = pl.ds(pl.multiple_of(r * pieces * SUB, SUB) + p * SUB, SUB)
            out_ref[at, :] = rate_ref[r] * jnp.exp2(barrier_ref[r] * warm[p]) + photo_ref[r] * glow[p]
        return carry

    lax.fori_loop(0, rate_ref.shape[0], one, 0, unroll=8)


def chemistry_kernel(z, species, *refs):
    pieces = z.blocks // SUB
    parts, (lit_ref, k_ref, table_ref, out_ref, state, made, lost_a, lost_b) = refs[:PARTS], refs[PARTS:]
    reactions = k_ref.shape[0] // z.blocks

    def cell(row, piece):
        return pl.ds(pl.multiple_of(row, SUB) + piece * SUB, SUB)

    lit = [lit_ref[pl.ds(p * SUB, SUB), :] == 1 for p in range(pieces)]
    steps = [jnp.where(lit[p], float(DAY_STEPS), 1.0) for p in range(pieces)]
    zero = jnp.zeros((SUB, LANES), jnp.float32)

    def prepare(at, p, value):
        made[at, :] = steps[p] * value
        lost_a[at, :] = steps[p]
        lost_b[at, :] = zero

    count = z.species // PARTS

    def begin(index, carry):
        for part, ref in enumerate(parts):
            for group in range(z.groups):
                for p in range(pieces):
                    value = ref[cell((group * count + index) * z.blocks, p), :]
                    at = cell((group * z.species + part * count + index) * z.blocks, p)
                    state[at, :] = value
                    prepare(at, p, value)
        return carry

    lax.fori_loop(0, count, begin, 0)

    def react(r, carry):
        first, second, product = table_ref[r], table_ref[reactions + r], table_ref[2 * reactions + r]
        for p in range(pieces):
            k = k_ref[cell(r * z.blocks, p), :]
            x = state[cell(first, p), :]
            y = state[cell(second, p), :]
            kx = k * x
            ky = k * y
            made[cell(product, p), :] += kx * y
            lost_a[cell(first, p), :] += ky
            lost_b[cell(second, p), :] += kx
        return carry

    for sub in range(DAY_STEPS):
        lax.fori_loop(0, reactions, react, 0, unroll=16)

        def finish(s, carry):
            for p in range(pieces):
                at = cell(s * z.blocks, p)
                value = made[at, :] / (lost_a[at, :] + lost_b[at, :])
                if sub < DAY_STEPS - 1:
                    prepare(at, p, value)
                    if sub == 0:
                        state[at, :] = value
                if sub > 0:
                    value = jnp.where(lit[p], value, state[at, :])
                    out_ref[at, :] = value
            return carry

        lax.fori_loop(0, species, finish, 0, unroll=4)


VMEM = pl.BlockSpec(memory_space=pltpu.VMEM)
SMEM = pl.BlockSpec(memory_space=pltpu.SMEM)


def rows_of(count):
    return jax.ShapeDtypeStruct((count, LANES), jnp.float32)


ANY = pl.BlockSpec(memory_space=pl.ANY)
HBM = pl.BlockSpec(memory_space=pltpu.HBM)


def pack(z, *flat):
    return pl.pallas_call(
        functools.partial(pack_kernel, z),
        out_shape=(rows_of(z.low_rows + z.edge_rows), rows_of(z.high_rows + z.edge_rows)),
        in_specs=[HBM] * 4,
        out_specs=(VMEM, VMEM),
        scratch_shapes=[pltpu.VMEM(a.shape, jnp.float32) for a in flat] + [pltpu.SemaphoreType.DMA((4,))],
        compiler_params=pltpu.CompilerParams(vmem_limit_bytes=12 << 20),
        name="pack",
    )(*flat)


def transport(z, part, *flat):
    count = z.species // PARTS
    return pl.pallas_call(
        functools.partial(transport_kernel, z, part * count, count),
        out_shape=rows_of(z.groups * count * z.blocks),
        in_specs=[VMEM] * 6,
        out_specs=VMEM,
        scratch_shapes=[
            pltpu.VMEM((6 * z.columns * z.span, LANES), jnp.float32),
            pltpu.VMEM((CHUNK * z.columns * z.span, LANES), jnp.float32),
            pltpu.VMEM((count * z.columns * z.span, LANES), jnp.float32),
            pltpu.VMEM((count * z.columns * z.rows, LANES), jnp.float32),
        ]
        + [pltpu.VMEM((z.span * z.columns, LANES), jnp.float32)] * (3 * TOGETHER),
        compiler_params=pltpu.CompilerParams(vmem_limit_bytes=24 << 20),
        cost_estimate=pl.CostEstimate(flops=400 * count * z.stride * LANES, bytes_accessed=0, transcendentals=0),
        name="transport",
    )(*flat)


def rates(z, after, warm, glow, lit, rate, barrier, photo):
    reactions = rate.shape[0]
    return pl.pallas_call(
        functools.partial(rates_kernel, z.blocks // SUB),
        out_shape=rows_of(reactions * z.blocks),
        in_specs=[ANY] + [VMEM] * 3 + [SMEM] * 3,
        out_specs=VMEM,
        compiler_params=pltpu.CompilerParams(vmem_limit_bytes=16 << 20),
        cost_estimate=pl.CostEstimate(
            flops=40 * reactions * z.blocks * LANES, bytes_accessed=0, transcendentals=0
        ),
        name="rates",
    )(after, warm, glow, lit, rate, barrier, photo)


def chemistry(z, species, *args):
    size = (species * z.blocks, LANES)
    return pl.pallas_call(
        functools.partial(chemistry_kernel, z, species),
        out_shape=rows_of(species * z.blocks),
        in_specs=[VMEM] * (PARTS + 2) + [SMEM],
        out_specs=VMEM,
        scratch_shapes=[pltpu.VMEM(size, jnp.float32)] * 4,
        compiler_params=pltpu.CompilerParams(vmem_limit_bytes=24 << 20),
        name="chemistry",
    )(*args)


def body(
    mixing_ratio_field,
    eastward_face_cfl,
    northward_face_cfl,
    upward_face_cfl,
    thermal_anomaly,
    radiant_flux,
    daylight_mask,
    baseline_kinetic_coefficient,
    arrhenius_barrier,
    photodissociation_factor,
    stoichiometry_table,
):
    groups = lax.axis_size("tracer")
    strips = lax.axis_size("space")
    z = Sizes(mixing_ratio_field, groups)
    flat = [
        flat_rows(a)
        for a in (mixing_ratio_field, eastward_face_cfl, northward_face_cfl, upward_face_cfl)
    ]
    low, high = pack(z, *flat)
    low = lax.ppermute(low, "space", [(i, i + 1) for i in range(strips - 1)])
    high = lax.ppermute(high, "space", [(i + 1, i) for i in range(strips - 1)])
    species = z.species * groups
    count = z.species // PARTS
    arrived = []
    for part in range(PARTS):
        moved = transport(z, part, *flat, low, high)
        regrouped = lax.all_to_all(
            moved.reshape(groups, count * z.blocks, LANES), "tracer", split_axis=0, concat_axis=0, tiled=True
        )
        arrived.append(regrouped.reshape(species // PARTS * z.blocks, LANES))
    lit = jnp.moveaxis(daylight_mask, 2, 1).reshape(z.blocks, 1)
    lit = jnp.broadcast_to(lit, (z.blocks, LANES))
    table, lit, _ = lax.optimization_barrier((stoichiometry_table, lit, moved))
    k = rates(
        z,
        moved,
        flat_rows(thermal_anomaly),
        flat_rows(radiant_flux),
        lit,
        baseline_kinetic_coefficient,
        arrhenius_barrier,
        photodissociation_factor,
    )
    out = chemistry(z, species, *arrived, lit, k, table.reshape(-1) * z.blocks)
    out = out.reshape(species, z.levels, z.tiles, z.part, LANES)
    return jnp.moveaxis(out, 2, 3).reshape(species, z.levels, z.part, z.width)


def solution(mesh):
    placed = (
        P("tracer", None, "space", None),
        P(None, "space", None),
        P(None, "space", None),
        P(None, "space", None),
        P(None, ("space", "tracer"), None),
        P(None, ("space", "tracer"), None),
        P(None, ("space", "tracer"), None),
        P(),
        P(),
        P(),
        P(),
    )
    return jax.shard_map(
        body,
        mesh=mesh,
        in_specs=placed,
        out_specs=P(None, None, ("space", "tracer"), None),
        check_vma=False,
    )
```

```python
import functools

import jax
import jax.numpy as jnp
from jax import lax
from jax.experimental import pallas as pl
from jax.experimental.pallas import tpu as pltpu
from jax.sharding import PartitionSpec as P


SECTIONS = 3
DAY_STEPS = 2
LANES = 128
SUB = 8
LOW = 2 * SECTIONS
HIGH = SECTIONS
PARTS = 2
TOGETHER = 8
CHUNK = 8
BATCHES = 4
LOG2E = 1.4426950408889634


def flat_rows(cells):
    *lead, rows, width = cells.shape
    sub = min(rows, SUB)
    split = cells.reshape(*lead, rows // sub, sub, width // LANES, LANES)
    return jnp.moveaxis(split, -2, -3).reshape(-1, LANES)


class Sizes:
    def __init__(self, field, groups):
        self.species, self.levels, self.rows, self.width = field.shape
        self.tiles = self.width // LANES
        self.groups = groups
        self.part = self.rows // groups
        self.blocks = self.levels * self.tiles * self.part
        self.stride = self.levels * self.rows * self.tiles
        self.columns = self.levels * self.tiles
        self.count = self.species // PARTS
        self.low_rows = LOW * self.columns * self.species
        self.high_rows = HIGH * self.columns * self.species
        self.span = self.rows + 2 * SUB
        self.edge_rows = 3 * self.columns * SUB

    def source_row(self, level, row, tile):
        return ((level * (self.rows // SUB) + row // SUB) * self.tiles + tile) * SUB + row % SUB

    def pairs(self):
        return [(level, tile) for level in range(self.levels) for tile in range(self.tiles)]


def middle(a, b):
    return jnp.maximum(jnp.minimum(a, b), jnp.minimum(jnp.maximum(a, b), 0.0))


def shift_columns(parts, amount):
    if amount > 0:
        return [pltpu.roll(parts[-1], 1, 1)] + parts[:-1]
    return parts[1:] + [pltpu.roll(parts[0], LANES - 1, 1)]


def spread_matrix(tiles, back):
    natural = lax.broadcasted_iota(jnp.int32, (tiles * LANES, tiles * LANES), 1 if back else 0)
    spread = lax.broadcasted_iota(jnp.int32, (tiles * LANES, tiles * LANES), 0 if back else 1)
    hit = natural == (spread % LANES) * tiles + spread // LANES
    return jnp.where(hit, 1.0, 0.0).astype(jnp.bfloat16)


def reorder(parts, matrix):
    x = jnp.concatenate(parts, axis=1)
    total = None
    for _ in range(3):
        piece = x.astype(jnp.bfloat16)
        x = x - piece.astype(jnp.float32)
        term = jnp.dot(piece, matrix, preferred_element_type=jnp.float32)
        total = term if total is None else total + term
    return [total[:, k * LANES : (k + 1) * LANES] for k in range(len(parts))]


def pack_kernel(z, x_ref, courant_ref, low_ref, high_ref, courant_out, *fields):
    forth = spread_matrix(z.tiles, False)

    def spread(flat, strips):
        split = flat.reshape(strips, z.rows // SUB, z.tiles, SUB, LANES)
        return reorder([split[:, :, t].reshape(strips * z.rows, LANES) for t in range(z.tiles)], forth)

    parts = spread(courant_ref[...], 3 * z.levels)
    shifted = shift_columns(parts, -1)
    for strip in range(3 * z.levels):
        rows = slice(strip * z.rows, (strip + 1) * z.rows)
        for tile in range(z.tiles):
            value = (shifted if strip // z.levels == 1 else parts)[tile][rows]
            col = strip * z.tiles + tile
            courant_out[pl.ds(col * z.rows, z.rows), :] = value
            low_ref[pl.ds(z.low_rows + col * SUB, SUB), :] = value[z.rows - SUB :]
            high_ref[pl.ds(z.high_rows + col * SUB, SUB), :] = value[:SUB]

    for part, field in enumerate(fields):

        def some(index, carry):
            strips = CHUNK * z.levels
            size = strips * z.tiles * z.rows
            start = pl.multiple_of((part * (z.count // CHUNK) + index) * size, SUB)
            values = spread(x_ref[pl.ds(start, size), :], strips)
            for strip in range(strips):
                for tile in range(z.tiles):
                    at = pl.multiple_of(index * size + (strip * z.tiles + tile) * z.rows, SUB)
                    field[pl.ds(at, z.rows), :] = values[tile][strip * z.rows : (strip + 1) * z.rows]
            return carry

        lax.fori_loop(0, z.count // CHUNK, some, 0)

        def edges(index, carry):
            for col in range(z.columns):
                source = (index * z.columns + col) * z.rows
                target = (part * z.count + index) * z.columns + col
                low_ref[pl.ds(target * LOW, LOW), :] = field[pl.ds(source + z.rows - LOW, LOW), :]
                high_ref[pl.ds(target * HIGH, HIGH), :] = field[pl.ds(source, HIGH), :]
            return carry

        lax.fori_loop(0, z.count, edges, 0, unroll=4)


def transport_kernel(z, part, field_in, courant_in, low_in, high_in, out_ref, coef, final, *scratch):
    span = z.span
    cols = range(z.columns)
    slots, scratch = scratch[: 4 * TOGETHER], scratch[4 * TOGETHER :]
    if part == 0:
        field_ref, courant_ref, low_ref, high_ref = field_in, courant_in, low_in, high_in
        low_edge, high_edge = low_in.at[pl.ds(z.low_rows, z.edge_rows)], high_in.at[pl.ds(z.high_rows, z.edge_rows)]
    else:
        field_ref, courant_ref, low_ref, high_ref, low_edge, high_edge, sems = scratch
        fixed = [
            pltpu.make_async_copy(courant_in, courant_ref, sems.at[0, 0]),
            pltpu.make_async_copy(low_in.at[pl.ds(z.low_rows, z.edge_rows)], low_edge, sems.at[0, 1]),
            pltpu.make_async_copy(high_in.at[pl.ds(z.high_rows, z.edge_rows)], high_edge, sems.at[0, 2]),
        ]

        def pieces(index):
            result = []
            for k, (source, target, rows, first) in enumerate(
                (
                    (field_in, field_ref, z.rows, 0),
                    (low_in, low_ref, LOW, part * z.count),
                    (high_in, high_ref, HIGH, part * z.count),
                )
            ):
                size = TOGETHER * z.columns * rows
                here = pl.ds(pl.multiple_of(index * size, SUB), size)
                there = pl.ds(pl.multiple_of(index * size + first * z.columns * rows, SUB), size)
                result.append(pltpu.make_async_copy(source.at[there], target.at[here], sems.at[index + 1, k]))
            return result

        for copy in fixed:
            copy.start()
        for index in range(z.count // TOGETHER):
            for copy in pieces(index):
                copy.start()
        for copy in fixed:
            copy.wait()

    def coef_row(kind, which, col, j):
        return ((kind * 2 + which) * z.columns + col) * span + j

    for kind in range(3):
        for col in cols:
            one = kind * z.columns + col
            tiles = [low_edge[pl.ds(one * SUB, SUB), :]]
            tiles += [courant_ref[pl.ds(one * z.rows + row, SUB), :] for row in range(0, z.rows, SUB)]
            tiles += [high_edge[pl.ds(one * SUB, SUB), :]]
            for k, value in enumerate(tiles):
                coef[pl.ds(coef_row(kind, 0, col, k * SUB), SUB), :] = value
                coef[pl.ds(coef_row(kind, 1, col, k * SUB), SUB), :] = 0.5 * value * (1.0 - value)

    def weights(kind, col, j):
        return [coef[pl.ds(coef_row(kind, which, col, j), SUB), :] for which in range(2)]

    def one_species(index, start, fields, fluxes):
        for col in cols:
            base = index * z.columns + col
            at = col * span + SUB
            start[pl.ds(at - LOW, LOW), :] = low_ref[pl.ds(base * LOW, LOW), :]
            start[pl.ds(at + z.rows, HIGH), :] = high_ref[pl.ds(base * HIGH, HIGH), :]
            start[pl.ds(at, z.rows), :] = field_ref[pl.ds(pl.multiple_of(base * z.rows, SUB), z.rows), :]
        for step in range(SECTIONS):
            write = fields[step % 2]
            source = start if step == 0 else fields[(step + 1) % 2]
            read = lambda col, j, ref=source: ref[pl.ds(col * span + j, SUB), :]
            bottom = SUB - LOW + 2 * (step + 1)
            top = SUB + z.rows + HIGH - (step + 1)
            for j in range(bottom - 1, top, SUB):
                for col in cols:
                    below, here, above = [read(col, j + k) for k in (-1, 0, 1)]
                    a, b = weights(0, col, j + 1)
                    fluxes[pl.ds(col * span + j, SUB), :] = a * here + b * middle(here - below, above - here)
            for j in range(bottom, top, SUB):
                c = []
                for col in cols:
                    leave = fluxes[pl.ds(col * span + j, SUB), :]
                    enter = fluxes[pl.ds(col * span + j - 1, SUB), :]
                    c.append(read(col, j) - (leave - enter))
                for level in range(z.levels):
                    mine = slice(level * z.tiles, (level + 1) * z.tiles)
                    row = c[mine]
                    back = [v - w for v, w in zip(row, shift_columns(row, 1))]
                    ahead = shift_columns(back, -1)
                    leave = []
                    for tile in range(z.tiles):
                        a, b = weights(1, level * z.tiles + tile, j)
                        leave.append(a * row[tile] + b * middle(back[tile], ahead[tile]))
                    enter = shift_columns(leave, 1)
                    c[mine] = [row[t] - (leave[t] - enter[t]) for t in range(z.tiles)]
                for tile in range(z.tiles):
                    column = [c[level * z.tiles + tile] for level in range(z.levels)]
                    steps = [column[0]]
                    steps += [column[k + 1] - column[k] for k in range(z.levels - 1)]
                    steps += [-column[-1]]
                    lift = None
                    for level in range(z.levels):
                        col = level * z.tiles + tile
                        a, b = weights(2, col, j)
                        rising = a * column[level] + b * middle(steps[level], steps[level + 1])
                        net = rising if lift is None else rising - lift
                        lift = rising
                        value = column[level] - net
                        if step < SECTIONS - 1:
                            write[pl.ds(col * span + j, SUB), :] = value
                        else:
                            base = (index * z.columns + col) * z.rows + j - SUB
                            final[pl.ds(pl.multiple_of(base, SUB), SUB), :] = value

    def some_species(index, carry):
        if part > 0:
            for copy in pieces(index):
                copy.wait()
        for k in range(TOGETHER):
            one_species(index * TOGETHER + k, slots[4 * k], slots[4 * k + 1 : 4 * k + 3], slots[4 * k + 3])
        return carry

    lax.fori_loop(0, z.count // TOGETHER, some_species, 0)

    back = spread_matrix(z.tiles, True)

    def scatter(index, carry):
        many = CHUNK * z.levels
        size = many * z.tiles * z.rows
        whole = final[pl.ds(pl.multiple_of(index * size, SUB), size), :].reshape(many, z.tiles, z.rows, LANES)
        parts = reorder([whole[:, t].reshape(many * z.rows, LANES) for t in range(z.tiles)], back)
        for one in range(many):
            k, level = divmod(one, z.levels)
            for tile in range(z.tiles):
                for group in range(z.groups):
                    start = one * z.rows + group * z.part
                    at = (group * z.count + index * CHUNK + k) * z.blocks + (level * z.tiles + tile) * z.part
                    out_ref[pl.ds(at, z.part), :] = parts[tile][start : start + z.part]
        return carry

    lax.fori_loop(0, z.count // CHUNK, scatter, 0)


def rates_kernel(pieces, after_ref, warm_ref, glow_ref, lit_ref, rate_ref, barrier_ref, photo_ref, out_ref):
    step = pl.program_id(0)
    many = out_ref.shape[0] // (pieces * SUB)
    warm = [(1.0 - warm_ref[pl.ds(p * SUB, SUB), :]) * LOG2E for p in range(pieces)]
    glow = [
        jnp.where(lit_ref[pl.ds(p * SUB, SUB), :] == 1, glow_ref[pl.ds(p * SUB, SUB), :], 0.0)
        for p in range(pieces)
    ]

    def one(i, carry):
        r = step * many + i
        for p in range(pieces):
            at = pl.ds(pl.multiple_of(i * pieces * SUB, SUB) + p * SUB, SUB)
            out_ref[at, :] = rate_ref[r] * jnp.exp2(barrier_ref[r] * warm[p]) + photo_ref[r] * glow[p]
        return carry

    lax.fori_loop(0, many, one, 0, unroll=8)


def chemistry_kernel(z, species, *refs):
    pieces = z.blocks // SUB
    sources, (lit_ref, k_hbm, table_ref, out_ref) = refs[:PARTS], refs[PARTS : PARTS + 4]
    parts, (k_ref, state, made, lost_a, lost_b, sems) = refs[PARTS + 4 : 2 * PARTS + 4], refs[2 * PARTS + 4 :]
    reactions = k_ref.shape[0] // z.blocks
    batch = reactions // BATCHES
    loads = [pltpu.make_async_copy(a, b, sems.at[i]) for i, (a, b) in enumerate(zip(sources, parts))]
    for i in range(BATCHES):
        at = pl.ds(i * batch * z.blocks, batch * z.blocks)
        loads.append(pltpu.make_async_copy(k_hbm.at[at], k_ref.at[at], sems.at[PARTS + i]))
    for load in loads:
        load.start()

    def cell(row, piece):
        return pl.ds(pl.multiple_of(row, SUB) + piece * SUB, SUB)

    lit = [lit_ref[pl.ds(p * SUB, SUB), :] == 1 for p in range(pieces)]
    steps = [jnp.where(lit[p], float(DAY_STEPS), 1.0) for p in range(pieces)]
    zero = jnp.zeros((SUB, LANES), jnp.float32)

    def prepare(at, p, value):
        made[at, :] = steps[p] * value
        lost_a[at, :] = steps[p]
        lost_b[at, :] = zero

    for part, ref in enumerate(parts):
        loads[part].wait()

        def begin(index, carry):
            for group in range(z.groups):
                for p in range(pieces):
                    value = ref[cell((group * z.count + index) * z.blocks, p), :]
                    at = cell((group * z.species + part * z.count + index) * z.blocks, p)
                    state[at, :] = value
                    prepare(at, p, value)
            return carry

        lax.fori_loop(0, z.count, begin, 0)

    def react(r, carry):
        first, second, product = table_ref[r], table_ref[reactions + r], table_ref[2 * reactions + r]
        for p in range(pieces):
            k = k_ref[cell(r * z.blocks, p), :]
            x = state[cell(first, p), :]
            y = state[cell(second, p), :]
            kx = k * x
            ky = k * y
            made[cell(product, p), :] += kx * y
            lost_a[cell(first, p), :] += ky
            lost_b[cell(second, p), :] += kx
        return carry

    for sub in range(DAY_STEPS):
        if sub == 0:
            for i in range(BATCHES):
                loads[PARTS + i].wait()
                lax.fori_loop(i * batch, (i + 1) * batch, react, 0, unroll=16)
        else:
            lax.fori_loop(0, reactions, react, 0, unroll=16)

        def finish(s, carry):
            for p in range(pieces):
                at = cell(s * z.blocks, p)
                value = made[at, :] / (lost_a[at, :] + lost_b[at, :])
                if sub < DAY_STEPS - 1:
                    prepare(at, p, value)
                    if sub == 0:
                        state[at, :] = value
                if sub > 0:
                    value = jnp.where(lit[p], value, state[at, :])
                    out_ref[at, :] = value
            return carry

        lax.fori_loop(0, species, finish, 0, unroll=4)


VMEM = pl.BlockSpec(memory_space=pltpu.VMEM)
SMEM = pl.BlockSpec(memory_space=pltpu.SMEM)


def rows_of(count):
    return jax.ShapeDtypeStruct((count, LANES), jnp.float32)


ANY = pl.BlockSpec(memory_space=pl.ANY)
HBM = pl.BlockSpec(memory_space=pltpu.HBM)


def pack(z, *flat):
    part = rows_of(z.count * z.columns * z.rows)
    return pl.pallas_call(
        functools.partial(pack_kernel, z),
        out_shape=(
            rows_of(z.low_rows + z.edge_rows),
            rows_of(z.high_rows + z.edge_rows),
            rows_of(3 * z.columns * z.rows),
        )
        + (part,) * PARTS,
        in_specs=[VMEM] * 2,
        out_specs=(VMEM,) * (3 + PARTS),
        compiler_params=pltpu.CompilerParams(vmem_limit_bytes=16 << 20),
        name="pack",
    )(*flat)


def transport(z, part, *flat):
    rows = [z.count * z.columns * k for k in (z.rows, LOW, HIGH)]
    size = z.span * z.columns
    scratch = [6 * size, z.count * z.columns * z.rows] + [size] * (4 * TOGETHER)
    params = {}
    if part == 0:
        params["vmem_limit_bytes"] = 24 << 20
    else:
        scratch += [rows[0], 3 * z.columns * z.rows, rows[1], rows[2], z.edge_rows, z.edge_rows]
    scratch = [pltpu.VMEM((n, LANES), jnp.float32) for n in scratch]
    if part > 0:
        scratch += [pltpu.SemaphoreType.DMA((z.count // TOGETHER + 1, 3))]
    return pl.pallas_call(
        functools.partial(transport_kernel, z, part),
        out_shape=rows_of(z.groups * z.count * z.blocks),
        in_specs=[VMEM if part == 0 else ANY] * 4,
        out_specs=VMEM,
        scratch_shapes=scratch,
        compiler_params=pltpu.CompilerParams(**params),
        cost_estimate=pl.CostEstimate(flops=400 * z.count * z.stride * LANES, bytes_accessed=0, transcendentals=0),
        name="transport",
    )(*flat)


def rates(z, after, warm, glow, lit, rate, barrier, photo):
    reactions = rate.shape[0]
    whole = lambda i: (0, 0)
    cells = pl.BlockSpec((z.blocks, LANES), whole)
    return pl.pallas_call(
        functools.partial(rates_kernel, z.blocks // SUB),
        out_shape=rows_of(reactions * z.blocks),
        grid=(BATCHES,),
        in_specs=[ANY] + [cells] * 3 + [SMEM] * 3,
        out_specs=pl.BlockSpec((reactions // BATCHES * z.blocks, LANES), lambda i: (i, 0)),
        cost_estimate=pl.CostEstimate(
            flops=40 * reactions * z.blocks * LANES, bytes_accessed=0, transcendentals=0
        ),
        name="rates",
    )(after, warm, glow, lit, rate, barrier, photo)


def chemistry(z, species, k, *args):
    size = species * z.blocks
    scratch = [size // PARTS] * PARTS + [k.shape[0]] + [size] * 4
    scratch = [pltpu.VMEM((n, LANES), jnp.float32) for n in scratch]
    parts, (lit, table) = args[:PARTS], args[PARTS:]
    return pl.pallas_call(
        functools.partial(chemistry_kernel, z, species),
        out_shape=rows_of(size),
        in_specs=[ANY] * PARTS + [VMEM, ANY, SMEM],
        out_specs=VMEM,
        scratch_shapes=scratch + [pltpu.SemaphoreType.DMA((PARTS + BATCHES,))],
        name="chemistry",
    )(*parts, lit, k, table)


def body(
    mixing_ratio_field,
    eastward_face_cfl,
    northward_face_cfl,
    upward_face_cfl,
    thermal_anomaly,
    radiant_flux,
    daylight_mask,
    baseline_kinetic_coefficient,
    arrhenius_barrier,
    photodissociation_factor,
    stoichiometry_table,
):
    groups = lax.axis_size("tracer")
    strips = lax.axis_size("space")
    z = Sizes(mixing_ratio_field, groups)
    courant = jnp.stack([eastward_face_cfl, northward_face_cfl, upward_face_cfl])
    low, high, courant, *fields = pack(z, flat_rows(mixing_ratio_field), flat_rows(courant))
    mask, table, _ = lax.optimization_barrier((daylight_mask, stoichiometry_table, courant))
    lit = jnp.broadcast_to(jnp.moveaxis(mask, 2, 1).reshape(z.blocks, 1), (z.blocks, LANES))
    k = rates(
        z,
        courant,
        flat_rows(thermal_anomaly),
        flat_rows(radiant_flux),
        lit,
        baseline_kinetic_coefficient,
        arrhenius_barrier,
        photodissociation_factor,
    )
    table = table.reshape(-1) * z.blocks
    low = lax.ppermute(low, "space", [(i, i + 1) for i in range(strips - 1)])
    high = lax.ppermute(high, "space", [(i + 1, i) for i in range(strips - 1)])
    low, high, k, lit, table = lax.optimization_barrier((low, high, k, lit, table))
    species = z.species * groups
    arrived = []
    moved = low
    for part in range(PARTS):
        field, _ = lax.optimization_barrier((fields[part], moved))
        moved = transport(z, part, field, courant, low, high)
        regrouped = lax.all_to_all(
            moved.reshape(groups, z.count * z.blocks, LANES), "tracer", split_axis=0, concat_axis=0, tiled=True
        )
        arrived.append(regrouped.reshape(species // PARTS * z.blocks, LANES))
    out = chemistry(z, species, k, *arrived, lit, table)
    out = out.reshape(species, z.levels, z.tiles, z.part, LANES)
    return jnp.moveaxis(out, 2, 3).reshape(species, z.levels, z.part, z.width)


def solution(mesh):
    placed = (
        P("tracer", None, "space", None),
        P(None, "space", None),
        P(None, "space", None),
        P(None, "space", None),
        P(None, ("space", "tracer"), None),
        P(None, ("space", "tracer"), None),
        P(None, ("space", "tracer"), None),
        P(),
        P(),
        P(),
        P(),
    )
    return jax.shard_map(
        body,
        mesh=mesh,
        in_specs=placed,
        out_specs=P(None, None, ("space", "tracer"), None),
        check_vma=False,
    )
```

```python
import functools

import jax
import jax.numpy as jnp
from jax import lax
from jax.experimental import pallas as pl
from jax.experimental.pallas import tpu as pltpu
from jax.sharding import PartitionSpec as P


SECTIONS = 3
DAY_STEPS = 2
LANES = 128
SUB = 8
LOW = 2 * SECTIONS
HIGH = SECTIONS
PARTS = 2
TOGETHER = 8
CHUNK = 8
LOG2E = 1.4426950408889634


def flat_rows(cells):
    *lead, rows, width = cells.shape
    sub = min(rows, SUB)
    split = cells.reshape(*lead, rows // sub, sub, width // LANES, LANES)
    return jnp.moveaxis(split, -2, -3).reshape(-1, LANES)


class Sizes:
    def __init__(self, field, groups):
        self.species, self.levels, self.rows, self.width = field.shape
        self.tiles = self.width // LANES
        self.groups = groups
        self.part = self.rows // groups
        self.blocks = self.levels * self.tiles * self.part
        self.stride = self.levels * self.rows * self.tiles
        self.columns = self.levels * self.tiles
        self.count = self.species // PARTS
        self.low_rows = LOW * self.columns * self.count
        self.high_rows = HIGH * self.columns * self.count
        self.span = self.rows + 2 * SUB
        self.edge_rows = 3 * self.columns * SUB

    def source_row(self, level, row, tile):
        return ((level * (self.rows // SUB) + row // SUB) * self.tiles + tile) * SUB + row % SUB

    def pairs(self):
        return [(level, tile) for level in range(self.levels) for tile in range(self.tiles)]


def middle(a, b):
    return jnp.maximum(jnp.minimum(a, b), jnp.minimum(jnp.maximum(a, b), 0.0))


def shift_columns(parts, amount):
    if amount > 0:
        return [pltpu.roll(parts[-1], 1, 1)] + parts[:-1]
    return parts[1:] + [pltpu.roll(parts[0], LANES - 1, 1)]


def spread_matrix(tiles, back):
    natural = lax.broadcasted_iota(jnp.int32, (tiles * LANES, tiles * LANES), 1 if back else 0)
    spread = lax.broadcasted_iota(jnp.int32, (tiles * LANES, tiles * LANES), 0 if back else 1)
    hit = natural == (spread % LANES) * tiles + spread // LANES
    return jnp.where(hit, 1.0, 0.0).astype(jnp.bfloat16)


def reorder(parts, matrix):
    x = jnp.concatenate(parts, axis=1)
    total = None
    for _ in range(3):
        piece = x.astype(jnp.bfloat16)
        x = x - piece.astype(jnp.float32)
        term = jnp.dot(piece, matrix, preferred_element_type=jnp.float32)
        total = term if total is None else total + term
    return [total[:, k * LANES : (k + 1) * LANES] for k in range(len(parts))]


def pack_kernel(z, part, x_ref, *refs):
    forth = spread_matrix(z.tiles, False)
    if part == 0:
        courant_ref, low_ref, high_ref, field, courant_out = refs
    else:
        low_ref, high_ref, field = refs

    def spread(flat, strips):
        split = flat.reshape(strips, z.rows // SUB, z.tiles, SUB, LANES)
        return reorder([split[:, :, t].reshape(strips * z.rows, LANES) for t in range(z.tiles)], forth)

    if part == 0:
        parts = spread(courant_ref[...], 3 * z.levels)
        shifted = shift_columns(parts, -1)
        for strip in range(3 * z.levels):
            rows = slice(strip * z.rows, (strip + 1) * z.rows)
            for tile in range(z.tiles):
                value = (shifted if strip // z.levels == 1 else parts)[tile][rows]
                col = strip * z.tiles + tile
                courant_out[pl.ds(col * z.rows, z.rows), :] = value
                low_ref[pl.ds(z.low_rows + col * SUB, SUB), :] = value[z.rows - SUB :]
                high_ref[pl.ds(z.high_rows + col * SUB, SUB), :] = value[:SUB]

    def some(index, carry):
        strips = CHUNK * z.levels
        size = strips * z.tiles * z.rows
        start = pl.multiple_of((part * (z.count // CHUNK) + index) * size, SUB)
        values = spread(x_ref[pl.ds(start, size), :], strips)
        for strip in range(strips):
            for tile in range(z.tiles):
                at = pl.multiple_of(index * size + (strip * z.tiles + tile) * z.rows, SUB)
                field[pl.ds(at, z.rows), :] = values[tile][strip * z.rows : (strip + 1) * z.rows]
        return carry

    lax.fori_loop(0, z.count // CHUNK, some, 0)

    def edges(index, carry):
        for col in range(z.columns):
            target = index * z.columns + col
            source = target * z.rows
            low_ref[pl.ds(target * LOW, LOW), :] = field[pl.ds(source + z.rows - LOW, LOW), :]
            high_ref[pl.ds(target * HIGH, HIGH), :] = field[pl.ds(source, HIGH), :]
        return carry

    lax.fori_loop(0, z.count, edges, 0, unroll=4)


def transport_kernel(z, field_ref, courant_ref, low_edge, high_edge, low_ref, high_ref, *refs):
    span = z.span
    cols = range(z.columns)
    outs, (coef, final, natural), slots = refs[: z.groups], refs[z.groups : z.groups + 3], refs[z.groups + 3 :]

    def coef_row(kind, which, col, j):
        return ((kind * 2 + which) * z.columns + col) * span + j

    for kind in range(3):
        for col in cols:
            one = kind * z.columns + col
            tiles = [low_edge[pl.ds(one * SUB, SUB), :]]
            tiles += [courant_ref[pl.ds(one * z.rows + row, SUB), :] for row in range(0, z.rows, SUB)]
            tiles += [high_edge[pl.ds(one * SUB, SUB), :]]
            for k, value in enumerate(tiles):
                coef[pl.ds(coef_row(kind, 0, col, k * SUB), SUB), :] = value
                coef[pl.ds(coef_row(kind, 1, col, k * SUB), SUB), :] = 0.5 * value * (1.0 - value)

    def weights(kind, col, j):
        return [coef[pl.ds(coef_row(kind, which, col, j), SUB), :] for which in range(2)]

    def one_species(index, start, fields, fluxes):
        for col in cols:
            base = index * z.columns + col
            at = col * span + SUB
            start[pl.ds(at - LOW, LOW), :] = low_ref[pl.ds(base * LOW, LOW), :]
            start[pl.ds(at + z.rows, HIGH), :] = high_ref[pl.ds(base * HIGH, HIGH), :]
            start[pl.ds(at, z.rows), :] = field_ref[pl.ds(pl.multiple_of(base * z.rows, SUB), z.rows), :]
        for step in range(SECTIONS):
            write = fields[step % 2]
            source = start if step == 0 else fields[(step + 1) % 2]
            read = lambda col, j, ref=source: ref[pl.ds(col * span + j, SUB), :]
            bottom = SUB - LOW + 2 * (step + 1)
            top = SUB + z.rows + HIGH - (step + 1)
            for j in range(bottom - 1, top, SUB):
                for col in cols:
                    below, here, above = [read(col, j + k) for k in (-1, 0, 1)]
                    a, b = weights(0, col, j + 1)
                    fluxes[pl.ds(col * span + j, SUB), :] = a * here + b * middle(here - below, above - here)
            for j in range(bottom, top, SUB):
                c = []
                for col in cols:
                    leave = fluxes[pl.ds(col * span + j, SUB), :]
                    enter = fluxes[pl.ds(col * span + j - 1, SUB), :]
                    c.append(read(col, j) - (leave - enter))
                for level in range(z.levels):
                    mine = slice(level * z.tiles, (level + 1) * z.tiles)
                    row = c[mine]
                    back = [v - w for v, w in zip(row, shift_columns(row, 1))]
                    ahead = shift_columns(back, -1)
                    leave = []
                    for tile in range(z.tiles):
                        a, b = weights(1, level * z.tiles + tile, j)
                        leave.append(a * row[tile] + b * middle(back[tile], ahead[tile]))
                    enter = shift_columns(leave, 1)
                    c[mine] = [row[t] - (leave[t] - enter[t]) for t in range(z.tiles)]
                for tile in range(z.tiles):
                    column = [c[level * z.tiles + tile] for level in range(z.levels)]
                    steps = [column[0]]
                    steps += [column[k + 1] - column[k] for k in range(z.levels - 1)]
                    steps += [-column[-1]]
                    lift = None
                    for level in range(z.levels):
                        col = level * z.tiles + tile
                        a, b = weights(2, col, j)
                        rising = a * column[level] + b * middle(steps[level], steps[level + 1])
                        net = rising if lift is None else rising - lift
                        lift = rising
                        value = column[level] - net
                        if step < SECTIONS - 1:
                            write[pl.ds(col * span + j, SUB), :] = value
                        else:
                            base = (index * z.columns + col) * z.rows + j - SUB
                            final[pl.ds(pl.multiple_of(base, SUB), SUB), :] = value

    def some_species(index, carry):
        for k in range(TOGETHER):
            one_species(index * TOGETHER + k, slots[4 * k], slots[4 * k + 1 : 4 * k + 3], slots[4 * k + 3])
        return carry

    lax.fori_loop(0, z.count // TOGETHER, some_species, 0)

    back = spread_matrix(z.tiles, True)
    me = lax.axis_index("tracer")

    def scatter(index, carry):
        many = CHUNK * z.levels
        size = many * z.tiles * z.rows
        whole = final[pl.ds(pl.multiple_of(index * size, SUB), size), :].reshape(many, z.tiles, z.rows, LANES)
        parts = reorder([whole[:, t].reshape(many * z.rows, LANES) for t in range(z.tiles)], back)
        for one in range(many):
            for tile in range(z.tiles):
                strip = one * z.tiles + tile
                natural[pl.ds(strip * z.rows, z.rows), :] = parts[tile][one * z.rows : (one + 1) * z.rows]
        for k, out_ref in enumerate(outs):
            first = (me ^ k) * z.part
            for strip in range(many * z.tiles):
                at = index * CHUNK * z.blocks + strip * z.part
                out_ref[pl.ds(at, z.part), :] = natural[pl.ds(strip * z.rows + first, z.part), :]
        return carry

    lax.fori_loop(0, z.count // CHUNK, scatter, 0)


def rates_kernel(pieces, warm_ref, glow_ref, lit_ref, rate_ref, barrier_ref, photo_ref, out_ref):
    warm = [(1.0 - warm_ref[pl.ds(p * SUB, SUB), :]) * LOG2E for p in range(pieces)]
    glow = [
        jnp.where(lit_ref[pl.ds(p * SUB, SUB), :] == 1, glow_ref[pl.ds(p * SUB, SUB), :], 0.0)
        for p in range(pieces)
    ]

    def one(r, carry):
        for p in range(pieces):
            at = pl.ds(pl.multiple_of(r * pieces * SUB, SUB) + p * SUB, SUB)
            out_ref[at, :] = rate_ref[r] * jnp.exp2(barrier_ref[r] * warm[p]) + photo_ref[r] * glow[p]
        return carry

    lax.fori_loop(0, rate_ref.shape[0], one, 0, unroll=8)


def chemistry_kernel(z, species, *refs):
    pieces = z.blocks // SUB
    sources = refs[: PARTS * z.groups]
    lit_ref, k_ref, table_ref, out_ref, state, made, lost_a, lost_b = refs[PARTS * z.groups :]
    reactions = k_ref.shape[0] // z.blocks

    def cell(row, piece):
        return pl.ds(pl.multiple_of(row, SUB) + piece * SUB, SUB)

    lit = [lit_ref[pl.ds(p * SUB, SUB), :] == 1 for p in range(pieces)]
    steps = [jnp.where(lit[p], float(DAY_STEPS), 1.0) for p in range(pieces)]
    zero = jnp.zeros((SUB, LANES), jnp.float32)
    me = lax.axis_index("tracer")

    def prepare(at, p, value):
        made[at, :] = steps[p] * value
        lost_a[at, :] = steps[p]
        lost_b[at, :] = zero

    def begin(index, carry):
        for number, ref in enumerate(sources):
            part, k = divmod(number, z.groups)
            first = (me ^ k) * z.species + part * z.count
            for p in range(pieces):
                value = ref[cell(index * z.blocks, p), :]
                at = cell((first + index) * z.blocks, p)
                state[at, :] = value
                prepare(at, p, value)
        return carry

    lax.fori_loop(0, z.count, begin, 0)

    def react(r, carry):
        first, second, product = table_ref[r], table_ref[reactions + r], table_ref[2 * reactions + r]
        for p in range(pieces):
            k = k_ref[cell(r * z.blocks, p), :]
            x = state[cell(first, p), :]
            y = state[cell(second, p), :]
            kx = k * x
            ky = k * y
            made[cell(product, p), :] += kx * y
            lost_a[cell(first, p), :] += ky
            lost_b[cell(second, p), :] += kx
        return carry

    for sub in range(DAY_STEPS):
        lax.fori_loop(0, reactions, react, 0, unroll=16)

        def finish(s, carry):
            for p in range(pieces):
                at = cell(s * z.blocks, p)
                value = made[at, :] / (lost_a[at, :] + lost_b[at, :])
                if sub < DAY_STEPS - 1:
                    prepare(at, p, value)
                    if sub == 0:
                        state[at, :] = value
                if sub > 0:
                    value = jnp.where(lit[p], value, state[at, :])
                    out_ref[at, :] = value
            return carry

        lax.fori_loop(0, species, finish, 0, unroll=4)


VMEM = pl.BlockSpec(memory_space=pltpu.VMEM)
SMEM = pl.BlockSpec(memory_space=pltpu.SMEM)


def rows_of(count):
    return jax.ShapeDtypeStruct((count, LANES), jnp.float32)


ANY = pl.BlockSpec(memory_space=pl.ANY)
HBM = pl.BlockSpec(memory_space=pltpu.HBM)


def pack(z, part, *flat):
    extra = z.edge_rows if part == 0 else 0
    rows = [z.low_rows + extra, z.high_rows + extra, z.count * z.columns * z.rows]
    if part == 0:
        rows.append(3 * z.columns * z.rows)
    return pl.pallas_call(
        functools.partial(pack_kernel, z, part),
        out_shape=tuple(rows_of(n) for n in rows),
        in_specs=[VMEM] * len(flat),
        out_specs=(VMEM,) * len(rows),
        compiler_params=pltpu.CompilerParams(vmem_limit_bytes=16 << 20),
        cost_estimate=pl.CostEstimate(flops=100 * z.count * z.stride * LANES, bytes_accessed=0, transcendentals=0),
        name="pack",
    )(*flat)


def transport(z, *flat):
    size = z.span * z.columns
    scratch = [6 * size, z.count * z.columns * z.rows, CHUNK * z.columns * z.rows] + [size] * (4 * TOGETHER)
    return pl.pallas_call(
        functools.partial(transport_kernel, z),
        out_shape=(rows_of(z.count * z.blocks),) * z.groups,
        in_specs=[VMEM] * len(flat),
        out_specs=(VMEM,) * z.groups,
        scratch_shapes=[pltpu.VMEM((n, LANES), jnp.float32) for n in scratch],
        compiler_params=pltpu.CompilerParams(vmem_limit_bytes=20 << 20),
        cost_estimate=pl.CostEstimate(flops=400 * z.count * z.stride * LANES, bytes_accessed=0, transcendentals=0),
        name="transport",
    )(*flat)


def rates(z, warm, glow, lit, rate, barrier, photo):
    reactions = rate.shape[0]
    return pl.pallas_call(
        functools.partial(rates_kernel, z.blocks // SUB),
        out_shape=rows_of(reactions * z.blocks),
        in_specs=[VMEM] * 3 + [SMEM] * 3,
        out_specs=VMEM,
        compiler_params=pltpu.CompilerParams(vmem_limit_bytes=16 << 20),
        cost_estimate=pl.CostEstimate(
            flops=40 * reactions * z.blocks * LANES, bytes_accessed=0, transcendentals=0
        ),
        name="rates",
    )(warm, glow, lit, rate, barrier, photo)


def chemistry(z, species, arrived, lit, k, table):
    size = species * z.blocks
    return pl.pallas_call(
        functools.partial(chemistry_kernel, z, species),
        out_shape=rows_of(size),
        in_specs=[VMEM] * (len(arrived) + 2) + [SMEM],
        out_specs=VMEM,
        scratch_shapes=[pltpu.VMEM((size, LANES), jnp.float32)] * 4,
        compiler_params=pltpu.CompilerParams(vmem_limit_bytes=20 << 20),
        name="chemistry",
    )(*arrived, lit, k, table)


def body(
    mixing_ratio_field,
    eastward_face_cfl,
    northward_face_cfl,
    upward_face_cfl,
    thermal_anomaly,
    radiant_flux,
    daylight_mask,
    baseline_kinetic_coefficient,
    arrhenius_barrier,
    photodissociation_factor,
    stoichiometry_table,
):
    groups = lax.axis_size("tracer")
    strips = lax.axis_size("space")
    z = Sizes(mixing_ratio_field, groups)
    courant = flat_rows(jnp.stack([eastward_face_cfl, northward_face_cfl, upward_face_cfl]))
    field = flat_rows(mixing_ratio_field)
    upward = [(i, i + 1) for i in range(strips - 1)]
    downward = [(i + 1, i) for i in range(strips - 1)]
    fields, halos = [], []
    for part in range(PARTS):
        if part == 0:
            low, high, ready, courant = pack(z, part, field, courant)
        else:
            field, _ = lax.optimization_barrier((field, ready))
            low, high, ready = pack(z, part, field)
        low = lax.ppermute(low, "space", upward)
        high = lax.ppermute(high, "space", downward)
        fields.append(ready)
        halos.append((low, high))
    low_edge = halos[0][0][z.low_rows :]
    high_edge = halos[0][1][z.high_rows :]
    arrived = []
    for part in range(PARTS):
        ready = fields[part]
        if part > 0:
            ready, _ = lax.optimization_barrier((ready, moved[0]))
        moved = transport(z, ready, courant, low_edge, high_edge, *halos[part])
        arrived.append(moved[0])
        for k in range(1, groups):
            arrived.append(lax.ppermute(moved[k], "tracer", [(i, i ^ k) for i in range(groups)]))
    mask, table, _ = lax.optimization_barrier((daylight_mask, stoichiometry_table, moved[0]))
    lit = jnp.broadcast_to(jnp.moveaxis(mask, 2, 1).reshape(z.blocks, 1), (z.blocks, LANES))
    k = rates(
        z,
        flat_rows(thermal_anomaly),
        flat_rows(radiant_flux),
        lit,
        baseline_kinetic_coefficient,
        arrhenius_barrier,
        photodissociation_factor,
    )
    species = z.species * groups
    out = chemistry(z, species, arrived, lit, k, table.reshape(-1) * z.blocks)
    out = out.reshape(species, z.levels, z.tiles, z.part, LANES)
    return jnp.moveaxis(out, 2, 3).reshape(species, z.levels, z.part, z.width)


def solution(mesh):
    placed = (
        P("tracer", None, "space", None),
        P(None, "space", None),
        P(None, "space", None),
        P(None, "space", None),
        P(None, ("space", "tracer"), None),
        P(None, ("space", "tracer"), None),
        P(None, ("space", "tracer"), None),
        P(),
        P(),
        P(),
        P(),
    )
    return jax.shard_map(
        body,
        mesh=mesh,
        in_specs=placed,
        out_specs=P(None, None, ("space", "tracer"), None),
        check_vma=False,
    )
```

```python
import functools

import jax
import jax.numpy as jnp
from jax import lax
from jax.experimental import pallas as pl
from jax.experimental.pallas import tpu as pltpu
from jax.sharding import PartitionSpec as P


SECTIONS = 3
DAY_STEPS = 2
LANES = 128
SUB = 8
LOW = 2 * SECTIONS
HIGH = SECTIONS
PARTS = 2
TOGETHER = 8
CHUNK = 8
LOG2E = 1.4426950408889634


def flat_rows(cells):
    *lead, rows, width = cells.shape
    sub = min(rows, SUB)
    split = cells.reshape(*lead, rows // sub, sub, width // LANES, LANES)
    return jnp.moveaxis(split, -2, -3).reshape(-1, LANES)


class Sizes:
    def __init__(self, field, groups):
        self.species, self.levels, self.rows, self.width = field.shape
        self.tiles = self.width // LANES
        self.groups = groups
        self.part = self.rows // groups
        self.blocks = self.levels * self.tiles * self.part
        self.stride = self.levels * self.rows * self.tiles
        self.columns = self.levels * self.tiles
        self.count = self.species // PARTS
        self.halo_rows = LOW * self.columns * self.count
        self.span = self.rows + 2 * SUB
        self.edge_rows = 3 * self.columns * SUB

    def source_row(self, level, row, tile):
        return ((level * (self.rows // SUB) + row // SUB) * self.tiles + tile) * SUB + row % SUB

    def pairs(self):
        return [(level, tile) for level in range(self.levels) for tile in range(self.tiles)]


def middle(a, b):
    return jnp.maximum(jnp.minimum(a, b), jnp.minimum(jnp.maximum(a, b), 0.0))


def shift_columns(parts, amount):
    if amount > 0:
        return [pltpu.roll(parts[-1], 1, 1)] + parts[:-1]
    return parts[1:] + [pltpu.roll(parts[0], LANES - 1, 1)]


def spread_matrix(tiles, back):
    natural = lax.broadcasted_iota(jnp.int32, (tiles * LANES, tiles * LANES), 1 if back else 0)
    spread = lax.broadcasted_iota(jnp.int32, (tiles * LANES, tiles * LANES), 0 if back else 1)
    hit = natural == (spread % LANES) * tiles + spread // LANES
    return jnp.where(hit, 1.0, 0.0).astype(jnp.bfloat16)


def reorder(parts, matrix):
    x = jnp.concatenate(parts, axis=1)
    total = None
    for _ in range(3):
        piece = x.astype(jnp.bfloat16)
        x = x - piece.astype(jnp.float32)
        term = jnp.dot(piece, matrix, preferred_element_type=jnp.float32)
        total = term if total is None else total + term
    return [total[:, k * LANES : (k + 1) * LANES] for k in range(len(parts))]


def pack_kernel(z, part, x_ref, *refs):
    forth = spread_matrix(z.tiles, False)
    if part == 0:
        courant_ref, near_ref, far_ref, field, courant_out = refs
    else:
        near_ref, far_ref, field = refs
    odd = lax.rem(lax.axis_index("space"), 2)
    sides = ((near_ref, odd), (far_ref, 1 - odd))

    def spread(flat, strips):
        split = flat.reshape(strips, z.rows // SUB, z.tiles, SUB, LANES)
        return reorder([split[:, :, t].reshape(strips * z.rows, LANES) for t in range(z.tiles)], forth)

    if part == 0:
        parts = spread(courant_ref[...], 3 * z.levels)
        shifted = shift_columns(parts, -1)
        for strip in range(3 * z.levels):
            rows = slice(strip * z.rows, (strip + 1) * z.rows)
            for tile in range(z.tiles):
                value = (shifted if strip // z.levels == 1 else parts)[tile][rows]
                col = strip * z.tiles + tile
                courant_out[pl.ds(col * z.rows, z.rows), :] = value

    def some(index, carry):
        strips = CHUNK * z.levels
        size = strips * z.tiles * z.rows
        start = pl.multiple_of((part * (z.count // CHUNK) + index) * size, SUB)
        values = spread(x_ref[pl.ds(start, size), :], strips)
        for strip in range(strips):
            for tile in range(z.tiles):
                at = pl.multiple_of(index * size + (strip * z.tiles + tile) * z.rows, SUB)
                field[pl.ds(at, z.rows), :] = values[tile][strip * z.rows : (strip + 1) * z.rows]
        return carry

    lax.fori_loop(0, z.count // CHUNK, some, 0)

    if part == 0:
        for ref, below in sides:
            for col in range(3 * z.columns):
                source = col * z.rows + (1 - below) * (z.rows - SUB)
                ref[pl.ds(z.halo_rows + col * SUB, SUB), :] = courant_out[pl.ds(pl.multiple_of(source, SUB), SUB), :]

    def edges(index, carry):
        for ref, below in sides:
            for col in range(z.columns):
                target = index * z.columns + col
                source = target * z.rows + (1 - below) * (z.rows - LOW)
                ref[pl.ds(target * LOW, LOW), :] = field[pl.ds(source, LOW), :]
        return carry

    lax.fori_loop(0, z.count, edges, 0, unroll=4)


def transport_kernel(z, field_ref, courant_ref, near_edge, far_edge, near_ref, far_ref, *refs):
    span = z.span
    cols = range(z.columns)
    outs, (coef, final, natural, halo, edge), slots = refs[: z.groups], refs[z.groups : z.groups + 5], refs[z.groups + 5 :]
    odd = lax.rem(lax.axis_index("space"), 2)
    for source, above in ((near_ref, 1 - odd), (far_ref, odd)):

        def place_halo(i, carry):
            target = pl.multiple_of(above * z.halo_rows + i * SUB, SUB)
            halo[pl.ds(target, SUB), :] = source[pl.ds(pl.multiple_of(i * SUB, SUB), SUB), :]
            return carry

        lax.fori_loop(0, z.halo_rows // SUB, place_halo, 0, unroll=12)
    for source, above in ((near_edge, 1 - odd), (far_edge, odd)):
        for row in range(0, z.edge_rows, SUB):
            target = pl.multiple_of(above * z.edge_rows + row, SUB)
            edge[pl.ds(target, SUB), :] = source[pl.ds(row, SUB), :]

    def coef_row(kind, which, col, j):
        return ((kind * 2 + which) * z.columns + col) * span + j

    for kind in range(3):
        for col in cols:
            one = kind * z.columns + col
            tiles = [edge[pl.ds(one * SUB, SUB), :]]
            tiles += [courant_ref[pl.ds(one * z.rows + row, SUB), :] for row in range(0, z.rows, SUB)]
            tiles += [edge[pl.ds(z.edge_rows + one * SUB, SUB), :]]
            for k, value in enumerate(tiles):
                coef[pl.ds(coef_row(kind, 0, col, k * SUB), SUB), :] = value
                coef[pl.ds(coef_row(kind, 1, col, k * SUB), SUB), :] = 0.5 * value * (1.0 - value)

    def weights(kind, col, j):
        return [coef[pl.ds(coef_row(kind, which, col, j), SUB), :] for which in range(2)]

    def one_species(index, start, fields, fluxes):
        for col in cols:
            base = index * z.columns + col
            at = col * span + SUB
            start[pl.ds(at - LOW, LOW), :] = halo[pl.ds(base * LOW, LOW), :]
            start[pl.ds(at + z.rows, HIGH), :] = halo[pl.ds(z.halo_rows + base * LOW, HIGH), :]
            start[pl.ds(at, z.rows), :] = field_ref[pl.ds(pl.multiple_of(base * z.rows, SUB), z.rows), :]
        for step in range(SECTIONS):
            write = fields[step % 2]
            source = start if step == 0 else fields[(step + 1) % 2]
            read = lambda col, j, ref=source: ref[pl.ds(col * span + j, SUB), :]
            bottom = SUB - LOW + 2 * (step + 1)
            top = SUB + z.rows + HIGH - (step + 1)
            for j in range(bottom - 1, top, SUB):
                for col in cols:
                    below, here, above = [read(col, j + k) for k in (-1, 0, 1)]
                    a, b = weights(0, col, j + 1)
                    fluxes[pl.ds(col * span + j, SUB), :] = a * here + b * middle(here - below, above - here)
            for j in range(bottom, top, SUB):
                c = []
                for col in cols:
                    leave = fluxes[pl.ds(col * span + j, SUB), :]
                    enter = fluxes[pl.ds(col * span + j - 1, SUB), :]
                    c.append(read(col, j) - (leave - enter))
                for level in range(z.levels):
                    mine = slice(level * z.tiles, (level + 1) * z.tiles)
                    row = c[mine]
                    back = [v - w for v, w in zip(row, shift_columns(row, 1))]
                    ahead = shift_columns(back, -1)
                    leave = []
                    for tile in range(z.tiles):
                        a, b = weights(1, level * z.tiles + tile, j)
                        leave.append(a * row[tile] + b * middle(back[tile], ahead[tile]))
                    enter = shift_columns(leave, 1)
                    c[mine] = [row[t] - (leave[t] - enter[t]) for t in range(z.tiles)]
                for tile in range(z.tiles):
                    column = [c[level * z.tiles + tile] for level in range(z.levels)]
                    steps = [column[0]]
                    steps += [column[k + 1] - column[k] for k in range(z.levels - 1)]
                    steps += [-column[-1]]
                    lift = None
                    for level in range(z.levels):
                        col = level * z.tiles + tile
                        a, b = weights(2, col, j)
                        rising = a * column[level] + b * middle(steps[level], steps[level + 1])
                        net = rising if lift is None else rising - lift
                        lift = rising
                        value = column[level] - net
                        if step < SECTIONS - 1:
                            write[pl.ds(col * span + j, SUB), :] = value
                        else:
                            base = (index * z.columns + col) * z.rows + j - SUB
                            final[pl.ds(pl.multiple_of(base, SUB), SUB), :] = value

    def some_species(index, carry):
        for k in range(TOGETHER):
            one_species(index * TOGETHER + k, slots[4 * k], slots[4 * k + 1 : 4 * k + 3], slots[4 * k + 3])
        return carry

    lax.fori_loop(0, z.count // TOGETHER, some_species, 0)

    back = spread_matrix(z.tiles, True)
    me = lax.axis_index("tracer")

    def scatter(index, carry):
        many = CHUNK * z.levels
        size = many * z.tiles * z.rows
        whole = final[pl.ds(pl.multiple_of(index * size, SUB), size), :].reshape(many, z.tiles, z.rows, LANES)
        parts = reorder([whole[:, t].reshape(many * z.rows, LANES) for t in range(z.tiles)], back)
        for one in range(many):
            for tile in range(z.tiles):
                strip = one * z.tiles + tile
                natural[pl.ds(strip * z.rows, z.rows), :] = parts[tile][one * z.rows : (one + 1) * z.rows]
        for k, out_ref in enumerate(outs):
            first = (me ^ k) * z.part
            for strip in range(many * z.tiles):
                at = index * CHUNK * z.blocks + strip * z.part
                out_ref[pl.ds(at, z.part), :] = natural[pl.ds(strip * z.rows + first, z.part), :]
        return carry

    lax.fori_loop(0, z.count // CHUNK, scatter, 0)


def rates_kernel(pieces, warm_ref, glow_ref, lit_ref, rate_ref, barrier_ref, photo_ref, out_ref):
    warm = [(1.0 - warm_ref[pl.ds(p * SUB, SUB), :]) * LOG2E for p in range(pieces)]
    glow = [
        jnp.where(lit_ref[pl.ds(p * SUB, SUB), :] == 1, glow_ref[pl.ds(p * SUB, SUB), :], 0.0)
        for p in range(pieces)
    ]

    def one(r, carry):
        for p in range(pieces):
            at = pl.ds(pl.multiple_of(r * pieces * SUB, SUB) + p * SUB, SUB)
            out_ref[at, :] = rate_ref[r] * jnp.exp2(barrier_ref[r] * warm[p]) + photo_ref[r] * glow[p]
        return carry

    lax.fori_loop(0, rate_ref.shape[0], one, 0, unroll=8)


def chemistry_kernel(z, species, *refs):
    pieces = z.blocks // SUB
    sources = refs[: PARTS * z.groups]
    lit_ref, k_ref, table_ref, out_ref, state, made, lost_a, lost_b = refs[PARTS * z.groups :]
    reactions = k_ref.shape[0] // z.blocks

    def cell(row, piece):
        return pl.ds(pl.multiple_of(row, SUB) + piece * SUB, SUB)

    lit = [lit_ref[pl.ds(p * SUB, SUB), :] == 1 for p in range(pieces)]
    steps = [jnp.where(lit[p], float(DAY_STEPS), 1.0) for p in range(pieces)]
    zero = jnp.zeros((SUB, LANES), jnp.float32)
    me = lax.axis_index("tracer")

    def prepare(at, p, value):
        made[at, :] = steps[p] * value
        lost_a[at, :] = steps[p]
        lost_b[at, :] = zero

    def begin(index, carry):
        for number, ref in enumerate(sources):
            part, k = divmod(number, z.groups)
            first = (me ^ k) * z.species + part * z.count
            for p in range(pieces):
                value = ref[cell(index * z.blocks, p), :]
                at = cell((first + index) * z.blocks, p)
                state[at, :] = value
                prepare(at, p, value)
        return carry

    lax.fori_loop(0, z.count, begin, 0)

    def react(r, carry):
        first, second, product = table_ref[r], table_ref[reactions + r], table_ref[2 * reactions + r]
        for p in range(pieces):
            k = k_ref[cell(r * z.blocks, p), :]
            x = state[cell(first, p), :]
            y = state[cell(second, p), :]
            kx = k * x
            ky = k * y
            made[cell(product, p), :] += kx * y
            lost_a[cell(first, p), :] += ky
            lost_b[cell(second, p), :] += kx
        return carry

    for sub in range(DAY_STEPS):
        lax.fori_loop(0, reactions, react, 0, unroll=16)

        def finish(s, carry):
            for p in range(pieces):
                at = cell(s * z.blocks, p)
                value = made[at, :] / (lost_a[at, :] + lost_b[at, :])
                if sub < DAY_STEPS - 1:
                    prepare(at, p, value)
                    if sub == 0:
                        state[at, :] = value
                if sub > 0:
                    value = jnp.where(lit[p], value, state[at, :])
                    out_ref[at, :] = value
            return carry

        lax.fori_loop(0, species, finish, 0, unroll=4)


VMEM = pl.BlockSpec(memory_space=pltpu.VMEM)
SMEM = pl.BlockSpec(memory_space=pltpu.SMEM)


def rows_of(count):
    return jax.ShapeDtypeStruct((count, LANES), jnp.float32)


ANY = pl.BlockSpec(memory_space=pl.ANY)
HBM = pl.BlockSpec(memory_space=pltpu.HBM)


def pack(z, part, *flat):
    extra = z.edge_rows if part == 0 else 0
    rows = [z.halo_rows + extra, z.halo_rows + extra, z.count * z.columns * z.rows]
    if part == 0:
        rows.append(3 * z.columns * z.rows)
    return pl.pallas_call(
        functools.partial(pack_kernel, z, part),
        out_shape=tuple(rows_of(n) for n in rows),
        in_specs=[VMEM] * len(flat),
        out_specs=(VMEM,) * len(rows),
        compiler_params=pltpu.CompilerParams(vmem_limit_bytes=16 << 20),
        cost_estimate=pl.CostEstimate(flops=100 * z.count * z.stride * LANES, bytes_accessed=0, transcendentals=0),
        name="pack",
    )(*flat)


def transport(z, *flat):
    size = z.span * z.columns
    scratch = [6 * size, z.count * z.columns * z.rows, CHUNK * z.columns * z.rows]
    scratch += [2 * z.halo_rows, 2 * z.edge_rows] + [size] * (4 * TOGETHER)
    return pl.pallas_call(
        functools.partial(transport_kernel, z),
        out_shape=(rows_of(z.count * z.blocks),) * z.groups,
        in_specs=[VMEM] * len(flat),
        out_specs=(VMEM,) * z.groups,
        scratch_shapes=[pltpu.VMEM((n, LANES), jnp.float32) for n in scratch],
        compiler_params=pltpu.CompilerParams(vmem_limit_bytes=20 << 20),
        cost_estimate=pl.CostEstimate(flops=400 * z.count * z.stride * LANES, bytes_accessed=0, transcendentals=0),
        name="transport",
    )(*flat)


def rates(z, warm, glow, lit, rate, barrier, photo):
    reactions = rate.shape[0]
    return pl.pallas_call(
        functools.partial(rates_kernel, z.blocks // SUB),
        out_shape=rows_of(reactions * z.blocks),
        in_specs=[VMEM] * 3 + [SMEM] * 3,
        out_specs=VMEM,
        compiler_params=pltpu.CompilerParams(vmem_limit_bytes=16 << 20),
        cost_estimate=pl.CostEstimate(
            flops=40 * reactions * z.blocks * LANES, bytes_accessed=0, transcendentals=0
        ),
        name="rates",
    )(warm, glow, lit, rate, barrier, photo)


def chemistry(z, species, arrived, lit, k, table):
    size = species * z.blocks
    return pl.pallas_call(
        functools.partial(chemistry_kernel, z, species),
        out_shape=rows_of(size),
        in_specs=[VMEM] * (len(arrived) + 2) + [SMEM],
        out_specs=VMEM,
        scratch_shapes=[pltpu.VMEM((size, LANES), jnp.float32)] * 4,
        compiler_params=pltpu.CompilerParams(vmem_limit_bytes=20 << 20),
        name="chemistry",
    )(*arrived, lit, k, table)


def body(
    mixing_ratio_field,
    eastward_face_cfl,
    northward_face_cfl,
    upward_face_cfl,
    thermal_anomaly,
    radiant_flux,
    daylight_mask,
    baseline_kinetic_coefficient,
    arrhenius_barrier,
    photodissociation_factor,
    stoichiometry_table,
):
    groups = lax.axis_size("tracer")
    strips = lax.axis_size("space")
    z = Sizes(mixing_ratio_field, groups)
    courant = flat_rows(jnp.stack([eastward_face_cfl, northward_face_cfl, upward_face_cfl]))
    field = flat_rows(mixing_ratio_field)
    near_pairs = [(i, i ^ 1) for i in range(strips) if i ^ 1 < strips]
    far_pairs = [(i, ((i + 1) ^ 1) - 1) for i in range(strips) if 0 <= ((i + 1) ^ 1) - 1 < strips]
    fields, halos = [], []
    for part in range(PARTS):
        if part == 0:
            near, far, ready, courant = pack(z, part, field, courant)
        else:
            field, _ = lax.optimization_barrier((field, ready))
            near, far, ready = pack(z, part, field)
        far = lax.ppermute(far, "space", far_pairs)
        near = lax.ppermute(near, "space", near_pairs)
        fields.append(ready)
        halos.append((near, far))
    edges = [halo[z.halo_rows :] for halo in halos[0]]
    arrived = []
    for part in range(PARTS):
        ready = fields[part]
        if part > 0:
            ready, _ = lax.optimization_barrier((ready, moved[0]))
        moved = transport(z, ready, courant, *edges, *halos[part])
        arrived.append(moved[0])
        for k in range(1, groups):
            arrived.append(lax.ppermute(moved[k], "tracer", [(i, i ^ k) for i in range(groups)]))
    mask, table, _ = lax.optimization_barrier((daylight_mask, stoichiometry_table, moved[0]))
    lit = jnp.broadcast_to(jnp.moveaxis(mask, 2, 1).reshape(z.blocks, 1), (z.blocks, LANES))
    k = rates(
        z,
        flat_rows(thermal_anomaly),
        flat_rows(radiant_flux),
        lit,
        baseline_kinetic_coefficient,
        arrhenius_barrier,
        photodissociation_factor,
    )
    species = z.species * groups
    out = chemistry(z, species, arrived, lit, k, table.reshape(-1) * z.blocks)
    out = out.reshape(species, z.levels, z.tiles, z.part, LANES)
    return jnp.moveaxis(out, 2, 3).reshape(species, z.levels, z.part, z.width)


def solution(mesh):
    placed = (
        P("tracer", None, "space", None),
        P(None, "space", None),
        P(None, "space", None),
        P(None, "space", None),
        P(None, ("space", "tracer"), None),
        P(None, ("space", "tracer"), None),
        P(None, ("space", "tracer"), None),
        P(),
        P(),
        P(),
        P(),
    )
    return jax.shard_map(
        body,
        mesh=mesh,
        in_specs=placed,
        out_specs=P(None, None, ("space", "tracer"), None),
        check_vma=False,
    )
```

```python
import functools

import jax
import jax.numpy as jnp
from jax import lax
from jax.experimental import pallas as pl
from jax.experimental.pallas import tpu as pltpu
from jax.sharding import PartitionSpec as P


SECTIONS = 3
DAY_STEPS = 2
LANES = 128
SUB = 8
LOW = 2 * SECTIONS
HIGH = SECTIONS
PARTS = 2
TOGETHER = 8
CHUNK = 8
BATCHES = 4
LOG2E = 1.4426950408889634


def flat_rows(cells):
    *lead, rows, width = cells.shape
    sub = min(rows, SUB)
    split = cells.reshape(*lead, rows // sub, sub, width // LANES, LANES)
    return jnp.moveaxis(split, -2, -3).reshape(-1, LANES)


class Sizes:
    def __init__(self, field, groups):
        self.species, self.levels, self.rows, self.width = field.shape
        self.tiles = self.width // LANES
        self.groups = groups
        self.part = self.rows // groups
        self.blocks = self.levels * self.tiles * self.part
        self.stride = self.levels * self.rows * self.tiles
        self.columns = self.levels * self.tiles
        self.count = self.species // PARTS
        self.area = self.tiles * self.part
        self.slices = self.levels if self.area % SUB == 0 else 1
        self.slab = self.blocks // self.slices
        self.halo_rows = LOW * self.columns * self.count
        self.span = self.rows + 2 * SUB
        self.edge_rows = 3 * self.columns * SUB

    def source_row(self, level, row, tile):
        return ((level * (self.rows // SUB) + row // SUB) * self.tiles + tile) * SUB + row % SUB

    def pairs(self):
        return [(level, tile) for level in range(self.levels) for tile in range(self.tiles)]


def middle(a, b):
    return jnp.maximum(jnp.minimum(a, b), jnp.minimum(jnp.maximum(a, b), 0.0))


def shift_columns(parts, amount):
    if amount > 0:
        return [pltpu.roll(parts[-1], 1, 1)] + parts[:-1]
    return parts[1:] + [pltpu.roll(parts[0], LANES - 1, 1)]


def spread_matrix(tiles, back):
    natural = lax.broadcasted_iota(jnp.int32, (tiles * LANES, tiles * LANES), 1 if back else 0)
    spread = lax.broadcasted_iota(jnp.int32, (tiles * LANES, tiles * LANES), 0 if back else 1)
    hit = natural == (spread % LANES) * tiles + spread // LANES
    return jnp.where(hit, 1.0, 0.0).astype(jnp.bfloat16)


def reorder(parts, matrix):
    x = jnp.concatenate(parts, axis=1)
    total = None
    for _ in range(3):
        piece = x.astype(jnp.bfloat16)
        x = x - piece.astype(jnp.float32)
        term = jnp.dot(piece, matrix, preferred_element_type=jnp.float32)
        total = term if total is None else total + term
    return [total[:, k * LANES : (k + 1) * LANES] for k in range(len(parts))]


def pack_kernel(z, part, x_ref, *refs):
    forth = spread_matrix(z.tiles, False)
    if part == 0:
        courant_ref, near_ref, far_ref, field, courant_out = refs
    else:
        near_ref, far_ref, field = refs
    odd = lax.rem(lax.axis_index("space"), 2)
    sides = ((near_ref, odd), (far_ref, 1 - odd))

    def spread(flat, strips):
        split = flat.reshape(strips, z.rows // SUB, z.tiles, SUB, LANES)
        return reorder([split[:, :, t].reshape(strips * z.rows, LANES) for t in range(z.tiles)], forth)

    if part == 0:
        parts = spread(courant_ref[...], 3 * z.levels)
        shifted = shift_columns(parts, -1)
        for strip in range(3 * z.levels):
            rows = slice(strip * z.rows, (strip + 1) * z.rows)
            for tile in range(z.tiles):
                value = (shifted if strip // z.levels == 1 else parts)[tile][rows]
                col = strip * z.tiles + tile
                courant_out[pl.ds(col * z.rows, z.rows), :] = value

    def some(index, carry):
        strips = CHUNK * z.levels
        size = strips * z.tiles * z.rows
        start = pl.multiple_of((part * (z.count // CHUNK) + index) * size, SUB)
        values = spread(x_ref[pl.ds(start, size), :], strips)
        for strip in range(strips):
            for tile in range(z.tiles):
                at = pl.multiple_of(index * size + (strip * z.tiles + tile) * z.rows, SUB)
                field[pl.ds(at, z.rows), :] = values[tile][strip * z.rows : (strip + 1) * z.rows]
        return carry

    lax.fori_loop(0, z.count // CHUNK, some, 0)

    if part == 0:
        for ref, below in sides:
            for col in range(3 * z.columns):
                source = col * z.rows + (1 - below) * (z.rows - SUB)
                ref[pl.ds(z.halo_rows + col * SUB, SUB), :] = courant_out[pl.ds(pl.multiple_of(source, SUB), SUB), :]

    def edges(index, carry):
        for ref, below in sides:
            for col in range(z.columns):
                target = index * z.columns + col
                source = target * z.rows + (1 - below) * (z.rows - LOW)
                ref[pl.ds(target * LOW, LOW), :] = field[pl.ds(source, LOW), :]
        return carry

    lax.fori_loop(0, z.count, edges, 0, unroll=4)


def transport_kernel(z, slices, field_ref, courant_ref, near_edge, far_edge, near_ref, far_ref, *refs):
    span = z.span
    cols = range(z.columns)
    total = z.groups * slices
    outs, (coef, final, natural, halo, edge), slots = refs[:total], refs[total : total + 5], refs[total + 5 :]
    odd = lax.rem(lax.axis_index("space"), 2)
    for source, above in ((near_ref, 1 - odd), (far_ref, odd)):

        def place_halo(i, carry):
            target = pl.multiple_of(above * z.halo_rows + i * SUB, SUB)
            halo[pl.ds(target, SUB), :] = source[pl.ds(pl.multiple_of(i * SUB, SUB), SUB), :]
            return carry

        lax.fori_loop(0, z.halo_rows // SUB, place_halo, 0, unroll=12)
    for source, above in ((near_edge, 1 - odd), (far_edge, odd)):
        for row in range(0, z.edge_rows, SUB):
            target = pl.multiple_of(above * z.edge_rows + row, SUB)
            edge[pl.ds(target, SUB), :] = source[pl.ds(row, SUB), :]

    def coef_row(kind, which, col, j):
        return ((kind * 2 + which) * z.columns + col) * span + j

    for kind in range(3):
        for col in cols:
            one = kind * z.columns + col
            tiles = [edge[pl.ds(one * SUB, SUB), :]]
            tiles += [courant_ref[pl.ds(one * z.rows + row, SUB), :] for row in range(0, z.rows, SUB)]
            tiles += [edge[pl.ds(z.edge_rows + one * SUB, SUB), :]]
            for k, value in enumerate(tiles):
                coef[pl.ds(coef_row(kind, 0, col, k * SUB), SUB), :] = value
                coef[pl.ds(coef_row(kind, 1, col, k * SUB), SUB), :] = 0.5 * value * (1.0 - value)

    def weights(kind, col, j):
        return [coef[pl.ds(coef_row(kind, which, col, j), SUB), :] for which in range(2)]

    def one_species(index, start, fields, fluxes):
        for col in cols:
            base = index * z.columns + col
            at = col * span + SUB
            start[pl.ds(at - LOW, LOW), :] = halo[pl.ds(base * LOW, LOW), :]
            start[pl.ds(at + z.rows, HIGH), :] = halo[pl.ds(z.halo_rows + base * LOW, HIGH), :]
            start[pl.ds(at, z.rows), :] = field_ref[pl.ds(pl.multiple_of(base * z.rows, SUB), z.rows), :]
        for step in range(SECTIONS):
            write = fields[step % 2]
            source = start if step == 0 else fields[(step + 1) % 2]
            read = lambda col, j, ref=source: ref[pl.ds(col * span + j, SUB), :]
            bottom = SUB - LOW + 2 * (step + 1)
            top = SUB + z.rows + HIGH - (step + 1)
            for j in range(bottom - 1, top, SUB):
                for col in cols:
                    below, here, above = [read(col, j + k) for k in (-1, 0, 1)]
                    a, b = weights(0, col, j + 1)
                    fluxes[pl.ds(col * span + j, SUB), :] = a * here + b * middle(here - below, above - here)
            for j in range(bottom, top, SUB):
                c = []
                for col in cols:
                    leave = fluxes[pl.ds(col * span + j, SUB), :]
                    enter = fluxes[pl.ds(col * span + j - 1, SUB), :]
                    c.append(read(col, j) - (leave - enter))
                for level in range(z.levels):
                    mine = slice(level * z.tiles, (level + 1) * z.tiles)
                    row = c[mine]
                    back = [v - w for v, w in zip(row, shift_columns(row, 1))]
                    ahead = shift_columns(back, -1)
                    leave = []
                    for tile in range(z.tiles):
                        a, b = weights(1, level * z.tiles + tile, j)
                        leave.append(a * row[tile] + b * middle(back[tile], ahead[tile]))
                    enter = shift_columns(leave, 1)
                    c[mine] = [row[t] - (leave[t] - enter[t]) for t in range(z.tiles)]
                for tile in range(z.tiles):
                    column = [c[level * z.tiles + tile] for level in range(z.levels)]
                    steps = [column[0]]
                    steps += [column[k + 1] - column[k] for k in range(z.levels - 1)]
                    steps += [-column[-1]]
                    lift = None
                    for level in range(z.levels):
                        col = level * z.tiles + tile
                        a, b = weights(2, col, j)
                        rising = a * column[level] + b * middle(steps[level], steps[level + 1])
                        net = rising if lift is None else rising - lift
                        lift = rising
                        value = column[level] - net
                        if step < SECTIONS - 1:
                            write[pl.ds(col * span + j, SUB), :] = value
                        else:
                            base = (index * z.columns + col) * z.rows + j - SUB
                            final[pl.ds(pl.multiple_of(base, SUB), SUB), :] = value

    def some_species(index, carry):
        for k in range(TOGETHER):
            one_species(index * TOGETHER + k, slots[4 * k], slots[4 * k + 1 : 4 * k + 3], slots[4 * k + 3])
        return carry

    lax.fori_loop(0, z.count // TOGETHER, some_species, 0)

    back = spread_matrix(z.tiles, True)
    me = lax.axis_index("tracer")

    def scatter(index, carry):
        many = CHUNK * z.levels
        size = many * z.tiles * z.rows
        whole = final[pl.ds(pl.multiple_of(index * size, SUB), size), :].reshape(many, z.tiles, z.rows, LANES)
        parts = reorder([whole[:, t].reshape(many * z.rows, LANES) for t in range(z.tiles)], back)
        for one in range(many):
            for tile in range(z.tiles):
                strip = one * z.tiles + tile
                natural[pl.ds(strip * z.rows, z.rows), :] = parts[tile][one * z.rows : (one + 1) * z.rows]
        share = z.columns // slices
        for k in range(z.groups):
            first = (me ^ k) * z.part
            for strip in range(many * z.tiles):
                one, col = divmod(strip, z.columns)
                out_ref = outs[k * slices + col // share]
                at = ((index * CHUNK + one) * share + col % share) * z.part
                out_ref[pl.ds(at, z.part), :] = natural[pl.ds(strip * z.rows + first, z.part), :]
        return carry

    lax.fori_loop(0, z.count // CHUNK, scatter, 0)


def rates_kernel(pieces, warm_ref, glow_ref, lit_ref, rate_ref, barrier_ref, photo_ref, out_ref):
    warm = [(1.0 - warm_ref[pl.ds(p * SUB, SUB), :]) * LOG2E for p in range(pieces)]
    glow = [
        jnp.where(lit_ref[pl.ds(p * SUB, SUB), :] == 1, glow_ref[pl.ds(p * SUB, SUB), :], 0.0)
        for p in range(pieces)
    ]

    def one(r, carry):
        for p in range(pieces):
            at = pl.ds(pl.multiple_of(r * pieces * SUB, SUB) + p * SUB, SUB)
            out_ref[at, :] = rate_ref[r] * jnp.exp2(barrier_ref[r] * warm[p]) + photo_ref[r] * glow[p]
        return carry

    lax.fori_loop(0, rate_ref.shape[0], one, 0, unroll=8)


def chemistry_kernel(z, species, number, *refs):
    pieces = z.slab // SUB
    total = PARTS * z.groups
    sources, (lit_ref, k_ref, table_ref) = refs[:total], refs[total : total + 3]
    out_hbm, result, state, made, lost_a, lost_b, sems = refs[-7:]
    reactions = k_ref.shape[0] // z.blocks
    base = number * z.slab

    def cell(row, piece):
        return pl.ds(pl.multiple_of(row, SUB) + piece * SUB, SUB)

    lit = [lit_ref[pl.ds(base + p * SUB, SUB), :] == 1 for p in range(pieces)]
    steps = [jnp.where(lit[p], float(DAY_STEPS), 1.0) for p in range(pieces)]
    zero = jnp.zeros((SUB, LANES), jnp.float32)
    me = lax.axis_index("tracer")

    def prepare(at, p, value):
        made[at, :] = steps[p] * value
        lost_a[at, :] = steps[p]
        lost_b[at, :] = zero

    def begin(index, carry):
        for i, ref in enumerate(sources):
            part, k = divmod(i, z.groups)
            first = (me ^ k) * z.species + part * z.count
            for p in range(pieces):
                if part < PARTS - 1:
                    value = ref[cell(index * z.blocks + base, p), :]
                else:
                    value = ref[cell(index * z.slab, p), :]
                at = cell((first + index) * z.slab, p)
                state[at, :] = value
                prepare(at, p, value)
        return carry

    lax.fori_loop(0, z.count, begin, 0)

    def react(r, carry):
        first, second, product = table_ref[r], table_ref[reactions + r], table_ref[2 * reactions + r]
        for p in range(pieces):
            k = k_ref[cell(r * z.blocks + base, p), :]
            x = state[cell(first, p), :]
            y = state[cell(second, p), :]
            kx = k * x
            ky = k * y
            made[cell(product, p), :] += kx * y
            lost_a[cell(first, p), :] += ky
            lost_b[cell(second, p), :] += kx
        return carry

    batch = species // BATCHES

    def export(i):
        rows = pl.ds(i * batch, batch)
        return pltpu.make_async_copy(result.at[rows], out_hbm.at[rows, pl.ds(base, z.slab)], sems.at[i])

    for sub in range(DAY_STEPS):
        lax.fori_loop(0, reactions, react, 0, unroll=16)

        def finish(s, carry):
            for p in range(pieces):
                at = cell(s * z.slab, p)
                value = made[at, :] / (lost_a[at, :] + lost_b[at, :])
                if sub < DAY_STEPS - 1:
                    prepare(at, p, value)
                    if sub == 0:
                        state[at, :] = value
                if sub > 0:
                    value = jnp.where(lit[p], value, state[at, :])
                    result[s, pl.ds(p * SUB, SUB), :] = value
            return carry

        if sub < DAY_STEPS - 1:
            lax.fori_loop(0, species, finish, 0, unroll=8)
    for i in range(BATCHES):
        lax.fori_loop(i * batch, (i + 1) * batch, finish, 0, unroll=8)
        export(i).start()
    for i in range(BATCHES):
        export(i).wait()


VMEM = pl.BlockSpec(memory_space=pltpu.VMEM)
SMEM = pl.BlockSpec(memory_space=pltpu.SMEM)


def rows_of(count):
    return jax.ShapeDtypeStruct((count, LANES), jnp.float32)


ANY = pl.BlockSpec(memory_space=pl.ANY)
HBM = pl.BlockSpec(memory_space=pltpu.HBM)


def pack(z, part, *flat):
    extra = z.edge_rows if part == 0 else 0
    rows = [z.halo_rows + extra, z.halo_rows + extra, z.count * z.columns * z.rows]
    if part == 0:
        rows.append(3 * z.columns * z.rows)
    return pl.pallas_call(
        functools.partial(pack_kernel, z, part),
        out_shape=tuple(rows_of(n) for n in rows),
        in_specs=[VMEM] * len(flat),
        out_specs=(VMEM,) * len(rows),
        compiler_params=pltpu.CompilerParams(vmem_limit_bytes=16 << 20),
        cost_estimate=pl.CostEstimate(flops=100 * z.count * z.stride * LANES, bytes_accessed=0, transcendentals=0),
        name="pack",
    )(*flat)


def transport(z, slices, *flat):
    size = z.span * z.columns
    scratch = [6 * size, z.count * z.columns * z.rows, CHUNK * z.columns * z.rows]
    scratch += [2 * z.halo_rows, 2 * z.edge_rows] + [size] * (4 * TOGETHER)
    return pl.pallas_call(
        functools.partial(transport_kernel, z, slices),
        out_shape=(rows_of(z.count * z.blocks // slices),) * (z.groups * slices),
        in_specs=[VMEM] * len(flat),
        out_specs=(VMEM,) * (z.groups * slices),
        scratch_shapes=[pltpu.VMEM((n, LANES), jnp.float32) for n in scratch],
        compiler_params=pltpu.CompilerParams(vmem_limit_bytes=20 << 20),
        cost_estimate=pl.CostEstimate(flops=400 * z.count * z.stride * LANES, bytes_accessed=0, transcendentals=0),
        name="transport",
    )(*flat)


def rates(z, warm, glow, lit, rate, barrier, photo):
    reactions = rate.shape[0]
    return pl.pallas_call(
        functools.partial(rates_kernel, z.blocks // SUB),
        out_shape=rows_of(reactions * z.blocks),
        in_specs=[VMEM] * 3 + [SMEM] * 3,
        out_specs=VMEM,
        compiler_params=pltpu.CompilerParams(vmem_limit_bytes=16 << 20),
        cost_estimate=pl.CostEstimate(
            flops=40 * reactions * z.blocks * LANES, bytes_accessed=0, transcendentals=0
        ),
        name="rates",
    )(warm, glow, lit, rate, barrier, photo)


def chemistry(z, species, number, arrived, lit, k, table, out):
    size = species * z.slab
    more = () if out is None else (out,)
    args = (*arrived, lit, k, table, *more)
    scratch = [pltpu.VMEM((species, z.slab, LANES), jnp.float32)]
    scratch += [pltpu.VMEM((size, LANES), jnp.float32)] * 4 + [pltpu.SemaphoreType.DMA((BATCHES,))]
    return pl.pallas_call(
        functools.partial(chemistry_kernel, z, species, number),
        out_shape=jax.ShapeDtypeStruct((species, z.blocks, LANES), jnp.float32),
        in_specs=[VMEM] * (len(arrived) + 2) + [SMEM] + [ANY] * len(more),
        out_specs=ANY,
        scratch_shapes=scratch,
        input_output_aliases={len(args) - 1: 0} if more else {},
        compiler_params=pltpu.CompilerParams(vmem_limit_bytes=20 << 20),
        cost_estimate=pl.CostEstimate(flops=400 * size * LANES, bytes_accessed=0, transcendentals=0),
        name="chemistry",
    )(*args)


def body(
    mixing_ratio_field,
    eastward_face_cfl,
    northward_face_cfl,
    upward_face_cfl,
    thermal_anomaly,
    radiant_flux,
    daylight_mask,
    baseline_kinetic_coefficient,
    arrhenius_barrier,
    photodissociation_factor,
    stoichiometry_table,
):
    groups = lax.axis_size("tracer")
    strips = lax.axis_size("space")
    z = Sizes(mixing_ratio_field, groups)
    courant = flat_rows(jnp.stack([eastward_face_cfl, northward_face_cfl, upward_face_cfl]))
    field = flat_rows(mixing_ratio_field)
    near_pairs = [(i, i ^ 1) for i in range(strips) if i ^ 1 < strips]
    far_pairs = [(i, ((i + 1) ^ 1) - 1) for i in range(strips) if 0 <= ((i + 1) ^ 1) - 1 < strips]
    fields, halos = [], []
    for part in range(PARTS):
        if part == 0:
            near, far, ready, courant = pack(z, part, field, courant)
        else:
            field, _ = lax.optimization_barrier((field, ready))
            near, far, ready = pack(z, part, field)
        far = lax.ppermute(far, "space", far_pairs)
        near = lax.ppermute(near, "space", near_pairs)
        fields.append(ready)
        halos.append((near, far))
    edges = [halo[z.halo_rows :] for halo in halos[0]]
    arrived = [[] for _ in range(z.slices)]
    for part in range(PARTS):
        ready = fields[part]
        slices = z.slices if part == PARTS - 1 else 1
        if part > 0:
            ready, _ = lax.optimization_barrier((ready, moved[0]))
        moved = transport(z, slices, ready, courant, *edges, *halos[part])
        for piece in range(slices):
            for k in range(groups):
                block = moved[k * slices + piece]
                if k > 0:
                    block = lax.ppermute(block, "tracer", [(i, i ^ k) for i in range(groups)])
                for number in range(z.slices):
                    if slices == 1 or number == piece:
                        arrived[number].append(block)
    mask, table, _ = lax.optimization_barrier((daylight_mask, stoichiometry_table, moved[0]))
    lit = jnp.broadcast_to(jnp.moveaxis(mask, 2, 1).reshape(z.blocks, 1), (z.blocks, LANES))
    k = rates(
        z,
        flat_rows(thermal_anomaly),
        flat_rows(radiant_flux),
        lit,
        baseline_kinetic_coefficient,
        arrhenius_barrier,
        photodissociation_factor,
    )
    species = z.species * groups
    table = table.reshape(-1) * z.slab
    out = None
    for number in range(z.slices):
        out = chemistry(z, species, number, arrived[number], lit, k, table, out)
    out = out.reshape(species, z.levels, z.tiles, z.part, LANES)
    return jnp.moveaxis(out, 2, 3).reshape(species, z.levels, z.part, z.width)


def solution(mesh):
    placed = (
        P("tracer", None, "space", None),
        P(None, "space", None),
        P(None, "space", None),
        P(None, "space", None),
        P(None, ("space", "tracer"), None),
        P(None, ("space", "tracer"), None),
        P(None, ("space", "tracer"), None),
        P(),
        P(),
        P(),
        P(),
    )
    return jax.shard_map(
        body,
        mesh=mesh,
        in_specs=placed,
        out_specs=P(None, None, ("space", "tracer"), None),
        check_vma=False,
    )
```

```python
import functools

import jax
import jax.numpy as jnp
from jax import lax
from jax.experimental import pallas as pl
from jax.experimental.pallas import tpu as pltpu
from jax.sharding import PartitionSpec as P


SECTIONS = 3
DAY_STEPS = 2
LANES = 128
SUB = 8
LOW = 2 * SECTIONS
HIGH = SECTIONS
PARTS = 2
SPLIT_LEVELS = False
WAYS = 2
TOGETHER = 8
CHUNK = 8
BATCHES = 4
LOG2E = 1.4426950408889634


def flat_rows(cells):
    *lead, rows, width = cells.shape
    sub = min(rows, SUB)
    split = cells.reshape(*lead, rows // sub, sub, width // LANES, LANES)
    return jnp.moveaxis(split, -2, -3).reshape(-1, LANES)


class Sizes:
    def __init__(self, field, groups):
        self.species, self.levels, self.rows, self.width = field.shape
        self.tiles = self.width // LANES
        self.groups = groups
        self.part = self.rows // groups
        self.blocks = self.levels * self.tiles * self.part
        self.stride = self.levels * self.rows * self.tiles
        self.columns = self.levels * self.tiles
        self.count = self.species // PARTS
        self.area = self.tiles * self.part
        self.slices = self.levels if SPLIT_LEVELS and self.area % SUB == 0 else 1
        self.slab = self.blocks // self.slices
        self.halo_rows = LOW * self.columns * self.count
        self.span = self.rows + 2 * SUB
        self.edge_rows = 3 * self.columns * SUB

    def source_row(self, level, row, tile):
        return ((level * (self.rows // SUB) + row // SUB) * self.tiles + tile) * SUB + row % SUB

    def pairs(self):
        return [(level, tile) for level in range(self.levels) for tile in range(self.tiles)]


def middle(a, b):
    return jnp.maximum(jnp.minimum(a, b), jnp.minimum(jnp.maximum(a, b), 0.0))


def shift_columns(parts, amount):
    if amount > 0:
        return [pltpu.roll(parts[-1], 1, 1)] + parts[:-1]
    return parts[1:] + [pltpu.roll(parts[0], LANES - 1, 1)]


def spread_matrix(tiles, back):
    natural = lax.broadcasted_iota(jnp.int32, (tiles * LANES, tiles * LANES), 1 if back else 0)
    spread = lax.broadcasted_iota(jnp.int32, (tiles * LANES, tiles * LANES), 0 if back else 1)
    hit = natural == (spread % LANES) * tiles + spread // LANES
    return jnp.where(hit, 1.0, 0.0).astype(jnp.bfloat16)


def reorder(parts, matrix):
    x = jnp.concatenate(parts, axis=1)
    total = None
    for _ in range(3):
        piece = x.astype(jnp.bfloat16)
        x = x - piece.astype(jnp.float32)
        term = jnp.dot(piece, matrix, preferred_element_type=jnp.float32)
        total = term if total is None else total + term
    return [total[:, k * LANES : (k + 1) * LANES] for k in range(len(parts))]


def pack_kernel(z, part, x_ref, *refs):
    forth = spread_matrix(z.tiles, False)
    if part == 0:
        courant_ref, near_ref, far_ref, field, courant_out = refs
    else:
        near_ref, far_ref, field = refs
    odd = lax.rem(lax.axis_index("space"), 2)
    sides = ((near_ref, odd), (far_ref, 1 - odd))

    def spread(flat, strips):
        split = flat.reshape(strips, z.rows // SUB, z.tiles, SUB, LANES)
        return reorder([split[:, :, t].reshape(strips * z.rows, LANES) for t in range(z.tiles)], forth)

    if part == 0:
        parts = spread(courant_ref[...], 3 * z.levels)
        shifted = shift_columns(parts, -1)
        for strip in range(3 * z.levels):
            rows = slice(strip * z.rows, (strip + 1) * z.rows)
            for tile in range(z.tiles):
                value = (shifted if strip // z.levels == 1 else parts)[tile][rows]
                col = strip * z.tiles + tile
                courant_out[pl.ds(col * z.rows, z.rows), :] = value

    def some(index, carry):
        strips = CHUNK * z.levels
        size = strips * z.tiles * z.rows
        start = pl.multiple_of((part * (z.count // CHUNK) + index) * size, SUB)
        values = spread(x_ref[pl.ds(start, size), :], strips)
        for strip in range(strips):
            for tile in range(z.tiles):
                at = pl.multiple_of(index * size + (strip * z.tiles + tile) * z.rows, SUB)
                field[pl.ds(at, z.rows), :] = values[tile][strip * z.rows : (strip + 1) * z.rows]
        return carry

    lax.fori_loop(0, z.count // CHUNK, some, 0)

    if part == 0:
        for ref, below in sides:
            for col in range(3 * z.columns):
                source = col * z.rows + (1 - below) * (z.rows - SUB)
                ref[pl.ds(z.halo_rows + col * SUB, SUB), :] = courant_out[pl.ds(pl.multiple_of(source, SUB), SUB), :]

    def edges(index, carry):
        for ref, below in sides:
            for col in range(z.columns):
                target = index * z.columns + col
                source = target * z.rows + (1 - below) * (z.rows - LOW)
                ref[pl.ds(target * LOW, LOW), :] = field[pl.ds(source, LOW), :]
        return carry

    lax.fori_loop(0, z.count, edges, 0, unroll=4)


def transport_kernel(z, slices, field_ref, courant_ref, near_edge, far_edge, near_ref, far_ref, *refs):
    span = z.span
    cols = range(z.columns)
    total = z.groups * slices
    outs, (coef, final, natural, halo, edge), slots = refs[:total], refs[total : total + 5], refs[total + 5 :]
    odd = lax.rem(lax.axis_index("space"), 2)
    for source, above in ((near_ref, 1 - odd), (far_ref, odd)):

        def place_halo(i, carry):
            target = pl.multiple_of(above * z.halo_rows + i * SUB, SUB)
            halo[pl.ds(target, SUB), :] = source[pl.ds(pl.multiple_of(i * SUB, SUB), SUB), :]
            return carry

        lax.fori_loop(0, z.halo_rows // SUB, place_halo, 0, unroll=12)
    for source, above in ((near_edge, 1 - odd), (far_edge, odd)):
        for row in range(0, z.edge_rows, SUB):
            target = pl.multiple_of(above * z.edge_rows + row, SUB)
            edge[pl.ds(target, SUB), :] = source[pl.ds(row, SUB), :]

    def coef_row(kind, which, col, j):
        return ((kind * 2 + which) * z.columns + col) * span + j

    for kind in range(3):
        for col in cols:
            one = kind * z.columns + col
            tiles = [edge[pl.ds(one * SUB, SUB), :]]
            tiles += [courant_ref[pl.ds(one * z.rows + row, SUB), :] for row in range(0, z.rows, SUB)]
            tiles += [edge[pl.ds(z.edge_rows + one * SUB, SUB), :]]
            for k, value in enumerate(tiles):
                coef[pl.ds(coef_row(kind, 0, col, k * SUB), SUB), :] = value
                coef[pl.ds(coef_row(kind, 1, col, k * SUB), SUB), :] = 0.5 * value * (1.0 - value)

    def weights(kind, col, j):
        return [coef[pl.ds(coef_row(kind, which, col, j), SUB), :] for which in range(2)]

    def one_species(index, start, fields, fluxes):
        for col in cols:
            base = index * z.columns + col
            at = col * span + SUB
            start[pl.ds(at - LOW, LOW), :] = halo[pl.ds(base * LOW, LOW), :]
            start[pl.ds(at + z.rows, HIGH), :] = halo[pl.ds(z.halo_rows + base * LOW, HIGH), :]
            start[pl.ds(at, z.rows), :] = field_ref[pl.ds(pl.multiple_of(base * z.rows, SUB), z.rows), :]
        for step in range(SECTIONS):
            write = fields[step % 2]
            source = start if step == 0 else fields[(step + 1) % 2]
            read = lambda col, j, ref=source: ref[pl.ds(col * span + j, SUB), :]
            bottom = SUB - LOW + 2 * (step + 1)
            top = SUB + z.rows + HIGH - (step + 1)
            for j in range(bottom - 1, top, SUB):
                for col in cols:
                    below, here, above = [read(col, j + k) for k in (-1, 0, 1)]
                    a, b = weights(0, col, j + 1)
                    fluxes[pl.ds(col * span + j, SUB), :] = a * here + b * middle(here - below, above - here)
            for j in range(bottom, top, SUB):
                c = []
                for col in cols:
                    leave = fluxes[pl.ds(col * span + j, SUB), :]
                    enter = fluxes[pl.ds(col * span + j - 1, SUB), :]
                    c.append(read(col, j) - (leave - enter))
                for level in range(z.levels):
                    mine = slice(level * z.tiles, (level + 1) * z.tiles)
                    row = c[mine]
                    back = [v - w for v, w in zip(row, shift_columns(row, 1))]
                    ahead = shift_columns(back, -1)
                    leave = []
                    for tile in range(z.tiles):
                        a, b = weights(1, level * z.tiles + tile, j)
                        leave.append(a * row[tile] + b * middle(back[tile], ahead[tile]))
                    enter = shift_columns(leave, 1)
                    c[mine] = [row[t] - (leave[t] - enter[t]) for t in range(z.tiles)]
                for tile in range(z.tiles):
                    column = [c[level * z.tiles + tile] for level in range(z.levels)]
                    steps = [column[0]]
                    steps += [column[k + 1] - column[k] for k in range(z.levels - 1)]
                    steps += [-column[-1]]
                    lift = None
                    for level in range(z.levels):
                        col = level * z.tiles + tile
                        a, b = weights(2, col, j)
                        rising = a * column[level] + b * middle(steps[level], steps[level + 1])
                        net = rising if lift is None else rising - lift
                        lift = rising
                        value = column[level] - net
                        if step < SECTIONS - 1:
                            write[pl.ds(col * span + j, SUB), :] = value
                        else:
                            base = (index * z.columns + col) * z.rows + j - SUB
                            final[pl.ds(pl.multiple_of(base, SUB), SUB), :] = value

    def some_species(index, carry):
        for k in range(TOGETHER):
            one_species(index * TOGETHER + k, slots[4 * k], slots[4 * k + 1 : 4 * k + 3], slots[4 * k + 3])
        return carry

    lax.fori_loop(0, z.count // TOGETHER, some_species, 0)

    back = spread_matrix(z.tiles, True)
    me = lax.axis_index("tracer")

    def scatter(index, carry):
        many = CHUNK * z.levels
        size = many * z.tiles * z.rows
        whole = final[pl.ds(pl.multiple_of(index * size, SUB), size), :].reshape(many, z.tiles, z.rows, LANES)
        parts = reorder([whole[:, t].reshape(many * z.rows, LANES) for t in range(z.tiles)], back)
        for one in range(many):
            for tile in range(z.tiles):
                strip = one * z.tiles + tile
                natural[pl.ds(strip * z.rows, z.rows), :] = parts[tile][one * z.rows : (one + 1) * z.rows]
        share = z.columns // slices
        for k in range(z.groups):
            first = (me ^ k) * z.part
            for strip in range(many * z.tiles):
                one, col = divmod(strip, z.columns)
                out_ref = outs[k * slices + col // share]
                at = ((index * CHUNK + one) * share + col % share) * z.part
                out_ref[pl.ds(at, z.part), :] = natural[pl.ds(strip * z.rows + first, z.part), :]
        return carry

    lax.fori_loop(0, z.count // CHUNK, scatter, 0)


def rates_kernel(pieces, warm_ref, glow_ref, lit_ref, rate_ref, barrier_ref, photo_ref, out_ref):
    warm = [(1.0 - warm_ref[pl.ds(p * SUB, SUB), :]) * LOG2E for p in range(pieces)]
    glow = [
        jnp.where(lit_ref[pl.ds(p * SUB, SUB), :] == 1, glow_ref[pl.ds(p * SUB, SUB), :], 0.0)
        for p in range(pieces)
    ]

    def one(r, carry):
        for p in range(pieces):
            at = pl.ds(pl.multiple_of(r * pieces * SUB, SUB) + p * SUB, SUB)
            out_ref[at, :] = rate_ref[r] * jnp.exp2(barrier_ref[r] * warm[p]) + photo_ref[r] * glow[p]
        return carry

    lax.fori_loop(0, rate_ref.shape[0], one, 0, unroll=8)


def chemistry_kernel(z, species, number, *refs):
    pieces = z.slab // SUB
    total = PARTS * z.groups
    sources, (lit_ref, k_ref, table_ref) = refs[:total], refs[total : total + 3]
    out_hbm, result, state = refs[total + 3 + (number > 0) :][:3]
    made, lost_a, lost_b = [refs[-1 - (3 - i) * WAYS :][:WAYS] for i in range(3)]
    sems = refs[-1]
    reactions = k_ref.shape[0] // z.blocks
    base = number * z.slab

    def cell(row, piece):
        return pl.ds(pl.multiple_of(row, SUB) + piece * SUB, SUB)

    lit = [lit_ref[pl.ds(base + p * SUB, SUB), :] == 1 for p in range(pieces)]
    steps = [jnp.where(lit[p], float(DAY_STEPS), 1.0) for p in range(pieces)]
    zero = jnp.zeros((SUB, LANES), jnp.float32)
    me = lax.axis_index("tracer")

    def prepare(at, p, value):
        for way in range(WAYS):
            made[way][at, :] = zero if way else steps[p] * value
            lost_a[way][at, :] = zero if way else steps[p]
            lost_b[way][at, :] = zero

    def begin(index, carry):
        for i, ref in enumerate(sources):
            part, k = divmod(i, z.groups)
            first = (me ^ k) * z.species + part * z.count
            for p in range(pieces):
                if part < PARTS - 1:
                    value = ref[cell(index * z.blocks + base, p), :]
                else:
                    value = ref[cell(index * z.slab, p), :]
                at = cell((first + index) * z.slab, p)
                state[at, :] = value
                prepare(at, p, value)
        return carry

    lax.fori_loop(0, z.count, begin, 0)

    def react(r, way):
        first, second, product = table_ref[r], table_ref[reactions + r], table_ref[2 * reactions + r]
        for p in range(pieces):
            k = k_ref[cell(r * z.blocks + base, p), :]
            x = state[cell(first, p), :]
            y = state[cell(second, p), :]
            kx = k * x
            ky = k * y
            made[way][cell(product, p), :] += kx * y
            lost_a[way][cell(first, p), :] += ky
            lost_b[way][cell(second, p), :] += kx

    def several(i, carry):
        for way in range(WAYS):
            react(i * WAYS + way, way)
        return carry

    batch = species // BATCHES

    def export(i):
        rows = pl.ds(i * batch, batch)
        return pltpu.make_async_copy(result.at[rows], out_hbm.at[rows, pl.ds(base, z.slab)], sems.at[i])

    for sub in range(DAY_STEPS):
        lax.fori_loop(0, reactions // WAYS, several, 0, unroll=16 // WAYS)

        def finish(s, carry):
            for p in range(pieces):
                at = cell(s * z.slab, p)
                top = sum(ref[at, :] for ref in made)
                value = top / sum(ref[at, :] for ref in (*lost_a, *lost_b))
                if sub < DAY_STEPS - 1:
                    prepare(at, p, value)
                    if sub == 0:
                        state[at, :] = value
                if sub > 0:
                    value = jnp.where(lit[p], value, state[at, :])
                    result[s, pl.ds(p * SUB, SUB), :] = value
            return carry

        if sub < DAY_STEPS - 1:
            lax.fori_loop(0, species, finish, 0, unroll=8)
    for i in range(BATCHES):
        lax.fori_loop(i * batch, (i + 1) * batch, finish, 0, unroll=8)
        export(i).start()
    for i in range(BATCHES):
        export(i).wait()


VMEM = pl.BlockSpec(memory_space=pltpu.VMEM)
SMEM = pl.BlockSpec(memory_space=pltpu.SMEM)


def rows_of(count):
    return jax.ShapeDtypeStruct((count, LANES), jnp.float32)


ANY = pl.BlockSpec(memory_space=pl.ANY)
HBM = pl.BlockSpec(memory_space=pltpu.HBM)


def pack(z, part, *flat):
    extra = z.edge_rows if part == 0 else 0
    rows = [z.halo_rows + extra, z.halo_rows + extra, z.count * z.columns * z.rows]
    if part == 0:
        rows.append(3 * z.columns * z.rows)
    return pl.pallas_call(
        functools.partial(pack_kernel, z, part),
        out_shape=tuple(rows_of(n) for n in rows),
        in_specs=[VMEM] * len(flat),
        out_specs=(VMEM,) * len(rows),
        compiler_params=pltpu.CompilerParams(vmem_limit_bytes=16 << 20),
        cost_estimate=pl.CostEstimate(flops=100 * z.count * z.stride * LANES, bytes_accessed=0, transcendentals=0),
        name="pack",
    )(*flat)


def transport(z, slices, *flat):
    size = z.span * z.columns
    scratch = [6 * size, z.count * z.columns * z.rows, CHUNK * z.columns * z.rows]
    scratch += [2 * z.halo_rows, 2 * z.edge_rows] + [size] * (4 * TOGETHER)
    return pl.pallas_call(
        functools.partial(transport_kernel, z, slices),
        out_shape=(rows_of(z.count * z.blocks // slices),) * (z.groups * slices),
        in_specs=[VMEM] * len(flat),
        out_specs=(VMEM,) * (z.groups * slices),
        scratch_shapes=[pltpu.VMEM((n, LANES), jnp.float32) for n in scratch],
        compiler_params=pltpu.CompilerParams(vmem_limit_bytes=20 << 20),
        cost_estimate=pl.CostEstimate(flops=400 * z.count * z.stride * LANES, bytes_accessed=0, transcendentals=0),
        name="transport",
    )(*flat)


def rates(z, warm, glow, lit, rate, barrier, photo):
    reactions = rate.shape[0]
    return pl.pallas_call(
        functools.partial(rates_kernel, z.blocks // SUB),
        out_shape=rows_of(reactions * z.blocks),
        in_specs=[VMEM] * 3 + [SMEM] * 3,
        out_specs=VMEM,
        compiler_params=pltpu.CompilerParams(vmem_limit_bytes=16 << 20),
        cost_estimate=pl.CostEstimate(
            flops=40 * reactions * z.blocks * LANES, bytes_accessed=0, transcendentals=0
        ),
        name="rates",
    )(warm, glow, lit, rate, barrier, photo)


def chemistry(z, species, number, arrived, lit, k, table, out):
    size = species * z.slab
    more = () if out is None else (out,)
    args = (*arrived, lit, k, table, *more)
    scratch = [pltpu.VMEM((species, z.slab, LANES), jnp.float32)]
    scratch += [pltpu.VMEM((size, LANES), jnp.float32)] * (1 + 3 * WAYS) + [pltpu.SemaphoreType.DMA((BATCHES,))]
    return pl.pallas_call(
        functools.partial(chemistry_kernel, z, species, number),
        out_shape=jax.ShapeDtypeStruct((species, z.blocks, LANES), jnp.float32),
        in_specs=[VMEM] * (len(arrived) + 2) + [SMEM] + [ANY] * len(more),
        out_specs=ANY,
        scratch_shapes=scratch,
        input_output_aliases={len(args) - 1: 0} if more else {},
        compiler_params=pltpu.CompilerParams(vmem_limit_bytes=28 << 20),
        cost_estimate=pl.CostEstimate(flops=400 * size * LANES, bytes_accessed=0, transcendentals=0),
        name="chemistry",
    )(*args)


def body(
    mixing_ratio_field,
    eastward_face_cfl,
    northward_face_cfl,
    upward_face_cfl,
    thermal_anomaly,
    radiant_flux,
    daylight_mask,
    baseline_kinetic_coefficient,
    arrhenius_barrier,
    photodissociation_factor,
    stoichiometry_table,
):
    groups = lax.axis_size("tracer")
    strips = lax.axis_size("space")
    z = Sizes(mixing_ratio_field, groups)
    courant = flat_rows(jnp.stack([eastward_face_cfl, northward_face_cfl, upward_face_cfl]))
    field = flat_rows(mixing_ratio_field)
    near_pairs = [(i, i ^ 1) for i in range(strips) if i ^ 1 < strips]
    far_pairs = [(i, ((i + 1) ^ 1) - 1) for i in range(strips) if 0 <= ((i + 1) ^ 1) - 1 < strips]
    fields, halos = [], []
    for part in range(PARTS):
        if part == 0:
            near, far, ready, courant = pack(z, part, field, courant)
        else:
            field, _ = lax.optimization_barrier((field, ready))
            near, far, ready = pack(z, part, field)
        far = lax.ppermute(far, "space", far_pairs)
        near = lax.ppermute(near, "space", near_pairs)
        fields.append(ready)
        halos.append((near, far))
    edges = [halo[z.halo_rows :] for halo in halos[0]]
    arrived = [[] for _ in range(z.slices)]
    for part in range(PARTS):
        ready = fields[part]
        slices = z.slices if part == PARTS - 1 else 1
        if part > 0:
            ready, _ = lax.optimization_barrier((ready, moved[0]))
        moved = transport(z, slices, ready, courant, *edges, *halos[part])
        for piece in range(slices):
            for k in range(groups):
                block = moved[k * slices + piece]
                if k > 0:
                    block = lax.ppermute(block, "tracer", [(i, i ^ k) for i in range(groups)])
                for number in range(z.slices):
                    if slices == 1 or number == piece:
                        arrived[number].append(block)
    mask, table, _ = lax.optimization_barrier((daylight_mask, stoichiometry_table, moved[0]))
    lit = jnp.broadcast_to(jnp.moveaxis(mask, 2, 1).reshape(z.blocks, 1), (z.blocks, LANES))
    k = rates(
        z,
        flat_rows(thermal_anomaly),
        flat_rows(radiant_flux),
        lit,
        baseline_kinetic_coefficient,
        arrhenius_barrier,
        photodissociation_factor,
    )
    species = z.species * groups
    table = table.reshape(-1) * z.slab
    out = None
    for number in range(z.slices):
        out = chemistry(z, species, number, arrived[number], lit, k, table, out)
    out = out.reshape(species, z.levels, z.tiles, z.part, LANES)
    return jnp.moveaxis(out, 2, 3).reshape(species, z.levels, z.part, z.width)


def solution(mesh):
    placed = (
        P("tracer", None, "space", None),
        P(None, "space", None),
        P(None, "space", None),
        P(None, "space", None),
        P(None, ("space", "tracer"), None),
        P(None, ("space", "tracer"), None),
        P(None, ("space", "tracer"), None),
        P(),
        P(),
        P(),
        P(),
    )
    return jax.shard_map(
        body,
        mesh=mesh,
        in_specs=placed,
        out_specs=P(None, None, ("space", "tracer"), None),
        check_vma=False,
    )
```

```python
import functools

import jax
import jax.numpy as jnp
from jax import lax
from jax.experimental import pallas as pl
from jax.experimental.pallas import tpu as pltpu
from jax.sharding import PartitionSpec as P


SECTIONS = 3
DAY_STEPS = 2
LANES = 128
SUB = 8
LOW = 2 * SECTIONS
HIGH = SECTIONS
PARTS = 2
SPLIT_LEVELS = False
WAYS = 2
TOGETHER = 8
CHUNK = 8
BATCHES = 4
LOG2E = 1.4426950408889634


def flat_rows(cells):
    *lead, rows, width = cells.shape
    sub = min(rows, SUB)
    split = cells.reshape(*lead, rows // sub, sub, width // LANES, LANES)
    return jnp.moveaxis(split, -2, -3).reshape(-1, LANES)


class Sizes:
    def __init__(self, field, groups):
        self.species, self.levels, self.rows, self.width = field.shape
        self.tiles = self.width // LANES
        self.groups = groups
        self.part = self.rows // groups
        self.blocks = self.levels * self.tiles * self.part
        self.stride = self.levels * self.rows * self.tiles
        self.columns = self.levels * self.tiles
        self.count = self.species // PARTS
        self.area = self.tiles * self.part
        self.slices = self.levels if SPLIT_LEVELS and self.area % SUB == 0 else 1
        self.slab = self.blocks // self.slices
        self.halo_rows = LOW * self.columns * self.count
        self.span = self.rows + 2 * SUB
        self.edge_rows = 3 * self.columns * SUB

    def source_row(self, level, row, tile):
        return ((level * (self.rows // SUB) + row // SUB) * self.tiles + tile) * SUB + row % SUB

    def pairs(self):
        return [(level, tile) for level in range(self.levels) for tile in range(self.tiles)]


def middle(a, b):
    return jnp.maximum(jnp.minimum(a, b), jnp.minimum(jnp.maximum(a, b), 0.0))


def shift_columns(parts, amount):
    if amount > 0:
        return [pltpu.roll(parts[-1], 1, 1)] + parts[:-1]
    return parts[1:] + [pltpu.roll(parts[0], LANES - 1, 1)]


def spread_matrix(tiles, back):
    natural = lax.broadcasted_iota(jnp.int32, (tiles * LANES, tiles * LANES), 1 if back else 0)
    spread = lax.broadcasted_iota(jnp.int32, (tiles * LANES, tiles * LANES), 0 if back else 1)
    hit = natural == (spread % LANES) * tiles + spread // LANES
    return jnp.where(hit, 1.0, 0.0).astype(jnp.bfloat16)


def reorder(parts, matrix):
    x = jnp.concatenate(parts, axis=1)
    total = None
    for _ in range(3):
        piece = x.astype(jnp.bfloat16)
        x = x - piece.astype(jnp.float32)
        term = jnp.dot(piece, matrix, preferred_element_type=jnp.float32)
        total = term if total is None else total + term
    return [total[:, k * LANES : (k + 1) * LANES] for k in range(len(parts))]


def pack_kernel(z, part, x_ref, *refs):
    forth = spread_matrix(z.tiles, False)
    if part == 0:
        courant_ref, near_ref, far_ref, field, courant_out = refs
    else:
        near_ref, far_ref, field = refs
    odd = lax.rem(lax.axis_index("space"), 2)
    sides = ((near_ref, odd), (far_ref, 1 - odd))

    def spread(flat, strips):
        split = flat.reshape(strips, z.rows // SUB, z.tiles, SUB, LANES)
        return reorder([split[:, :, t].reshape(strips * z.rows, LANES) for t in range(z.tiles)], forth)

    if part == 0:
        parts = spread(courant_ref[...], 3 * z.levels)
        shifted = shift_columns(parts, -1)
        for strip in range(3 * z.levels):
            rows = slice(strip * z.rows, (strip + 1) * z.rows)
            for tile in range(z.tiles):
                value = (shifted if strip // z.levels == 1 else parts)[tile][rows]
                col = strip * z.tiles + tile
                courant_out[pl.ds(col * z.rows, z.rows), :] = value

    def some(index, carry):
        strips = CHUNK * z.levels
        size = strips * z.tiles * z.rows
        values = spread(x_ref[pl.ds(pl.multiple_of(index * size, SUB), size), :], strips)
        for strip in range(strips):
            for tile in range(z.tiles):
                at = pl.multiple_of(index * size + (strip * z.tiles + tile) * z.rows, SUB)
                field[pl.ds(at, z.rows), :] = values[tile][strip * z.rows : (strip + 1) * z.rows]
        return carry

    lax.fori_loop(0, z.count // CHUNK, some, 0)

    if part == 0:
        for ref, below in sides:
            for col in range(3 * z.columns):
                source = col * z.rows + (1 - below) * (z.rows - SUB)
                ref[pl.ds(z.halo_rows + col * SUB, SUB), :] = courant_out[pl.ds(pl.multiple_of(source, SUB), SUB), :]

    def edges(index, carry):
        for ref, below in sides:
            for col in range(z.columns):
                target = index * z.columns + col
                source = target * z.rows + (1 - below) * (z.rows - LOW)
                ref[pl.ds(target * LOW, LOW), :] = field[pl.ds(source, LOW), :]
        return carry

    lax.fori_loop(0, z.count, edges, 0, unroll=4)


def transport_kernel(z, slices, field_ref, courant_ref, near_edge, far_edge, near_ref, far_ref, *refs):
    span = z.span
    cols = range(z.columns)
    total = z.groups * slices
    outs, (coef, final, natural, halo, edge), slots = refs[:total], refs[total : total + 5], refs[total + 5 :]
    odd = lax.rem(lax.axis_index("space"), 2)
    for source, above in ((near_ref, 1 - odd), (far_ref, odd)):

        def place_halo(i, carry):
            target = pl.multiple_of(above * z.halo_rows + i * SUB, SUB)
            halo[pl.ds(target, SUB), :] = source[pl.ds(pl.multiple_of(i * SUB, SUB), SUB), :]
            return carry

        lax.fori_loop(0, z.halo_rows // SUB, place_halo, 0, unroll=12)
    for source, above in ((near_edge, 1 - odd), (far_edge, odd)):
        for row in range(0, z.edge_rows, SUB):
            target = pl.multiple_of(above * z.edge_rows + row, SUB)
            edge[pl.ds(target, SUB), :] = source[pl.ds(row, SUB), :]

    def coef_row(kind, which, col, j):
        return ((kind * 2 + which) * z.columns + col) * span + j

    for kind in range(3):
        for col in cols:
            one = kind * z.columns + col
            tiles = [edge[pl.ds(one * SUB, SUB), :]]
            tiles += [courant_ref[pl.ds(one * z.rows + row, SUB), :] for row in range(0, z.rows, SUB)]
            tiles += [edge[pl.ds(z.edge_rows + one * SUB, SUB), :]]
            for k, value in enumerate(tiles):
                coef[pl.ds(coef_row(kind, 0, col, k * SUB), SUB), :] = value
                coef[pl.ds(coef_row(kind, 1, col, k * SUB), SUB), :] = 0.5 * value * (1.0 - value)

    def weights(kind, col, j):
        return [coef[pl.ds(coef_row(kind, which, col, j), SUB), :] for which in range(2)]

    def one_species(index, start, fields, fluxes):
        for col in cols:
            base = index * z.columns + col
            at = col * span + SUB
            start[pl.ds(at - LOW, LOW), :] = halo[pl.ds(base * LOW, LOW), :]
            start[pl.ds(at + z.rows, HIGH), :] = halo[pl.ds(z.halo_rows + base * LOW, HIGH), :]
            start[pl.ds(at, z.rows), :] = field_ref[pl.ds(pl.multiple_of(base * z.rows, SUB), z.rows), :]
        for step in range(SECTIONS):
            write = fields[step % 2]
            source = start if step == 0 else fields[(step + 1) % 2]
            read = lambda col, j, ref=source: ref[pl.ds(col * span + j, SUB), :]
            bottom = SUB - LOW + 2 * (step + 1)
            top = SUB + z.rows + HIGH - (step + 1)
            for j in range(bottom - 1, top, SUB):
                for col in cols:
                    below, here, above = [read(col, j + k) for k in (-1, 0, 1)]
                    a, b = weights(0, col, j + 1)
                    fluxes[pl.ds(col * span + j, SUB), :] = a * here + b * middle(here - below, above - here)
            for j in range(bottom, top, SUB):
                c = []
                for col in cols:
                    leave = fluxes[pl.ds(col * span + j, SUB), :]
                    enter = fluxes[pl.ds(col * span + j - 1, SUB), :]
                    c.append(read(col, j) - (leave - enter))
                for level in range(z.levels):
                    mine = slice(level * z.tiles, (level + 1) * z.tiles)
                    row = c[mine]
                    back = [v - w for v, w in zip(row, shift_columns(row, 1))]
                    ahead = shift_columns(back, -1)
                    leave = []
                    for tile in range(z.tiles):
                        a, b = weights(1, level * z.tiles + tile, j)
                        leave.append(a * row[tile] + b * middle(back[tile], ahead[tile]))
                    enter = shift_columns(leave, 1)
                    c[mine] = [row[t] - (leave[t] - enter[t]) for t in range(z.tiles)]
                for tile in range(z.tiles):
                    column = [c[level * z.tiles + tile] for level in range(z.levels)]
                    steps = [column[0]]
                    steps += [column[k + 1] - column[k] for k in range(z.levels - 1)]
                    steps += [-column[-1]]
                    lift = None
                    for level in range(z.levels):
                        col = level * z.tiles + tile
                        a, b = weights(2, col, j)
                        rising = a * column[level] + b * middle(steps[level], steps[level + 1])
                        net = rising if lift is None else rising - lift
                        lift = rising
                        value = column[level] - net
                        if step < SECTIONS - 1:
                            write[pl.ds(col * span + j, SUB), :] = value
                        else:
                            base = (index * z.columns + col) * z.rows + j - SUB
                            final[pl.ds(pl.multiple_of(base, SUB), SUB), :] = value

    def some_species(index, carry):
        for k in range(TOGETHER):
            one_species(index * TOGETHER + k, slots[4 * k], slots[4 * k + 1 : 4 * k + 3], slots[4 * k + 3])
        return carry

    lax.fori_loop(0, z.count // TOGETHER, some_species, 0)

    back = spread_matrix(z.tiles, True)
    me = lax.axis_index("tracer")

    def scatter(index, carry):
        many = CHUNK * z.levels
        size = many * z.tiles * z.rows
        whole = final[pl.ds(pl.multiple_of(index * size, SUB), size), :].reshape(many, z.tiles, z.rows, LANES)
        parts = reorder([whole[:, t].reshape(many * z.rows, LANES) for t in range(z.tiles)], back)
        for one in range(many):
            for tile in range(z.tiles):
                strip = one * z.tiles + tile
                natural[pl.ds(strip * z.rows, z.rows), :] = parts[tile][one * z.rows : (one + 1) * z.rows]
        share = z.columns // slices
        for k in range(z.groups):
            first = (me ^ k) * z.part
            for strip in range(many * z.tiles):
                one, col = divmod(strip, z.columns)
                out_ref = outs[k * slices + col // share]
                at = ((index * CHUNK + one) * share + col % share) * z.part
                out_ref[pl.ds(at, z.part), :] = natural[pl.ds(strip * z.rows + first, z.part), :]
        return carry

    lax.fori_loop(0, z.count // CHUNK, scatter, 0)


def rates_kernel(pieces, warm_ref, glow_ref, lit_ref, rate_ref, barrier_ref, photo_ref, out_ref):
    warm = [(1.0 - warm_ref[pl.ds(p * SUB, SUB), :]) * LOG2E for p in range(pieces)]
    glow = [
        jnp.where(lit_ref[pl.ds(p * SUB, SUB), :] == 1, glow_ref[pl.ds(p * SUB, SUB), :], 0.0)
        for p in range(pieces)
    ]

    def one(r, carry):
        for p in range(pieces):
            at = pl.ds(pl.multiple_of(r * pieces * SUB, SUB) + p * SUB, SUB)
            out_ref[at, :] = rate_ref[r] * jnp.exp2(barrier_ref[r] * warm[p]) + photo_ref[r] * glow[p]
        return carry

    lax.fori_loop(0, rate_ref.shape[0], one, 0, unroll=8)


def chemistry_kernel(z, species, number, *refs):
    pieces = z.slab // SUB
    total = PARTS * z.groups
    sources, (lit_ref, k_ref, table_in) = refs[:total], refs[total : total + 3]
    out_hbm, result, state = refs[total + 3 + (number > 0) :][:3]
    made, lost_a, lost_b = [refs[-1 - (3 - i) * WAYS :][:WAYS] for i in range(3)]
    sems = refs[-1]
    table_ref = refs[-2 - 3 * WAYS]
    table_load = pltpu.make_async_copy(table_in, table_ref, sems.at[BATCHES])
    table_load.start()
    reactions = k_ref.shape[0] // z.blocks
    base = number * z.slab

    def cell(row, piece):
        return pl.ds(pl.multiple_of(row, SUB) + piece * SUB, SUB)

    lit = [lit_ref[pl.ds(base + p * SUB, SUB), :] == 1 for p in range(pieces)]
    steps = [jnp.where(lit[p], float(DAY_STEPS), 1.0) for p in range(pieces)]
    zero = jnp.zeros((SUB, LANES), jnp.float32)
    me = lax.axis_index("tracer")

    def prepare(at, p, value):
        for way in range(WAYS):
            made[way][at, :] = zero if way else steps[p] * value
            lost_a[way][at, :] = zero if way else steps[p]
            lost_b[way][at, :] = zero

    def begin(index, carry):
        for i, ref in enumerate(sources):
            part, k = divmod(i, z.groups)
            first = (me ^ k) * z.species + part * z.count
            for p in range(pieces):
                if part < PARTS - 1:
                    value = ref[cell(index * z.blocks + base, p), :]
                else:
                    value = ref[cell(index * z.slab, p), :]
                at = cell((first + index) * z.slab, p)
                state[at, :] = value
                prepare(at, p, value)
        return carry

    lax.fori_loop(0, z.count, begin, 0)

    table_load.wait()

    def react(r, way):
        first, second, product = table_ref[r], table_ref[reactions + r], table_ref[2 * reactions + r]
        for p in range(pieces):
            k = k_ref[cell(r * z.blocks + base, p), :]
            x = state[cell(first, p), :]
            y = state[cell(second, p), :]
            kx = k * x
            ky = k * y
            made[way][cell(product, p), :] += kx * y
            lost_a[way][cell(first, p), :] += ky
            lost_b[way][cell(second, p), :] += kx

    def several(i, carry):
        for way in range(WAYS):
            react(i * WAYS + way, way)
        return carry

    batch = species // BATCHES

    def export(i):
        rows = pl.ds(i * batch, batch)
        return pltpu.make_async_copy(result.at[rows], out_hbm.at[rows, pl.ds(base, z.slab)], sems.at[i])

    for sub in range(DAY_STEPS):
        lax.fori_loop(0, reactions // WAYS, several, 0, unroll=16 // WAYS)

        def finish(s, carry):
            for p in range(pieces):
                at = cell(s * z.slab, p)
                top = sum(ref[at, :] for ref in made)
                value = top / sum(ref[at, :] for ref in (*lost_a, *lost_b))
                if sub < DAY_STEPS - 1:
                    prepare(at, p, value)
                    if sub == 0:
                        state[at, :] = value
                if sub > 0:
                    value = jnp.where(lit[p], value, state[at, :])
                    result[s, pl.ds(p * SUB, SUB), :] = value
            return carry

        if sub < DAY_STEPS - 1:
            lax.fori_loop(0, species, finish, 0, unroll=8)
    for i in range(BATCHES):
        lax.fori_loop(i * batch, (i + 1) * batch, finish, 0, unroll=8)
        export(i).start()
    for i in range(BATCHES):
        export(i).wait()


VMEM = pl.BlockSpec(memory_space=pltpu.VMEM)
SMEM = pl.BlockSpec(memory_space=pltpu.SMEM)


def rows_of(count):
    return jax.ShapeDtypeStruct((count, LANES), jnp.float32)


ANY = pl.BlockSpec(memory_space=pl.ANY)
HBM = pl.BlockSpec(memory_space=pltpu.HBM)


def pack(z, part, *flat):
    extra = z.edge_rows if part == 0 else 0
    rows = [z.halo_rows + extra, z.halo_rows + extra, z.count * z.columns * z.rows]
    if part == 0:
        rows.append(3 * z.columns * z.rows)
    return pl.pallas_call(
        functools.partial(pack_kernel, z, part),
        out_shape=tuple(rows_of(n) for n in rows),
        in_specs=[VMEM] * len(flat),
        out_specs=(VMEM,) * len(rows),
        compiler_params=pltpu.CompilerParams(vmem_limit_bytes=16 << 20),
        cost_estimate=pl.CostEstimate(flops=100 * z.count * z.stride * LANES, bytes_accessed=0, transcendentals=0),
        name="pack",
    )(*flat)


def transport(z, slices, *flat):
    size = z.span * z.columns
    scratch = [6 * size, z.count * z.columns * z.rows, CHUNK * z.columns * z.rows]
    scratch += [2 * z.halo_rows, 2 * z.edge_rows] + [size] * (4 * TOGETHER)
    return pl.pallas_call(
        functools.partial(transport_kernel, z, slices),
        out_shape=(rows_of(z.count * z.blocks // slices),) * (z.groups * slices),
        in_specs=[VMEM] * len(flat),
        out_specs=(VMEM,) * (z.groups * slices),
        scratch_shapes=[pltpu.VMEM((n, LANES), jnp.float32) for n in scratch],
        compiler_params=pltpu.CompilerParams(vmem_limit_bytes=20 << 20),
        cost_estimate=pl.CostEstimate(flops=400 * z.count * z.stride * LANES, bytes_accessed=0, transcendentals=0),
        name="transport",
    )(*flat)


def rates(z, warm, glow, lit, rate, barrier, photo):
    reactions = rate.shape[0]
    return pl.pallas_call(
        functools.partial(rates_kernel, z.blocks // SUB),
        out_shape=rows_of(reactions * z.blocks),
        in_specs=[VMEM] * 3 + [SMEM] * 3,
        out_specs=VMEM,
        compiler_params=pltpu.CompilerParams(vmem_limit_bytes=16 << 20),
        cost_estimate=pl.CostEstimate(
            flops=40 * reactions * z.blocks * LANES, bytes_accessed=0, transcendentals=0
        ),
        name="rates",
    )(warm, glow, lit, rate, barrier, photo)


def chemistry(z, species, number, arrived, lit, k, table, out):
    size = species * z.slab
    more = () if out is None else (out,)
    args = (*arrived, lit, k, table, *more)
    scratch = [pltpu.VMEM((species, z.slab, LANES), jnp.float32)]
    buffer = pltpu.VMEM((size, LANES), jnp.float32)
    scratch += [buffer, pltpu.SMEM(table.shape, jnp.int32)] + [buffer] * (3 * WAYS)
    scratch += [pltpu.SemaphoreType.DMA((BATCHES + 1,))]
    return pl.pallas_call(
        functools.partial(chemistry_kernel, z, species, number),
        out_shape=jax.ShapeDtypeStruct((species, z.blocks, LANES), jnp.float32),
        in_specs=[VMEM] * (len(arrived) + 2) + [ANY] * (1 + len(more)),
        out_specs=ANY,
        scratch_shapes=scratch,
        input_output_aliases={len(args) - 1: 0} if more else {},
        compiler_params=pltpu.CompilerParams(vmem_limit_bytes=28 << 20),
        cost_estimate=pl.CostEstimate(flops=400 * size * LANES, bytes_accessed=0, transcendentals=0),
        name="chemistry",
    )(*args)


def body(
    mixing_ratio_field,
    eastward_face_cfl,
    northward_face_cfl,
    upward_face_cfl,
    thermal_anomaly,
    radiant_flux,
    daylight_mask,
    baseline_kinetic_coefficient,
    arrhenius_barrier,
    photodissociation_factor,
    stoichiometry_table,
):
    groups = lax.axis_size("tracer")
    strips = lax.axis_size("space")
    z = Sizes(mixing_ratio_field, groups)
    courant = flat_rows(jnp.stack([eastward_face_cfl, northward_face_cfl, upward_face_cfl]))
    whole = mixing_ratio_field
    near_pairs = [(i, i ^ 1) for i in range(strips) if i ^ 1 < strips]
    far_pairs = [(i, ((i + 1) ^ 1) - 1) for i in range(strips) if 0 <= ((i + 1) ^ 1) - 1 < strips]
    fields, halos = [], []
    for part in range(PARTS):
        if part == 0:
            near, far, ready, courant = pack(z, part, flat_rows(whole[: z.count]), courant)
        else:
            whole, _ = lax.optimization_barrier((whole, ready))
            near, far, ready = pack(z, part, flat_rows(whole[part * z.count : (part + 1) * z.count]))
        far = lax.ppermute(far, "space", far_pairs)
        near = lax.ppermute(near, "space", near_pairs)
        fields.append(ready)
        halos.append((near, far))
    edges = [halo[z.halo_rows :] for halo in halos[0]]
    arrived = [[] for _ in range(z.slices)]
    for part in range(PARTS):
        ready = fields[part]
        slices = z.slices if part == PARTS - 1 else 1
        if part > 0:
            ready, _ = lax.optimization_barrier((ready, moved[0]))
        moved = transport(z, slices, ready, courant, *edges, *halos[part])
        for piece in range(slices):
            for k in range(groups):
                block = moved[k * slices + piece]
                if k > 0:
                    block = lax.ppermute(block, "tracer", [(i, i ^ k) for i in range(groups)])
                for number in range(z.slices):
                    if slices == 1 or number == piece:
                        arrived[number].append(block)
    mask, table, _ = lax.optimization_barrier((daylight_mask, stoichiometry_table, moved[0]))
    lit = jnp.broadcast_to(jnp.moveaxis(mask, 2, 1).reshape(z.blocks, 1), (z.blocks, LANES))
    k = rates(
        z,
        flat_rows(thermal_anomaly),
        flat_rows(radiant_flux),
        lit,
        baseline_kinetic_coefficient,
        arrhenius_barrier,
        photodissociation_factor,
    )
    species = z.species * groups
    table = table.reshape(-1) * z.slab
    out = None
    for number in range(z.slices):
        out = chemistry(z, species, number, arrived[number], lit, k, table, out)
    out = out.reshape(species, z.levels, z.tiles, z.part, LANES)
    return jnp.moveaxis(out, 2, 3).reshape(species, z.levels, z.part, z.width)


def solution(mesh):
    placed = (
        P("tracer", None, "space", None),
        P(None, "space", None),
        P(None, "space", None),
        P(None, "space", None),
        P(None, ("space", "tracer"), None),
        P(None, ("space", "tracer"), None),
        P(None, ("space", "tracer"), None),
        P(),
        P(),
        P(),
        P(),
    )
    return jax.shard_map(
        body,
        mesh=mesh,
        in_specs=placed,
        out_specs=P(None, None, ("space", "tracer"), None),
        check_vma=False,
    )
```

```python
import functools

import jax
import jax.numpy as jnp
from jax import lax
from jax.experimental import pallas as pl
from jax.experimental.pallas import tpu as pltpu
from jax.sharding import PartitionSpec as P


SECTIONS = 3
DAY_STEPS = 2
LANES = 128
SUB = 8
LOW = 2 * SECTIONS
HIGH = SECTIONS
PARTS = 2
SPLIT_LEVELS = False
WAYS = 2
TOGETHER = 8
CHUNK = 16
BATCHES = 4
LOG2E = 1.4426950408889634


def flat_rows(cells):
    *lead, rows, width = cells.shape
    sub = min(rows, SUB)
    split = cells.reshape(*lead, rows // sub, sub, width // LANES, LANES)
    return jnp.moveaxis(split, -2, -3).reshape(-1, LANES)


class Sizes:
    def __init__(self, field, groups):
        self.species, self.levels, self.rows, self.width = field.shape
        self.tiles = self.width // LANES
        self.groups = groups
        self.part = self.rows // groups
        self.blocks = self.levels * self.tiles * self.part
        self.stride = self.levels * self.rows * self.tiles
        self.columns = self.levels * self.tiles
        self.count = self.species // PARTS
        self.area = self.tiles * self.part
        self.slices = self.levels if SPLIT_LEVELS and self.area % SUB == 0 else 1
        self.slab = self.blocks // self.slices
        self.halo_rows = LOW * self.columns * self.count
        self.span = self.rows + 2 * SUB
        self.edge_rows = 3 * self.columns * SUB

    def source_row(self, level, row, tile):
        return ((level * (self.rows // SUB) + row // SUB) * self.tiles + tile) * SUB + row % SUB

    def pairs(self):
        return [(level, tile) for level in range(self.levels) for tile in range(self.tiles)]


def middle(a, b):
    return jnp.maximum(jnp.minimum(a, b), jnp.minimum(jnp.maximum(a, b), 0.0))


def shift_columns(parts, amount):
    if amount > 0:
        return [pltpu.roll(parts[-1], 1, 1)] + parts[:-1]
    return parts[1:] + [pltpu.roll(parts[0], LANES - 1, 1)]


def spread_matrix(tiles, back):
    natural = lax.broadcasted_iota(jnp.int32, (tiles * LANES, tiles * LANES), 1 if back else 0)
    spread = lax.broadcasted_iota(jnp.int32, (tiles * LANES, tiles * LANES), 0 if back else 1)
    hit = natural == (spread % LANES) * tiles + spread // LANES
    return jnp.where(hit, 1.0, 0.0).astype(jnp.bfloat16)


def reorder(parts, matrix):
    x = jnp.concatenate(parts, axis=1)
    total = None
    for _ in range(3):
        piece = x.astype(jnp.bfloat16)
        x = x - piece.astype(jnp.float32)
        term = jnp.dot(piece, matrix, preferred_element_type=jnp.float32)
        total = term if total is None else total + term
    return [total[:, k * LANES : (k + 1) * LANES] for k in range(len(parts))]


def pack_kernel(z, part, x_ref, *refs):
    forth = spread_matrix(z.tiles, False)
    if part == 0:
        winds, (near_ref, far_ref, field, courant_out) = refs[:3], refs[3:]
    else:
        near_ref, far_ref, field = refs
    odd = lax.rem(lax.axis_index("space"), 2)
    sides = ((near_ref, odd), (far_ref, 1 - odd))

    def spread(flat, strips):
        split = flat.reshape(strips, z.rows // SUB, z.tiles, SUB, LANES)
        return reorder([split[:, :, t].reshape(strips * z.rows, LANES) for t in range(z.tiles)], forth)

    if part == 0:
        parts = spread(jnp.concatenate([wind[...] for wind in winds]), 3 * z.levels)
        shifted = shift_columns(parts, -1)
        for strip in range(3 * z.levels):
            rows = slice(strip * z.rows, (strip + 1) * z.rows)
            for tile in range(z.tiles):
                value = (shifted if strip // z.levels == 1 else parts)[tile][rows]
                col = strip * z.tiles + tile
                courant_out[pl.ds(col * z.rows, z.rows), :] = value

    def some(index, carry):
        strips = CHUNK * z.levels
        size = strips * z.tiles * z.rows
        values = spread(x_ref[pl.ds(pl.multiple_of(index * size, SUB), size), :], strips)
        for strip in range(strips):
            for tile in range(z.tiles):
                at = pl.multiple_of(index * size + (strip * z.tiles + tile) * z.rows, SUB)
                field[pl.ds(at, z.rows), :] = values[tile][strip * z.rows : (strip + 1) * z.rows]
        return carry

    lax.fori_loop(0, z.count // CHUNK, some, 0)

    if part == 0:
        for ref, below in sides:
            for col in range(3 * z.columns):
                source = col * z.rows + (1 - below) * (z.rows - SUB)
                ref[pl.ds(z.halo_rows + col * SUB, SUB), :] = courant_out[pl.ds(pl.multiple_of(source, SUB), SUB), :]

    def edges(index, carry):
        for ref, below in sides:
            for col in range(z.columns):
                target = index * z.columns + col
                source = target * z.rows + (1 - below) * (z.rows - LOW)
                ref[pl.ds(target * LOW, LOW), :] = field[pl.ds(source, LOW), :]
        return carry

    lax.fori_loop(0, z.count, edges, 0, unroll=4)


def transport_kernel(z, slices, field_ref, courant_ref, near_edge, far_edge, near_ref, far_ref, *refs):
    span = z.span
    cols = range(z.columns)
    total = z.groups * slices
    outs, (coef, final, natural, halo, edge), slots = refs[:total], refs[total : total + 5], refs[total + 5 :]
    odd = lax.rem(lax.axis_index("space"), 2)
    for source, above in ((near_ref, 1 - odd), (far_ref, odd)):

        def place_halo(i, carry):
            target = pl.multiple_of(above * z.halo_rows + i * SUB, SUB)
            halo[pl.ds(target, SUB), :] = source[pl.ds(pl.multiple_of(i * SUB, SUB), SUB), :]
            return carry

        lax.fori_loop(0, z.halo_rows // SUB, place_halo, 0, unroll=12)
    for source, above in ((near_edge, 1 - odd), (far_edge, odd)):
        for row in range(0, z.edge_rows, SUB):
            target = pl.multiple_of(above * z.edge_rows + row, SUB)
            edge[pl.ds(target, SUB), :] = source[pl.ds(row, SUB), :]

    def coef_row(kind, which, col, j):
        return ((kind * 2 + which) * z.columns + col) * span + j

    for kind in range(3):
        for col in cols:
            one = kind * z.columns + col
            tiles = [edge[pl.ds(one * SUB, SUB), :]]
            tiles += [courant_ref[pl.ds(one * z.rows + row, SUB), :] for row in range(0, z.rows, SUB)]
            tiles += [edge[pl.ds(z.edge_rows + one * SUB, SUB), :]]
            for k, value in enumerate(tiles):
                coef[pl.ds(coef_row(kind, 0, col, k * SUB), SUB), :] = value
                coef[pl.ds(coef_row(kind, 1, col, k * SUB), SUB), :] = 0.5 * value * (1.0 - value)

    def weights(kind, col, j):
        return [coef[pl.ds(coef_row(kind, which, col, j), SUB), :] for which in range(2)]

    def one_species(index, start, fields, fluxes):
        for col in cols:
            base = index * z.columns + col
            at = col * span + SUB
            start[pl.ds(at - LOW, LOW), :] = halo[pl.ds(base * LOW, LOW), :]
            start[pl.ds(at + z.rows, HIGH), :] = halo[pl.ds(z.halo_rows + base * LOW, HIGH), :]
            start[pl.ds(at, z.rows), :] = field_ref[pl.ds(pl.multiple_of(base * z.rows, SUB), z.rows), :]
        for step in range(SECTIONS):
            write = fields[step % 2]
            source = start if step == 0 else fields[(step + 1) % 2]
            read = lambda col, j, ref=source: ref[pl.ds(col * span + j, SUB), :]
            bottom = SUB - LOW + 2 * (step + 1)
            top = SUB + z.rows + HIGH - (step + 1)
            for j in range(bottom - 1, top, SUB):
                for col in cols:
                    below, here, above = [read(col, j + k) for k in (-1, 0, 1)]
                    a, b = weights(0, col, j + 1)
                    fluxes[pl.ds(col * span + j, SUB), :] = a * here + b * middle(here - below, above - here)
            for j in range(bottom, top, SUB):
                c = []
                for col in cols:
                    leave = fluxes[pl.ds(col * span + j, SUB), :]
                    enter = fluxes[pl.ds(col * span + j - 1, SUB), :]
                    c.append(read(col, j) - (leave - enter))
                for level in range(z.levels):
                    mine = slice(level * z.tiles, (level + 1) * z.tiles)
                    row = c[mine]
                    back = [v - w for v, w in zip(row, shift_columns(row, 1))]
                    ahead = shift_columns(back, -1)
                    leave = []
                    for tile in range(z.tiles):
                        a, b = weights(1, level * z.tiles + tile, j)
                        leave.append(a * row[tile] + b * middle(back[tile], ahead[tile]))
                    enter = shift_columns(leave, 1)
                    c[mine] = [row[t] - (leave[t] - enter[t]) for t in range(z.tiles)]
                for tile in range(z.tiles):
                    column = [c[level * z.tiles + tile] for level in range(z.levels)]
                    steps = [column[0]]
                    steps += [column[k + 1] - column[k] for k in range(z.levels - 1)]
                    steps += [-column[-1]]
                    lift = None
                    for level in range(z.levels):
                        col = level * z.tiles + tile
                        a, b = weights(2, col, j)
                        rising = a * column[level] + b * middle(steps[level], steps[level + 1])
                        net = rising if lift is None else rising - lift
                        lift = rising
                        value = column[level] - net
                        if step < SECTIONS - 1:
                            write[pl.ds(col * span + j, SUB), :] = value
                        else:
                            base = (index * z.columns + col) * z.rows + j - SUB
                            final[pl.ds(pl.multiple_of(base, SUB), SUB), :] = value

    def some_species(index, carry):
        for k in range(TOGETHER):
            one_species(index * TOGETHER + k, slots[4 * k], slots[4 * k + 1 : 4 * k + 3], slots[4 * k + 3])
        return carry

    lax.fori_loop(0, z.count // TOGETHER, some_species, 0)

    back = spread_matrix(z.tiles, True)
    me = lax.axis_index("tracer")

    def scatter(index, carry):
        many = CHUNK * z.levels
        size = many * z.tiles * z.rows
        whole = final[pl.ds(pl.multiple_of(index * size, SUB), size), :].reshape(many, z.tiles, z.rows, LANES)
        parts = reorder([whole[:, t].reshape(many * z.rows, LANES) for t in range(z.tiles)], back)
        for one in range(many):
            for tile in range(z.tiles):
                strip = one * z.tiles + tile
                natural[pl.ds(strip * z.rows, z.rows), :] = parts[tile][one * z.rows : (one + 1) * z.rows]
        share = z.columns // slices
        for k in range(z.groups):
            first = (me ^ k) * z.part
            for strip in range(many * z.tiles):
                one, col = divmod(strip, z.columns)
                out_ref = outs[k * slices + col // share]
                at = ((index * CHUNK + one) * share + col % share) * z.part
                out_ref[pl.ds(at, z.part), :] = natural[pl.ds(strip * z.rows + first, z.part), :]
        return carry

    lax.fori_loop(0, z.count // CHUNK, scatter, 0)


def rates_kernel(pieces, warm_ref, glow_ref, lit_ref, rate_ref, barrier_ref, photo_ref, out_ref):
    warm = [(1.0 - warm_ref[pl.ds(p * SUB, SUB), :]) * LOG2E for p in range(pieces)]
    glow = [
        jnp.where(lit_ref[pl.ds(p * SUB, SUB), :] == 1, glow_ref[pl.ds(p * SUB, SUB), :], 0.0)
        for p in range(pieces)
    ]

    def one(r, carry):
        for p in range(pieces):
            at = pl.ds(pl.multiple_of(r * pieces * SUB, SUB) + p * SUB, SUB)
            out_ref[at, :] = rate_ref[r] * jnp.exp2(barrier_ref[r] * warm[p]) + photo_ref[r] * glow[p]
        return carry

    lax.fori_loop(0, rate_ref.shape[0], one, 0, unroll=8)


def chemistry_kernel(z, species, number, *refs):
    pieces = z.slab // SUB
    total = PARTS * z.groups
    sources, (lit_ref, k_ref, table_in) = refs[:total], refs[total : total + 3]
    out_hbm, result, state = refs[total + 3 + (number > 0) :][:3]
    made, lost_a, lost_b = [refs[-1 - (3 - i) * WAYS :][:WAYS] for i in range(3)]
    sems = refs[-1]
    table_ref = refs[-2 - 3 * WAYS]
    table_load = pltpu.make_async_copy(table_in, table_ref, sems.at[BATCHES])
    table_load.start()
    reactions = k_ref.shape[0] // z.blocks
    base = number * z.slab

    def cell(row, piece):
        return pl.ds(pl.multiple_of(row, SUB) + piece * SUB, SUB)

    lit = [lit_ref[pl.ds(base + p * SUB, SUB), :] == 1 for p in range(pieces)]
    steps = [jnp.where(lit[p], float(DAY_STEPS), 1.0) for p in range(pieces)]
    zero = jnp.zeros((SUB, LANES), jnp.float32)
    me = lax.axis_index("tracer")

    def prepare(at, p, value):
        for way in range(WAYS):
            made[way][at, :] = zero if way else steps[p] * value
            lost_a[way][at, :] = zero if way else steps[p]
            lost_b[way][at, :] = zero

    def begin(index, carry):
        for i, ref in enumerate(sources):
            part, k = divmod(i, z.groups)
            first = (me ^ k) * z.species + part * z.count
            for p in range(pieces):
                if part < PARTS - 1:
                    value = ref[cell(index * z.blocks + base, p), :]
                else:
                    value = ref[cell(index * z.slab, p), :]
                at = cell((first + index) * z.slab, p)
                state[at, :] = value
                prepare(at, p, value)
        return carry

    lax.fori_loop(0, z.count, begin, 0)

    table_load.wait()

    def react(r, way):
        first, second, product = table_ref[r], table_ref[reactions + r], table_ref[2 * reactions + r]
        for p in range(pieces):
            k = k_ref[cell(r * z.blocks + base, p), :]
            x = state[cell(first, p), :]
            y = state[cell(second, p), :]
            kx = k * x
            ky = k * y
            made[way][cell(product, p), :] += kx * y
            lost_a[way][cell(first, p), :] += ky
            lost_b[way][cell(second, p), :] += kx

    def several(i, carry):
        for way in range(WAYS):
            react(i * WAYS + way, way)
        return carry

    batch = species // BATCHES

    def export(i):
        rows = pl.ds(i * batch, batch)
        return pltpu.make_async_copy(result.at[rows], out_hbm.at[rows, pl.ds(base, z.slab)], sems.at[i])

    for sub in range(DAY_STEPS):
        lax.fori_loop(0, reactions // WAYS, several, 0, unroll=16 // WAYS)

        def finish(s, carry):
            for p in range(pieces):
                at = cell(s * z.slab, p)
                top = sum(ref[at, :] for ref in made)
                value = top / sum(ref[at, :] for ref in (*lost_a, *lost_b))
                if sub < DAY_STEPS - 1:
                    prepare(at, p, value)
                    if sub == 0:
                        state[at, :] = value
                if sub > 0:
                    value = jnp.where(lit[p], value, state[at, :])
                    result[s, pl.ds(p * SUB, SUB), :] = value
            return carry

        if sub < DAY_STEPS - 1:
            lax.fori_loop(0, species, finish, 0, unroll=8)
    for i in range(BATCHES):
        lax.fori_loop(i * batch, (i + 1) * batch, finish, 0, unroll=8)
        export(i).start()
    for i in range(BATCHES):
        export(i).wait()


VMEM = pl.BlockSpec(memory_space=pltpu.VMEM)
SMEM = pl.BlockSpec(memory_space=pltpu.SMEM)


def rows_of(count):
    return jax.ShapeDtypeStruct((count, LANES), jnp.float32)


ANY = pl.BlockSpec(memory_space=pl.ANY)
HBM = pl.BlockSpec(memory_space=pltpu.HBM)


def pack(z, part, *flat):
    extra = z.edge_rows if part == 0 else 0
    rows = [z.halo_rows + extra, z.halo_rows + extra, z.count * z.columns * z.rows]
    if part == 0:
        rows.append(3 * z.columns * z.rows)
    return pl.pallas_call(
        functools.partial(pack_kernel, z, part),
        out_shape=tuple(rows_of(n) for n in rows),
        in_specs=[VMEM] * len(flat),
        out_specs=(VMEM,) * len(rows),
        compiler_params=pltpu.CompilerParams(vmem_limit_bytes=16 << 20),
        cost_estimate=pl.CostEstimate(flops=100 * z.count * z.stride * LANES, bytes_accessed=0, transcendentals=0),
        name="pack",
    )(*flat)


def transport(z, slices, *flat):
    size = z.span * z.columns
    scratch = [6 * size, z.count * z.columns * z.rows, CHUNK * z.columns * z.rows]
    scratch += [2 * z.halo_rows, 2 * z.edge_rows] + [size] * (4 * TOGETHER)
    return pl.pallas_call(
        functools.partial(transport_kernel, z, slices),
        out_shape=(rows_of(z.count * z.blocks // slices),) * (z.groups * slices),
        in_specs=[VMEM] * len(flat),
        out_specs=(VMEM,) * (z.groups * slices),
        scratch_shapes=[pltpu.VMEM((n, LANES), jnp.float32) for n in scratch],
        compiler_params=pltpu.CompilerParams(vmem_limit_bytes=20 << 20),
        cost_estimate=pl.CostEstimate(flops=400 * z.count * z.stride * LANES, bytes_accessed=0, transcendentals=0),
        name="transport",
    )(*flat)


def rates(z, warm, glow, lit, rate, barrier, photo):
    reactions = rate.shape[0]
    return pl.pallas_call(
        functools.partial(rates_kernel, z.blocks // SUB),
        out_shape=rows_of(reactions * z.blocks),
        in_specs=[VMEM] * 3 + [SMEM] * 3,
        out_specs=VMEM,
        compiler_params=pltpu.CompilerParams(vmem_limit_bytes=16 << 20),
        cost_estimate=pl.CostEstimate(
            flops=40 * reactions * z.blocks * LANES, bytes_accessed=0, transcendentals=0
        ),
        name="rates",
    )(warm, glow, lit, rate, barrier, photo)


def chemistry(z, species, number, arrived, lit, k, table, out):
    size = species * z.slab
    more = () if out is None else (out,)
    args = (*arrived, lit, k, table, *more)
    scratch = [pltpu.VMEM((species, z.slab, LANES), jnp.float32)]
    buffer = pltpu.VMEM((size, LANES), jnp.float32)
    scratch += [buffer, pltpu.SMEM(table.shape, jnp.int32)] + [buffer] * (3 * WAYS)
    scratch += [pltpu.SemaphoreType.DMA((BATCHES + 1,))]
    return pl.pallas_call(
        functools.partial(chemistry_kernel, z, species, number),
        out_shape=jax.ShapeDtypeStruct((species, z.blocks, LANES), jnp.float32),
        in_specs=[VMEM] * (len(arrived) + 2) + [ANY] * (1 + len(more)),
        out_specs=ANY,
        scratch_shapes=scratch,
        input_output_aliases={len(args) - 1: 0} if more else {},
        compiler_params=pltpu.CompilerParams(vmem_limit_bytes=28 << 20),
        cost_estimate=pl.CostEstimate(flops=400 * size * LANES, bytes_accessed=0, transcendentals=0),
        name="chemistry",
    )(*args)


def body(
    mixing_ratio_field,
    eastward_face_cfl,
    northward_face_cfl,
    upward_face_cfl,
    thermal_anomaly,
    radiant_flux,
    daylight_mask,
    baseline_kinetic_coefficient,
    arrhenius_barrier,
    photodissociation_factor,
    stoichiometry_table,
):
    groups = lax.axis_size("tracer")
    strips = lax.axis_size("space")
    z = Sizes(mixing_ratio_field, groups)
    winds = [flat_rows(a) for a in (eastward_face_cfl, northward_face_cfl, upward_face_cfl)]
    whole = mixing_ratio_field
    near_pairs = [(i, i ^ 1) for i in range(strips) if i ^ 1 < strips]
    far_pairs = [(i, ((i + 1) ^ 1) - 1) for i in range(strips) if 0 <= ((i + 1) ^ 1) - 1 < strips]
    fields, halos = [], []
    for part in range(PARTS):
        if part == 0:
            near, far, ready, courant = pack(z, part, flat_rows(whole[: z.count]), *winds)
        else:
            whole, _ = lax.optimization_barrier((whole, ready))
            near, far, ready = pack(z, part, flat_rows(whole[part * z.count : (part + 1) * z.count]))
        far = lax.ppermute(far, "space", far_pairs)
        near = lax.ppermute(near, "space", near_pairs)
        fields.append(ready)
        halos.append((near, far))
    edges = [halo[z.halo_rows :] for halo in halos[0]]
    arrived = [[] for _ in range(z.slices)]
    for part in range(PARTS):
        ready = fields[part]
        slices = z.slices if part == PARTS - 1 else 1
        if part > 0:
            ready, _ = lax.optimization_barrier((ready, moved[0]))
        moved = transport(z, slices, ready, courant, *edges, *halos[part])
        for piece in range(slices):
            for k in range(groups):
                block = moved[k * slices + piece]
                if k > 0:
                    block = lax.ppermute(block, "tracer", [(i, i ^ k) for i in range(groups)])
                for number in range(z.slices):
                    if slices == 1 or number == piece:
                        arrived[number].append(block)
    mask, table, _ = lax.optimization_barrier((daylight_mask, stoichiometry_table, moved[0]))
    lit = jnp.broadcast_to(jnp.moveaxis(mask, 2, 1).reshape(z.blocks, 1), (z.blocks, LANES))
    k = rates(
        z,
        flat_rows(thermal_anomaly),
        flat_rows(radiant_flux),
        lit,
        baseline_kinetic_coefficient,
        arrhenius_barrier,
        photodissociation_factor,
    )
    species = z.species * groups
    table = table.reshape(-1) * z.slab
    out = None
    for number in range(z.slices):
        out = chemistry(z, species, number, arrived[number], lit, k, table, out)
    out = out.reshape(species, z.levels, z.tiles, z.part, LANES)
    return jnp.moveaxis(out, 2, 3).reshape(species, z.levels, z.part, z.width)


def solution(mesh):
    placed = (
        P("tracer", None, "space", None),
        P(None, "space", None),
        P(None, "space", None),
        P(None, "space", None),
        P(None, ("space", "tracer"), None),
        P(None, ("space", "tracer"), None),
        P(None, ("space", "tracer"), None),
        P(),
        P(),
        P(),
        P(),
    )
    return jax.shard_map(
        body,
        mesh=mesh,
        in_specs=placed,
        out_specs=P(None, None, ("space", "tracer"), None),
        check_vma=False,
    )
```
